32 devices in a mesh: seq: 8 (over z, y), tp: 4 (over x, core).
Axes of the slice: x: 2, y: 2, z: 4, core: 2. Of those that a mesh axis runs over, the one named last changes fastest.
Arguments:
- tokens: bfloat16 [4096, 2560], P('seq', 'tp'), may hold values from -6 to 6
- gate_weight: bfloat16 [2560, 5120], P(None, 'tp'), may hold values from -0.125 to 0.125
- inner_weight: bfloat16 [2560, 5120], P(None, 'tp'), may hold values from -0.125 to 0.125
- state_weight: bfloat16 [2560, 256], replicated, may hold values from -0.125 to 0.125
- step_weight: bfloat16 [2560, 80], P(None, 'tp'), may hold values from -0.125 to 0.125
- conv_inner: float32 [4, 5120], P(None, 'tp'), may hold values from -3 to 3
- conv_state: float32 [4, 256], replicated, may hold values from -3 to 3
- step_bias: float32 [80], P('tp'), may hold values from -3 to 1
- decay_rate: float32 [80], P('tp'), may hold values from 1e-05 to 0.02
- skip_gain: float32 [80], P('tp'), may hold values from 0.5 to 2
- norm_gain: float32 [5120], P('tp'), may hold values from 0.1 to 1.9
- out_weight: bfloat16 [5120, 2560], P('tp'), may hold values from -0.078125 to 0.078125
Outputs:
- layer_out: bfloat16 [4096, 2560], P(('seq', 'tp'))
The draws below stay inside these ranges and needn't reach their ends.
All inputs are finite; a program needn't handle non-finite values.
Results may differ from the reference program's by a relative error of at most 0.018.
Values may be sent and summed in bfloat16 or wider, within the bound.
A program may use at most 128 MiB of HBM per device.

```python
import math
import jax
import jax.numpy as jnp
from jax import lax

D = 2560
HEADS = 80
HEAD_DIM = 64
STATE = 128
KERNEL = 4
GROUP = 256
INNER = 5120
TOKENS = 4096


def block_levels(stream_key, shape, shards, smallest, top_value):
    def one(position, parts):
        steps = jax.random.uniform(jax.random.fold_in(jax.random.fold_in(stream_key, 6), position), (parts,), jnp.float32, smallest / len(shards), top_value / len(shards))
        return jnp.repeat(jnp.exp(steps), shape[position] // parts).reshape((-1,) + (1,) * (len(shape) - position - 1))

    level = one(*shards[0])
    for cut in shards[1:]:
        level = level * one(*cut)
    return level


def centred(rng, shape, width, reach, split=(), kind=jnp.bfloat16):
    array = width * jax.random.normal(rng, shape, jnp.float32)
    if split:
        array = array * block_levels(rng, shape, split, -0.22, 0.18)
    return jnp.clip(array, -reach, reach).astype(kind)


def setup_inputs(seed: int = 0) -> dict:
    key_list = jax.random.split(jax.random.key(seed), 13)
    return {
        "tokens": centred(key_list[0], (TOKENS, D), 1.0, 6.0, ((0, 8), (1, 4))),
        "gate_weight": centred(key_list[1], (D, INNER), D ** -0.5, 0.125, ((1, 4),)),
        "inner_weight": centred(key_list[2], (D, INNER), D ** -0.5, 0.125, ((1, 4),)),
        "state_weight": centred(key_list[3], (D, 2 * STATE), D ** -0.5, 0.125),
        "step_weight": centred(key_list[4], (D, HEADS), D ** -0.5, 0.125, ((1, 4),)),
        "conv_inner": centred(key_list[5], (KERNEL, INNER), KERNEL ** -0.5, 3.0, ((1, 4),), jnp.float32),
        "conv_state": centred(key_list[6], (KERNEL, 2 * STATE), KERNEL ** -0.5, 3.0, (), jnp.float32),
        "step_bias": jnp.clip(-3.0 + 4.0 * jax.random.uniform(key_list[7], (HEADS,), jnp.float32) ** block_levels(key_list[7], (HEADS,), ((0, 4),), -0.2, 0.2), -3.0, 1.0),
        "decay_rate": jnp.clip(jnp.exp(math.log(0.02) - 7.6009025 * jax.random.uniform(key_list[8], (HEADS,), jnp.float32) ** block_levels(key_list[8], (HEADS,), ((0, 4),), -0.2, 0.2)), 9.999999747378752e-06, 0.02),
        "skip_gain": jnp.clip(0.5 + 1.5 * jax.random.uniform(key_list[9], (HEADS,), jnp.float32) ** block_levels(key_list[9], (HEADS,), ((0, 4),), -0.2, 0.2), 0.5, 2.0),
        "norm_gain": jnp.clip(1.0 + 0.18 * jax.random.normal(key_list[10], (INNER,), jnp.float32), 0.1, 1.9),
        "out_weight": centred(key_list[11], (INNER, D), INNER ** -0.5, 0.078125, ((0, 4),)),
    }


def reference(tokens, gate_weight, inner_weight, state_weight, step_weight, conv_inner, conv_state, step_bias, decay_rate, skip_gain, norm_gain, out_weight):
    gate_act = jnp.dot(tokens, gate_weight, preferred_element_type=jnp.float32).astype(jnp.bfloat16)
    mixed_in = jnp.concatenate([jnp.dot(tokens, inner_weight, preferred_element_type=jnp.float32), jnp.dot(tokens, state_weight, preferred_element_type=jnp.float32)], axis=1).astype(jnp.bfloat16)
    step_raw = jnp.dot(tokens, step_weight, preferred_element_type=jnp.float32)
    kernel = jnp.concatenate([conv_inner, conv_state], axis=1)
    padded = jnp.concatenate([jnp.zeros((KERNEL - 1, mixed_in.shape[1]), jnp.bfloat16), mixed_in], axis=0)
    conv_sum = jnp.zeros(mixed_in.shape, jnp.float32)
    for tap in range(KERNEL):
        conv_sum = conv_sum + padded[tap:tap + TOKENS].astype(jnp.float32) * kernel[tap][None, :]
    conv_out = jax.nn.silu(conv_sum).astype(jnp.bfloat16)
    inner_act = conv_out[:, :INNER].reshape(TOKENS, HEADS, HEAD_DIM)
    inject = conv_out[:, INNER:INNER + STATE]
    readout = conv_out[:, INNER + STATE:]
    time_step = jax.nn.softplus(step_raw + step_bias[None, :])
    log_decay = -time_step * decay_rate[None, :]
    blocks = TOKENS // GROUP
    causal = jnp.arange(GROUP)[:, None] >= jnp.arange(GROUP)[None, :]
    highest = lax.Precision.HIGHEST

    def advance(carried, block):
        inner_blk, inject_blk, readout_blk, step_blk, log_blk = block
        cumulative = jnp.cumsum(log_blk, axis=0)
        scores = jnp.dot(readout_blk, inject_blk.T, preferred_element_type=jnp.float32)
        log_gaps = cumulative.T[:, :, None] - cumulative.T[:, None, :]
        decay_mask = jnp.exp(jnp.where(causal[None], log_gaps, -jnp.inf))
        mixing = (scores[None] * decay_mask * step_blk.T[:, None, :]).astype(jnp.bfloat16)
        intra_out = jnp.einsum('hts,shp->thp', mixing.astype(jnp.float32), inner_blk.astype(jnp.float32), precision=highest)
        state_reads = jnp.einsum('tn,hpn->thp', readout_blk.astype(jnp.float32), carried, precision=highest) * jnp.exp(cumulative)[:, :, None]
        ending = cumulative[-1]
        tail_weight = jnp.exp(ending[None, :] - cumulative) * step_blk
        contribution = jnp.einsum('thp,tn->hpn', inner_blk.astype(jnp.float32) * tail_weight[:, :, None], inject_blk.astype(jnp.float32), precision=highest)
        carried = jnp.exp(ending)[:, None, None] * carried + contribution
        return (carried, intra_out + state_reads)
    start_state = jnp.zeros((HEADS, HEAD_DIM, STATE), jnp.float32)
    stacked = (inner_act.reshape(blocks, GROUP, HEADS, HEAD_DIM), inject.reshape(blocks, GROUP, STATE), readout.reshape(blocks, GROUP, STATE), time_step.reshape(blocks, GROUP, HEADS), log_decay.reshape(blocks, GROUP, HEADS))
    final_state, block_outs = lax.scan(advance, start_state, stacked)
    ssd_out = block_outs.reshape(TOKENS, HEADS, HEAD_DIM) + skip_gain[None, :, None] * inner_act.astype(jnp.float32)
    gated = ssd_out.reshape(TOKENS, INNER) * jax.nn.silu(gate_act.astype(jnp.float32))
    mean_square = lax.optimization_barrier(jnp.mean(gated * gated, axis=1))
    normed = (gated * lax.rsqrt(mean_square + 1e-05)[:, None] * norm_gain[None, :]).astype(jnp.bfloat16)
    return jnp.dot(normed, out_weight, preferred_element_type=jnp.float32).astype(jnp.bfloat16)
```

```python
import jax
import jax.numpy as jnp
from jax import lax
from jax.experimental import pallas as pl
from jax.experimental.pallas import tpu as pltpu
from jax.sharding import PartitionSpec as P

GROUP = 256
HALO = 16


def swapped(shard, by):
    size = lax.axis_size("tp")
    return lax.ppermute(shard, "tp", [(i, i ^ by) for i in range(size)])


def shifted(shard, by):
    size = lax.axis_size("seq")
    return lax.ppermute(shard, "seq", [(i, i + by) for i in range(size - by)])


def gather_features(rows):
    size = lax.axis_size("tp")
    me = lax.axis_index("tp")
    width = rows.shape[1]
    held = [(0, rows)]
    step = size // 2
    while step >= 1:
        held = held + [(code ^ step, swapped(part, step)) for code, part in held]
        step //= 2
    parts = dict(held)
    full = jnp.zeros((rows.shape[0], width * size), rows.dtype)
    for code in range(size):
        full = lax.dynamic_update_slice(full, parts[code], (0, (me ^ code) * width))
    return full


def sum_over_tp(part):
    size = lax.axis_size("tp")
    step = 1
    while step < size:
        part = part + swapped(part, step)
        step *= 2
    return part


def prefix_kernel(mine_ref, decay_ref, owner_ref, out_ref):
    owner = owner_ref[...]
    carried = jnp.zeros(mine_ref.shape[1:], jnp.float32)
    for i in range(mine_ref.shape[0]):
        out_ref[i] = carried.astype(jnp.bfloat16)
        log_row = jnp.sum(owner * decay_ref[i : i + 1, :], axis=1, keepdims=True)
        carried = carried * jnp.exp(log_row) + mine_ref[i].astype(jnp.float32)


def earlier_state(local_state, decay_total, head_width, cover):
    size = lax.axis_size("seq")
    rows, states = local_state.shape
    share = rows // size
    me = lax.axis_index("seq")
    heads = decay_total.shape[0]
    wide = jnp.pad(decay_total, (0, -heads % 128))
    wide = jnp.broadcast_to(wide[None, None, :], (size, 1, wide.shape[0]))
    decay_all = lax.all_to_all(wide, "seq", 0, 0, tiled=True)[:, 0, :heads]
    blocks = local_state.reshape(size, share, states)
    blocks, decay_all = lax.optimization_barrier((blocks, decay_all))
    mine = lax.all_to_all(blocks, "seq", 0, 0, tiled=True)
    mine, cover = lax.optimization_barrier((mine, cover))
    row_head = (me * share + jnp.arange(share)) // head_width
    owner = (row_head[:, None] == jnp.arange(decay_total.shape[0])[None, :]).astype(jnp.float32)
    prefixes = pl.pallas_call(
        prefix_kernel,
        out_shape=jax.ShapeDtypeStruct(mine.shape, jnp.bfloat16),
        cost_estimate=pl.CostEstimate(flops=0, bytes_accessed=4 * mine.size, transcendentals=0),
    )(mine, decay_all, owner)
    return lax.all_to_all(prefixes, "seq", 0, 0, tiled=True).reshape(rows, states), cover


def per_head(table, first, count, width, lanes):
    lane = lax.broadcasted_iota(jnp.int32, (table.shape[0], lanes), 1)
    spread = jnp.broadcast_to(table[:, first : first + 1], (table.shape[0], lanes))
    for k in range(1, count):
        spread = jnp.where(lane >= k * width, table[:, first + k : first + k + 1], spread)
    return spread


def silu(value):
    return value * (0.5 * jnp.tanh(0.5 * value) + 0.5)


def conv_kernel(blocks, head_width, lanes, *refs):
    inner_refs, state_refs = refs[:blocks], refs[blocks : 2 * blocks]
    tap_inner, tap_state, tail_ref = refs[2 * blocks : 2 * blocks + 3]
    x_ref, bc_ref, contribution_ref = refs[2 * blocks + 3 :]
    taps = tap_inner.shape[0]
    heads_per = lanes // head_width

    def mixed(chunk_refs, b, span, kernel):
        if b == 0:
            padded = chunk_refs[0][:, span].astype(jnp.float32)
        else:
            last = chunk_refs[b - 1].shape[0] - HALO
            edge = chunk_refs[b - 1][last:, span].astype(jnp.float32)
            padded = jnp.concatenate([edge, chunk_refs[b][:, span].astype(jnp.float32)], axis=0)
        total = padded * kernel[taps - 1 : taps]
        for tap in range(taps - 1):
            total = total + pltpu.roll(padded, taps - 1 - tap, 0) * kernel[tap : tap + 1]
        return silu(total[HALO:]).astype(jnp.bfloat16)

    for b in range(blocks):
        rows = slice(b * GROUP, (b + 1) * GROUP)
        bc = mixed(state_refs, b, slice(None), tap_state[...])
        bc_ref[rows] = bc
        inject = bc[:, : bc.shape[1] // 2]
        tail = tail_ref[rows]
        for p in range(x_ref.shape[1] // lanes):
            span = slice(p * lanes, (p + 1) * lanes)
            x = mixed(inner_refs, b, span, tap_inner[:, span])
            x_ref[rows, span] = x
            weight = per_head(tail, p * heads_per, heads_per, head_width, lanes)
            scaled = (x.astype(jnp.float32) * weight).astype(jnp.bfloat16)
            contribution_ref[b, span] = lax.dot_general(
                scaled, inject, (((0,), (0,)), ((), ())), preferred_element_type=jnp.float32
            )


def intra_kernel(head_width, lanes, x_ref, bc_ref, cum_ref, cum_t_ref, step_t_ref, skip_ref, out_ref):
    states = bc_ref.shape[1] // 2
    heads_per = lanes // head_width
    scores = lax.dot_general(
        bc_ref[:, states:], bc_ref[:, :states], (((1,), (1,)), ((), ())),
        preferred_element_type=jnp.float32,
    )
    t = lax.broadcasted_iota(jnp.int32, scores.shape, 0)
    s = lax.broadcasted_iota(jnp.int32, scores.shape, 1)
    scores = jnp.where(s <= t, scores, 0.0)
    lane = lax.broadcasted_iota(jnp.int32, (x_ref.shape[0], lanes), 1)
    for p in range(x_ref.shape[1] // lanes):
        span = slice(p * lanes, (p + 1) * lanes)
        x = x_ref[:, span]
        total = None
        for k in range(heads_per):
            h = p * heads_per + k
            gaps = jnp.minimum(cum_ref[:, h : h + 1] - cum_t_ref[h : h + 1, :], 0.0)
            mixing = (scores * jnp.exp(gaps) * step_t_ref[h : h + 1, :]).astype(jnp.bfloat16)
            part = jnp.dot(mixing, x, preferred_element_type=jnp.float32)
            total = part if k == 0 else jnp.where(lane >= k * head_width, part, total)
        out_ref[:, span] = total + skip_ref[:, span] * x.astype(jnp.float32)


def gate_kernel(head_width, lanes, intra_ref, bc_ref, cum_ref, gate_ref, gain_ref, state_ref, out_ref, square_ref):
    states = bc_ref.shape[1] // 2
    heads_per = lanes // head_width
    readout = bc_ref[:, states:]
    grown = jnp.exp(cum_ref[...])
    squares = jnp.zeros((readout.shape[0], lanes), jnp.float32)
    for p in range(intra_ref.shape[1] // lanes):
        span = slice(p * lanes, (p + 1) * lanes)
        reads = lax.dot_general(
            readout, state_ref[0, span], (((1,), (1,)), ((), ())), preferred_element_type=jnp.float32
        )
        weight = per_head(grown, p * heads_per, heads_per, head_width, lanes)
        g = (intra_ref[:, span] + reads * weight) * silu(gate_ref[:, span].astype(jnp.float32))
        squares = squares + g * g
        out_ref[:, span] = (g * gain_ref[:, span]).astype(jnp.bfloat16)
    square_ref[...] = jnp.sum(squares, axis=1, keepdims=True)


def project(rows, *weights):
    return [jnp.dot(rows, weight, preferred_element_type=jnp.float32) for weight in weights]


ROWS = 128
PIECES = 5
MESH = pl.DeviceIdType.MESH
HIGHEST = lax.Precision.HIGHEST


def softplus(value):
    return jnp.maximum(value, 0.0) + jnp.log1p(jnp.exp(-jnp.abs(value)))


def chunk_of(index):
    return pl.ds(pl.multiple_of(index * ROWS, ROWS), ROWS)


def tile_of(index, width):
    return pl.ds(pl.multiple_of(index * width, width), width)


def layer_kernel(
    head_width,
    tok_in, gate_in, inner_in, statew_in, stepw_in, convi_in, convs_in, bias_in, rate_in, skip_in, gain_in, outw_in,
    out_ref,
    full, gate_w, inner_w, state_w, step_w, conv_i, conv_s, bias, rate, skip, gain, out_w,
    raw, halo, step_acc, x_ref, bc_ref, y_ref, gate_ref, gated, scaled,
    cum_ref, step_ref, ends, state, starts, state_out, owned, prefixes, carried, decay_out, decay_in,
    square_out, square_in, near_out, near_in, far_acc, far_out, far_in, own_out, own_in, own_acc, result,
    local_sem, x_send, x_recv, d_send, d_recv, f_send, f_recv, halo_send, halo_recv,
    state_send, state_recv, decay_send, decay_recv, back_send, back_recv,
    sq_send, sq_recv, near_send, near_recv, far_send, far_recv, own_send, own_recv, out_sem,
):
    seq_count, tp_count = lax.axis_size("seq"), lax.axis_size("tp")
    seq, tp = lax.axis_index("seq"), lax.axis_index("tp")
    chip, core = tp // 2, tp % 2
    mate, across = chip * 2 + 1 - core, (1 - chip) * 2 + core
    rows, half = full.shape[1], full.shape[2]
    width = half // 2
    channels = inner_w.shape[1]
    states = state_w.shape[1] // 2
    heads = step_w.shape[1]
    chunks = rows // ROWS
    tile = min(256, channels)
    tiles = channels // tile
    spans = channels // 128
    per_span = 128 // head_width
    share = states // seq_count
    piece = out_w.shape[1] // PIECES
    f32, bf16 = jnp.float32, jnp.bfloat16

    def at_tp(index):
        return {"seq": seq, "tp": index}

    def at_seq(index):
        return {"seq": index, "tp": tp}

    def remote(src, dst, send, recv, device):
        return pltpu.make_async_remote_copy(
            src_ref=src, dst_ref=dst, send_sem=send, recv_sem=recv, device_id=device, device_id_type=MESH
        )

    barrier = pltpu.get_barrier_semaphore()
    for step in range(1, tp_count):
        pl.semaphore_signal(barrier, inc=1, device_id=at_tp((tp + step) % tp_count), device_id_type=MESH)
    for step in range(1, seq_count):
        pl.semaphore_signal(barrier, inc=1, device_id=at_seq((seq + step) % seq_count), device_id_type=MESH)

    mine = pl.ds(pl.multiple_of(core * width, width), width)
    theirs = pl.ds(pl.multiple_of((1 - core) * width, width), width)
    near_rows = pl.ds(pl.multiple_of(chip * half, half), half)
    far_rows = pl.ds(pl.multiple_of((1 - chip) * half, half), half)
    loads = [
        (tok_in, full.at[chip, :, mine]),
        (inner_in.at[near_rows], inner_w.at[near_rows]),
        (statew_in.at[near_rows], state_w.at[near_rows]),
        (stepw_in.at[near_rows], step_w.at[near_rows]),
        (inner_in.at[far_rows], inner_w.at[far_rows]),
        (statew_in.at[far_rows], state_w.at[far_rows]),
        (stepw_in.at[far_rows], step_w.at[far_rows]),
        (convi_in, conv_i),
        (convs_in, conv_s),
        (bias_in, bias),
        (rate_in, rate),
        (skip_in, skip),
        (gain_in, gain),
        (gate_in, gate_w),
        (outw_in, out_w),
    ]
    loads = [pltpu.make_async_copy(src, dst, local_sem.at[i]) for i, (src, dst) in enumerate(loads)]
    for load in loads:
        load.start()
    loads[0].wait()
    pl.semaphore_wait(barrier, tp_count - 1 + seq_count - 1)

    def crossing(c):
        part = full.at[chip, chunk_of(c), mine]
        return remote(part, part, x_send.at[c], x_recv.at[c], at_tp(across))

    def beside(c):
        part = full.at[chip, chunk_of(c), mine]
        return remote(part, part, d_send.at[c], d_recv.at[c], at_tp(mate))

    def forwarded(c):
        part = full.at[1 - chip, chunk_of(c), mine]
        return remote(part, part, f_send.at[c], f_recv.at[c], at_tp(mate))

    def arrived(side, columns, c, send, recv):
        part = full.at[side, chunk_of(c), columns]
        return remote(part, part, send.at[c], recv.at[c], at_tp(mate))

    order = [chunks - 1] + list(range(chunks - 1))
    for c in order:
        crossing(c).start()
        beside(c).start()

    for load in loads[1:4]:
        load.wait()
    for c in order:
        arrived(chip, theirs, c, d_send, d_recv).wait_recv()

    near = full.at[chip]

    def first(j, _):
        cols = tile_of(j, tile)
        raw[:, cols] = jnp.dot(near[...], inner_w[near_rows, cols], preferred_element_type=f32)
        return 0

    lax.fori_loop(0, tiles, first, 0)
    raw[:, channels:] = jnp.dot(near[...], state_w[near_rows, :], preferred_element_type=f32)
    step_acc[...] = jnp.dot(near[...], step_w[near_rows, :], preferred_element_type=f32)
    for load in loads[4:13]:
        load.wait()

    def rounded(value):
        return value.astype(bf16).astype(f32)

    def project_chunk(c):
        arrived(1 - chip, mine, c, x_send, x_recv).wait_recv()
        forwarded(c).start()
        arrived(1 - chip, theirs, c, f_send, f_recv).wait_recv()
        at = chunk_of(c)

        def second(j, _):
            cols = tile_of(j, tile)
            more = jnp.dot(full[1 - chip, at, :], inner_w[far_rows, cols], preferred_element_type=f32)
            raw[at, cols] = rounded(raw[at, cols] + more)
            return 0

        lax.fori_loop(0, tiles, second, 0)
        more = jnp.dot(full[1 - chip, at, :], state_w[far_rows, :], preferred_element_type=f32)
        raw[at, channels:] = rounded(raw[at, channels:] + more)
        more = jnp.dot(full[1 - chip, at, :], step_w[far_rows, :], preferred_element_type=f32)
        step_acc[at, :] += more

    t_row = lax.broadcasted_iota(jnp.int32, (ROWS, ROWS), 0)
    s_col = lax.broadcasted_iota(jnp.int32, (ROWS, ROWS), 1)
    causal = s_col <= t_row

    def mix_chunk(c):
        at = chunk_of(c)
        time_step = softplus(step_acc[at, :] + bias[...])
        decay = -time_step * rate[...]
        cum = jnp.dot(causal.astype(f32), decay, preferred_element_type=f32, precision=HIGHEST)
        ending = cum[ROWS - 1 :, :]
        tail = jnp.exp(ending - cum) * time_step
        cum_ref[at, :] = cum
        step_ref[at, :] = time_step
        ends[c] = jnp.broadcast_to(ending, ends.shape[1:])
        before = pl.ds(pl.multiple_of(jnp.maximum(c * ROWS - 8, 0), 8), 8)

        def conv(span, kernel):
            edge = jnp.where(c == 0, halo[:, span], raw[before, span])
            padded = jnp.concatenate([edge, raw[at, span]], axis=0)
            taps = kernel.shape[0]
            total = padded * kernel[taps - 1 : taps]
            for tap in range(taps - 1):
                total = total + pltpu.roll(padded, taps - 1 - tap, 0) * kernel[tap : tap + 1]
            return silu(total[8:]).astype(bf16)

        for p in range(2 * states // 128):
            span = slice(p * 128, (p + 1) * 128)
            bc_ref[at, span] = conv(slice(channels + p * 128, channels + (p + 1) * 128), conv_s[:, span])
        for p in range(spans):
            span = slice(p * 128, (p + 1) * 128)
            x = conv(span, conv_i[:, span])
            x_ref[at, span] = x
            weight = per_head(tail, p * per_span, per_span, head_width, 128)
            scaled[:, span] = (x.astype(f32) * weight).astype(bf16)
        starts[c] = state[...].astype(bf16)
        inject = bc_ref[at, :states]
        grown = jnp.exp(ending)
        for j in range(tiles):
            cols = slice(j * tile, (j + 1) * tile)
            add = lax.dot_general(
                inject, scaled[:, cols], (((0,), (0,)), ((), ())), preferred_element_type=f32
            )
            heads_tile = tile // head_width
            weight = per_head(grown, j * heads_tile, heads_tile, head_width, tile)
            state[:, cols] = state[:, cols] * weight + add

    state[...] = jnp.zeros_like(state)
    last = chunks - 1
    project_chunk(last)
    tail_rows = raw.at[rows - 8 :, :]

    def to_next():
        return remote(tail_rows, halo, halo_send, halo_recv, at_seq(jnp.minimum(seq + 1, seq_count - 1)))

    @pl.when(seq < seq_count - 1)
    def _():
        to_next().start()

    @pl.when(seq == 0)
    def _():
        halo[...] = jnp.zeros_like(halo)

    def step_chunk(c, _):
        project_chunk(c)

        @pl.when((c == 0) & (seq > 0))
        def _():
            remote(tail_rows, halo, halo_send, halo_recv, at_seq(jnp.maximum(seq - 1, 0))).wait_recv()

        mix_chunk(c)
        return 0

    lax.fori_loop(0, last, step_chunk, 0)
    mix_chunk(last)

    def share_of(o):
        return pl.ds(pl.multiple_of(o * share, share), share)

    total_end = ends[0]
    for c in range(1, chunks):
        total_end = total_end + ends[c]
    decay_out[...] = jnp.concatenate(
        [total_end, jnp.zeros((8, 128 - heads), f32)], axis=1
    )
    state_out[...] = state[...].astype(bf16)

    def decay_copy(o):
        return remote(decay_out, decay_in.at[seq], decay_send.at[o], decay_recv.at[seq], at_seq(o))

    def state_copy(o):
        return remote(state_out.at[share_of(o)], owned.at[seq], state_send.at[o], state_recv.at[seq], at_seq(o))

    def back_copy(i):
        return remote(prefixes.at[i], carried.at[share_of(seq)], back_send.at[i], back_recv.at[seq], at_seq(i))

    for step in range(1, seq_count):
        o = (seq + step) % seq_count

        @pl.when(seq < seq_count - 1)
        def _():
            decay_copy(o).start()
            state_copy(o).start()

    @pl.when(seq < seq_count - 1)
    def _():
        decay_in[seq] = decay_out[...]
        owned[seq] = state_out[share_of(seq), :]

    def inside(c, _):
        at = chunk_of(c)
        cum = cum_ref[at, :]
        eye = (t_row == s_col).astype(f32)
        flip = (((0,), (0,)), ((), ()))
        cum_t = lax.dot_general(cum, eye, flip, preferred_element_type=f32, precision=HIGHEST)
        step_t = lax.dot_general(step_ref[at, :], eye, flip, preferred_element_type=f32, precision=HIGHEST)
        readout = bc_ref[at, states:]
        scores = lax.dot_general(
            readout, bc_ref[at, :states], (((1,), (1,)), ((), ())), preferred_element_type=f32
        )
        scores = jnp.where(causal, scores, 0.0)
        grown = jnp.exp(cum)
        lane = lax.broadcasted_iota(jnp.int32, (ROWS, 128), 1)
        for p in range(spans):
            span = slice(p * 128, (p + 1) * 128)
            x = x_ref[at, span]
            mixes, parts = [], []
            for k in range(per_span):
                h = p * per_span + k
                gaps = jnp.minimum(cum[:, h : h + 1] - cum_t[h : h + 1, :], 0.0)
                mixes.append((scores * jnp.exp(gaps) * step_t[h : h + 1, :]).astype(bf16))
                own = (lane >= k * head_width) & (lane < (k + 1) * head_width)
                parts.append(jnp.where(own, x, jnp.zeros_like(x)))
            total = jnp.dot(
                jnp.concatenate(mixes, axis=1), jnp.concatenate(parts, axis=0), preferred_element_type=f32
            )
            reads = jnp.dot(readout, starts[c, :, span], preferred_element_type=f32)
            weight = per_head(grown, p * per_span, per_span, head_width, 128)
            direct = per_head(skip[...], p * per_span, per_span, head_width, 128)
            y_ref[at, span] = total + reads * weight + direct * x.astype(f32)
        return 0

    lax.fori_loop(0, chunks, inside, 0)

    for j in range(seq_count - 1):

        @pl.when(seq != j)
        def _():
            remote(decay_out, decay_in.at[j], decay_send.at[j], decay_recv.at[j], at_seq(j)).wait_recv()
            remote(
                state_out.at[share_of(j)], owned.at[j], state_send.at[j], state_recv.at[j], at_seq(j)
            ).wait_recv()

    for p in range(tiles):
        cols = slice(p * tile, (p + 1) * tile)
        heads_tile = tile // head_width
        run = owned[0, :, cols].astype(f32)
        prefixes[0, :, cols] = jnp.zeros((share, tile), bf16)
        prefixes[1, :, cols] = run.astype(bf16)
        for i in range(2, seq_count):
            grown = jnp.exp(decay_in[i - 1][:1, :])
            run = run * per_head(grown, p * heads_tile, heads_tile, head_width, tile) + owned[i - 1, :, cols].astype(f32)
            prefixes[i, :, cols] = run.astype(bf16)
    for i in range(seq_count - 1, 0, -1):

        @pl.when(seq != i)
        def _():
            back_copy(i).start()

    carried[share_of(seq), :] = prefixes[seq]

    loads[13].wait()

    def gate_tile(j, _):
        cols = tile_of(j, tile)
        value = jnp.dot(full[0], gate_w[:half, cols], preferred_element_type=f32)
        value = value + jnp.dot(full[1], gate_w[half:, cols], preferred_element_type=f32)
        gate_ref[:, cols] = silu(rounded(value))
        return 0

    lax.fori_loop(0, tiles, gate_tile, 0)
    loads[14].wait()

    @pl.when(seq == 0)
    def _():
        carried[...] = jnp.zeros_like(carried)

    for o in range(seq_count):

        @pl.when((seq > 0) & (seq != o))
        def _():
            remote(
                prefixes.at[o], carried.at[share_of(o)], back_send.at[o], back_recv.at[o], at_seq(o)
            ).wait_recv()

    def gate_block(b):
        at = chunk_of(b)
        offset = jnp.zeros_like(ends[0])
        for c in range(chunks - 1):
            offset = offset + jnp.where(b > c, ends[c], jnp.zeros_like(ends[c]))
        grown = jnp.exp(cum_ref[at, :] + offset[:1, :])
        readout = bc_ref[at, states:]
        squares = jnp.zeros((ROWS, 128), f32)
        for p in range(spans):
            span = slice(p * 128, (p + 1) * 128)
            reads = jnp.dot(readout, carried[:, span], preferred_element_type=f32)
            weight = per_head(grown, p * per_span, per_span, head_width, 128)
            g = (y_ref[at, span] + reads * weight) * gate_ref[at, span]
            squares = squares + g * g
            gated[at, span] = (g * gain[:, span]).astype(bf16)
        square_out[b] = lax.dot_general(
            jnp.ones((8, 128), f32), squares, (((1,), (1,)), ((), ())),
            preferred_element_type=f32, precision=HIGHEST,
        )

    def square_copy(b):
        return remote(square_out.at[b], square_in.at[tp], sq_send.at[b], sq_recv.at[tp], at_tp(b))

    far_first = (1 - chip) * 2

    def gate_far(k, _):
        gate_block(far_first + k)
        return 0

    lax.fori_loop(0, 2, gate_far, 0)
    diagonal = (1 - chip) * 2 + 1 - core
    square_copy(across).start()
    square_copy(diagonal).start()

    def near_copy(p):
        return remote(near_out.at[p], near_in.at[p], near_send.at[p], near_recv.at[p], at_tp(mate))

    def far_copy(p):
        return remote(far_out.at[p], far_in.at[p], far_send.at[p], far_recv.at[p], at_tp(across))

    def own_copy(p):
        return remote(own_out.at[p], own_in.at[p], own_send.at[p], own_recv.at[p], at_tp(mate))

    def pass_on(p):
        near_copy(p).wait_recv()
        far_out[p] = (far_acc[p] + near_in[p].astype(f32)).astype(bf16)
        far_copy(p).start()

    def far_piece(p, _):
        cols = tile_of(p, piece)
        near_out[p] = jnp.dot(gated[chunk_of(diagonal), :], out_w[:, cols], preferred_element_type=f32).astype(bf16)
        near_copy(p).start()
        far_acc[p] = jnp.dot(gated[chunk_of(across), :], out_w[:, cols], preferred_element_type=f32)

        @pl.when(p > 0)
        def _():
            pass_on(jnp.maximum(p - 1, 0))

        return 0

    lax.fori_loop(0, PIECES, far_piece, 0)
    pass_on(PIECES - 1)

    def gate_near(k, _):
        gate_block(chip * 2 + k)
        return 0

    lax.fori_loop(0, 2, gate_near, 0)
    square_copy(mate).start()

    def own_piece(p, _):
        cols = tile_of(p, piece)
        own_out[p] = jnp.dot(gated[chunk_of(mate), :], out_w[:, cols], preferred_element_type=f32).astype(bf16)
        own_copy(p).start()
        own_acc[p] = jnp.dot(gated[chunk_of(tp), :], out_w[:, cols], preferred_element_type=f32)
        return 0

    lax.fori_loop(0, PIECES, own_piece, 0)

    square = square_out[tp]
    for step in range(1, tp_count):
        source = (tp + step) % tp_count
        remote(square_out.at[0], square_in.at[source], sq_send.at[0], sq_recv.at[source], at_tp(source)).wait_recv()
        square = square + square_in[source]
    mean = square[:1, :] / (channels * tp_count)
    spread = jnp.broadcast_to(lax.rsqrt(mean + 1e-05), (ROWS, ROWS))
    scale = jnp.sum(jnp.where(t_row == s_col, spread, 0.0), axis=1, keepdims=True)

    def out_copy(p):
        cols = tile_of(p, piece)
        return pltpu.make_async_copy(result.at[:, cols], out_ref.at[:, cols], out_sem.at[p])

    def finish(p, _):
        own_copy(p).wait_recv()
        far_copy(p).wait_recv()
        total = own_acc[p] + own_in[p].astype(f32) + far_in[p].astype(f32)
        result[:, tile_of(p, piece)] = (total * scale).astype(bf16)
        out_copy(p).start()
        return 0

    lax.fori_loop(0, PIECES, finish, 0)

    for c in range(chunks):
        crossing(c).wait_send()
        beside(c).wait_send()
        forwarded(c).wait_send()

    @pl.when(seq < seq_count - 1)
    def _():
        to_next().wait_send()

    for o in range(seq_count):

        @pl.when((seq < seq_count - 1) & (seq != o))
        def _():
            decay_copy(o).wait_send()
            state_copy(o).wait_send()

        if o > 0:

            @pl.when(seq != o)
            def _():
                back_copy(o).wait_send()

    for b in (across, diagonal, mate):
        square_copy(b).wait_send()
    for p in range(PIECES):
        near_copy(p).wait_send()
        far_copy(p).wait_send()
        own_copy(p).wait_send()
        out_copy(p).wait()


def fused(
    tokens, gate_weight, inner_weight, state_weight, step_weight, conv_inner, conv_state,
    step_bias, decay_rate, skip_gain, norm_gain, out_weight,
):
    rows, width = tokens.shape
    channels = inner_weight.shape[1]
    heads = step_weight.shape[1]
    head_width = channels // heads
    states = state_weight.shape[1] // 2
    depth, out_width = inner_weight.shape[0], out_weight.shape[1]
    seq_count, tp_count = lax.axis_size("seq"), lax.axis_size("tp")
    chunks = rows // ROWS
    share = states // seq_count
    piece = out_width // PIECES
    f32, bf16 = jnp.float32, jnp.bfloat16
    dma, vmem = pltpu.SemaphoreType.DMA, pltpu.VMEM
    args = (
        tokens, gate_weight, inner_weight, state_weight, step_weight, conv_inner, conv_state,
        step_bias[None, :], decay_rate[None, :], skip_gain[None, :], norm_gain[None, :], out_weight,
    )
    scratch = [
        vmem((2, rows, 2 * width), bf16),
        vmem((depth, channels), bf16),
        vmem((depth, channels), bf16),
        vmem((depth, 2 * states), bf16),
        vmem((depth, heads), bf16),
        vmem(conv_inner.shape, f32),
        vmem(conv_state.shape, f32),
        vmem((1, heads), f32),
        vmem((1, heads), f32),
        vmem((1, heads), f32),
        vmem((1, channels), f32),
        vmem((channels, out_width), bf16),
        vmem((rows, channels + 2 * states), f32),
        vmem((8, channels + 2 * states), f32),
        vmem((rows, heads), f32),
        vmem((rows, channels), bf16),
        vmem((rows, 2 * states), bf16),
        vmem((rows, channels), f32),
        vmem((rows, channels), f32),
        vmem((rows, channels), bf16),
        vmem((ROWS, channels), bf16),
        vmem((rows, heads), f32),
        vmem((rows, heads), f32),
        vmem((chunks, 8, heads), f32),
        vmem((states, channels), f32),
        vmem((chunks, states, channels), bf16),
        vmem((states, channels), bf16),
        vmem((seq_count, share, channels), bf16),
        vmem((seq_count, share, channels), bf16),
        vmem((states, channels), bf16),
        vmem((8, 128), f32),
        vmem((seq_count, 8, 128), f32),
        vmem((tp_count, 8, ROWS), f32),
        vmem((tp_count, 8, ROWS), f32),
    ]
    half_sums = vmem((PIECES, ROWS, piece), bf16)
    whole_sums = vmem((PIECES, ROWS, piece), f32)
    scratch += [half_sums, half_sums, whole_sums, half_sums, half_sums, half_sums, half_sums, whole_sums]
    scratch += [vmem((ROWS, out_width), bf16)]
    scratch += [dma((15,))] + [dma((chunks,))] * 6 + [dma, dma] + [dma((seq_count,))] * 6
    scratch += [dma((tp_count,))] * 2 + [dma((PIECES,))] * 7
    anywhere = pl.BlockSpec(memory_space=pl.ANY)
    return pl.pallas_call(
        lambda *refs: layer_kernel(head_width, *refs),
        out_shape=jax.ShapeDtypeStruct((rows // tp_count, out_width), bf16),
        in_specs=[anywhere] * len(args),
        out_specs=anywhere,
        scratch_shapes=scratch,
        compiler_params=pltpu.CompilerParams(
            collective_id=0, has_side_effects=True, vmem_limit_bytes=60 * 1024 * 1024
        ),
        name="layer",
    )(*args)


def on_device(
    tokens,
    gate_weight,
    inner_weight,
    state_weight,
    step_weight,
    conv_inner,
    conv_state,
    step_bias,
    decay_rate,
    skip_gain,
    norm_gain,
    out_weight,
):
    tok_rows = tokens.shape[0]
    width_inner = inner_weight.shape[1]
    head_count = step_weight.shape[1]
    head_width = width_inner // head_count
    state_size = state_weight.shape[1] // 2
    blocks = tok_rows // GROUP
    size_tp = lax.axis_size("tp")
    me = lax.axis_index("tp")

    chunks = [None] * blocks
    for b in range(blocks - 1, -1, -1):
        chunks[b] = gather_features(tokens[b * GROUP : (b + 1) * GROUP])
    halo = shifted(chunks[-1][GROUP - HALO :], 1)
    chunks[0] = jnp.concatenate([halo, chunks[0]], axis=0)

    inner_raw, state_raw, step_raw = [None] * blocks, [None] * blocks, [None] * blocks
    for b in range(blocks - 1, -1, -1):
        i_b, s_b, t_b = project(chunks[b], inner_weight, state_weight, step_weight)
        inner_raw[b], state_raw[b] = i_b.astype(jnp.bfloat16), s_b.astype(jnp.bfloat16)
        step_raw[b] = t_b[HALO:] if b == 0 else t_b

    lanes = max(128, head_width)
    time_step = jax.nn.softplus(jnp.concatenate(step_raw, axis=0) + step_bias[None, :])
    log_decay = -time_step * decay_rate[None, :]
    grouped = log_decay.reshape(blocks, GROUP, head_count)
    cumulative = jnp.cumsum(grouped, axis=1)
    ending = cumulative[:, -1]
    tail = (jnp.exp(ending[:, None] - cumulative)).reshape(tok_rows, head_count) * time_step
    cumulative = cumulative.reshape(tok_rows, head_count)

    def cost(flops, count, exps):
        return pl.CostEstimate(flops=flops, bytes_accessed=count, transcendentals=exps)

    whole = tok_rows * width_inner
    x, bc, contribution = pl.pallas_call(
        lambda *refs: conv_kernel(blocks, head_width, lanes, *refs),
        out_shape=(
            jax.ShapeDtypeStruct((tok_rows, width_inner), jnp.bfloat16),
            jax.ShapeDtypeStruct((tok_rows, 2 * state_size), jnp.bfloat16),
            jax.ShapeDtypeStruct((blocks, width_inner, state_size), jnp.float32),
        ),
        cost_estimate=cost(2 * whole * state_size, 6 * whole, whole),
        name="conv",
    )(*inner_raw, *state_raw, conv_inner, conv_state, tail)
    contribution = contribution.reshape(blocks, head_count, head_width, state_size)
    local_state = jnp.zeros((head_count, head_width, state_size), jnp.float32)
    for b in range(blocks):
        local_state = jnp.exp(ending[b])[:, None, None] * local_state + contribution[b]

    def by_rows(width):
        return pl.BlockSpec((GROUP, width), lambda b: (b, 0))

    def by_columns(height):
        return pl.BlockSpec((height, GROUP), lambda b: (0, b))

    def fixed(width):
        return pl.BlockSpec((1, width), lambda b: (0, 0))

    intra = pl.pallas_call(
        lambda *refs: intra_kernel(head_width, lanes, *refs),
        grid=(blocks,),
        in_specs=[
            by_rows(width_inner),
            by_rows(2 * state_size),
            by_rows(head_count),
            by_columns(head_count),
            by_columns(head_count),
            fixed(width_inner),
        ],
        out_specs=by_rows(width_inner),
        out_shape=jax.ShapeDtypeStruct((tok_rows, width_inner), jnp.float32),
        cost_estimate=cost(4 * whole * GROUP, 6 * whole, GROUP * tok_rows * head_count),
        name="intra",
    )(x, bc, cumulative, cumulative.T, time_step.T, jnp.repeat(skip_gain, head_width)[None, :])

    gate = jnp.concatenate(
        [
            jnp.dot(c[c.shape[0] - GROUP :], gate_weight, preferred_element_type=jnp.float32).astype(jnp.bfloat16)
            for c in chunks
        ],
        axis=0,
    )

    carried, intra = earlier_state(
        local_state.astype(jnp.bfloat16).reshape(width_inner, state_size),
        jnp.sum(ending, axis=0),
        head_width,
        intra,
    )
    carried = carried.astype(jnp.float32).reshape(head_count, head_width, state_size)
    states = []
    for b in range(blocks):
        states.append(carried.astype(jnp.bfloat16).reshape(1, width_inner, state_size))
        carried = jnp.exp(ending[b])[:, None, None] * carried + contribution[b]

    gated, squares = pl.pallas_call(
        lambda *refs: gate_kernel(head_width, lanes, *refs),
        grid=(blocks,),
        in_specs=[
            by_rows(width_inner),
            by_rows(2 * state_size),
            by_rows(head_count),
            by_rows(width_inner),
            fixed(width_inner),
            pl.BlockSpec((1, width_inner, state_size), lambda b: (b, 0, 0)),
        ],
        out_specs=(by_rows(width_inner), by_rows(1)),
        out_shape=(
            jax.ShapeDtypeStruct((tok_rows, width_inner), jnp.bfloat16),
            jax.ShapeDtypeStruct((tok_rows, 1), jnp.float32),
        ),
        cost_estimate=cost(2 * whole * state_size, 8 * whole, whole),
        name="gate",
    )(intra, bc, cumulative, gate, norm_gain[None, :], jnp.concatenate(states, axis=0))

    square_total = sum_over_tp(squares[:, 0])
    share = tok_rows // size_tp
    mean_square = lax.dynamic_slice(square_total, (me * share,), (share,)) / (width_inner * size_tp)
    scale = lax.rsqrt(mean_square + 1e-05)[:, None]

    if size_tp != 4:
        part = jnp.dot(gated, out_weight, preferred_element_type=jnp.float32).astype(jnp.bfloat16)
        total = lax.psum_scatter(part, "tp", scatter_dimension=0, tiled=True)
        return (total.astype(jnp.float32) * scale).astype(jnp.bfloat16)

    side = me // 2

    def reduced(chip, weight):
        rows = lax.dynamic_slice(gated, (chip * 2 * share, 0), (2 * share, width_inner))
        both = jnp.dot(rows, weight, preferred_element_type=jnp.float32).astype(jnp.bfloat16)
        shape = (share, weight.shape[1])
        away = lax.dynamic_slice(both, ((1 - me % 2) * share, 0), shape)
        own = lax.dynamic_slice(both, ((me % 2) * share, 0), shape)
        return own.astype(jnp.float32) + swapped(away, 1).astype(jnp.float32)

    cuts = 2
    width_out = out_weight.shape[1] // cuts
    weights = [out_weight[:, c * width_out : (c + 1) * width_out] for c in range(cuts)]
    arrived = [swapped(reduced(side ^ 1, w).astype(jnp.bfloat16), 2) for w in weights]
    results = []
    for w, other in zip(weights, arrived):
        total = reduced(side, w) + other.astype(jnp.float32)
        results.append((total * scale).astype(jnp.bfloat16))
    return jnp.concatenate(results, axis=1)


def solution(mesh):
    in_specs = (
        P("seq", "tp"),
        P(None, "tp"),
        P(None, "tp"),
        P(),
        P(None, "tp"),
        P(None, "tp"),
        P(),
        P("tp"),
        P("tp"),
        P("tp"),
        P("tp"),
        P("tp", None),
    )
    out_specs = P(("seq", "tp"), None)
    quick = mesh.shape["tp"] == 4 and mesh.shape["seq"] == 8
    return jax.shard_map(
        fused if quick else on_device, mesh=mesh, in_specs=in_specs, out_specs=out_specs, check_vma=False
    )
```

```python
import jax
import jax.numpy as jnp
from jax import lax
from jax.experimental import pallas as pl
from jax.experimental.pallas import tpu as pltpu
from jax.sharding import PartitionSpec as P

GROUP = 256
HALO = 16


def swapped(shard, by):
    size = lax.axis_size("tp")
    return lax.ppermute(shard, "tp", [(i, i ^ by) for i in range(size)])


def shifted(shard, by):
    size = lax.axis_size("seq")
    return lax.ppermute(shard, "seq", [(i, i + by) for i in range(size - by)])


def gather_features(rows):
    size = lax.axis_size("tp")
    me = lax.axis_index("tp")
    width = rows.shape[1]
    held = [(0, rows)]
    step = size // 2
    while step >= 1:
        held = held + [(code ^ step, swapped(part, step)) for code, part in held]
        step //= 2
    parts = dict(held)
    full = jnp.zeros((rows.shape[0], width * size), rows.dtype)
    for code in range(size):
        full = lax.dynamic_update_slice(full, parts[code], (0, (me ^ code) * width))
    return full


def sum_over_tp(part):
    size = lax.axis_size("tp")
    step = 1
    while step < size:
        part = part + swapped(part, step)
        step *= 2
    return part


def prefix_kernel(mine_ref, decay_ref, owner_ref, out_ref):
    owner = owner_ref[...]
    carried = jnp.zeros(mine_ref.shape[1:], jnp.float32)
    for i in range(mine_ref.shape[0]):
        out_ref[i] = carried.astype(jnp.bfloat16)
        log_row = jnp.sum(owner * decay_ref[i : i + 1, :], axis=1, keepdims=True)
        carried = carried * jnp.exp(log_row) + mine_ref[i].astype(jnp.float32)


def earlier_state(local_state, decay_total, head_width, cover):
    size = lax.axis_size("seq")
    rows, states = local_state.shape
    share = rows // size
    me = lax.axis_index("seq")
    heads = decay_total.shape[0]
    wide = jnp.pad(decay_total, (0, -heads % 128))
    wide = jnp.broadcast_to(wide[None, None, :], (size, 1, wide.shape[0]))
    decay_all = lax.all_to_all(wide, "seq", 0, 0, tiled=True)[:, 0, :heads]
    blocks = local_state.reshape(size, share, states)
    blocks, decay_all = lax.optimization_barrier((blocks, decay_all))
    mine = lax.all_to_all(blocks, "seq", 0, 0, tiled=True)
    mine, cover = lax.optimization_barrier((mine, cover))
    row_head = (me * share + jnp.arange(share)) // head_width
    owner = (row_head[:, None] == jnp.arange(decay_total.shape[0])[None, :]).astype(jnp.float32)
    prefixes = pl.pallas_call(
        prefix_kernel,
        out_shape=jax.ShapeDtypeStruct(mine.shape, jnp.bfloat16),
        cost_estimate=pl.CostEstimate(flops=0, bytes_accessed=4 * mine.size, transcendentals=0),
    )(mine, decay_all, owner)
    return lax.all_to_all(prefixes, "seq", 0, 0, tiled=True).reshape(rows, states), cover


def per_head(table, first, count, width, lanes):
    lane = lax.broadcasted_iota(jnp.int32, (table.shape[0], lanes), 1)
    spread = jnp.broadcast_to(table[:, first : first + 1], (table.shape[0], lanes))
    for k in range(1, count):
        spread = jnp.where(lane >= k * width, table[:, first + k : first + k + 1], spread)
    return spread


def silu(value):
    return value * (0.5 * jnp.tanh(0.5 * value) + 0.5)


def conv_kernel(blocks, head_width, lanes, *refs):
    inner_refs, state_refs = refs[:blocks], refs[blocks : 2 * blocks]
    tap_inner, tap_state, tail_ref = refs[2 * blocks : 2 * blocks + 3]
    x_ref, bc_ref, contribution_ref = refs[2 * blocks + 3 :]
    taps = tap_inner.shape[0]
    heads_per = lanes // head_width

    def mixed(chunk_refs, b, span, kernel):
        if b == 0:
            padded = chunk_refs[0][:, span].astype(jnp.float32)
        else:
            last = chunk_refs[b - 1].shape[0] - HALO
            edge = chunk_refs[b - 1][last:, span].astype(jnp.float32)
            padded = jnp.concatenate([edge, chunk_refs[b][:, span].astype(jnp.float32)], axis=0)
        total = padded * kernel[taps - 1 : taps]
        for tap in range(taps - 1):
            total = total + pltpu.roll(padded, taps - 1 - tap, 0) * kernel[tap : tap + 1]
        return silu(total[HALO:]).astype(jnp.bfloat16)

    for b in range(blocks):
        rows = slice(b * GROUP, (b + 1) * GROUP)
        bc = mixed(state_refs, b, slice(None), tap_state[...])
        bc_ref[rows] = bc
        inject = bc[:, : bc.shape[1] // 2]
        tail = tail_ref[rows]
        for p in range(x_ref.shape[1] // lanes):
            span = slice(p * lanes, (p + 1) * lanes)
            x = mixed(inner_refs, b, span, tap_inner[:, span])
            x_ref[rows, span] = x
            weight = per_head(tail, p * heads_per, heads_per, head_width, lanes)
            scaled = (x.astype(jnp.float32) * weight).astype(jnp.bfloat16)
            contribution_ref[b, span] = lax.dot_general(
                scaled, inject, (((0,), (0,)), ((), ())), preferred_element_type=jnp.float32
            )


def intra_kernel(head_width, lanes, x_ref, bc_ref, cum_ref, cum_t_ref, step_t_ref, skip_ref, out_ref):
    states = bc_ref.shape[1] // 2
    heads_per = lanes // head_width
    scores = lax.dot_general(
        bc_ref[:, states:], bc_ref[:, :states], (((1,), (1,)), ((), ())),
        preferred_element_type=jnp.float32,
    )
    t = lax.broadcasted_iota(jnp.int32, scores.shape, 0)
    s = lax.broadcasted_iota(jnp.int32, scores.shape, 1)
    scores = jnp.where(s <= t, scores, 0.0)
    lane = lax.broadcasted_iota(jnp.int32, (x_ref.shape[0], lanes), 1)
    for p in range(x_ref.shape[1] // lanes):
        span = slice(p * lanes, (p + 1) * lanes)
        x = x_ref[:, span]
        total = None
        for k in range(heads_per):
            h = p * heads_per + k
            gaps = jnp.minimum(cum_ref[:, h : h + 1] - cum_t_ref[h : h + 1, :], 0.0)
            mixing = (scores * jnp.exp(gaps) * step_t_ref[h : h + 1, :]).astype(jnp.bfloat16)
            part = jnp.dot(mixing, x, preferred_element_type=jnp.float32)
            total = part if k == 0 else jnp.where(lane >= k * head_width, part, total)
        out_ref[:, span] = total + skip_ref[:, span] * x.astype(jnp.float32)


def gate_kernel(head_width, lanes, intra_ref, bc_ref, cum_ref, gate_ref, gain_ref, state_ref, out_ref, square_ref):
    states = bc_ref.shape[1] // 2
    heads_per = lanes // head_width
    readout = bc_ref[:, states:]
    grown = jnp.exp(cum_ref[...])
    squares = jnp.zeros((readout.shape[0], lanes), jnp.float32)
    for p in range(intra_ref.shape[1] // lanes):
        span = slice(p * lanes, (p + 1) * lanes)
        reads = lax.dot_general(
            readout, state_ref[0, span], (((1,), (1,)), ((), ())), preferred_element_type=jnp.float32
        )
        weight = per_head(grown, p * heads_per, heads_per, head_width, lanes)
        g = (intra_ref[:, span] + reads * weight) * silu(gate_ref[:, span].astype(jnp.float32))
        squares = squares + g * g
        out_ref[:, span] = (g * gain_ref[:, span]).astype(jnp.bfloat16)
    square_ref[...] = jnp.sum(squares, axis=1, keepdims=True)


def project(rows, *weights):
    return [jnp.dot(rows, weight, preferred_element_type=jnp.float32) for weight in weights]


ROWS = 128
PIECES = 10
VMEM_LIMIT = 56 * 1024 * 1024
MESH = pl.DeviceIdType.MESH
HIGHEST = lax.Precision.HIGHEST


def softplus(value):
    return jnp.maximum(value, 0.0) + jnp.log1p(jnp.exp(-jnp.abs(value)))


def chunk_of(index):
    return pl.ds(pl.multiple_of(index * ROWS, ROWS), ROWS)


def tile_of(index, width):
    return pl.ds(pl.multiple_of(index * width, width), width)


def layer_kernel(
    head_width,
    tok_in, gate_in, inner_in, statew_in, stepw_in, convi_in, convs_in, bias_in, rate_in, skip_in, gain_in, outw_in,
    out_ref,
    full, gate_w, inner_w, state_w, step_w, conv_i, conv_s, bias, rate, skip, gain, out_w,
    raw, halo, step_acc, x_ref, bc_ref, y_ref, gate_ref, gated, scaled,
    cum_ref, step_ref, ends, state, starts, state_out, owned, prefixes, carried, decay_out, decay_in,
    square_out, square_in, near_out, near_in, far_acc, far_out, far_in, own_out, own_in, own_acc, both,
    local_sem, x_send, x_recv, d_send, d_recv, f_send, f_recv, halo_send, halo_recv,
    state_send, state_recv, decay_send, decay_recv, back_send, back_recv,
    sq_send, sq_recv, near_send, near_recv, far_send, far_recv, own_send, own_recv,
):
    seq_count, tp_count = lax.axis_size("seq"), lax.axis_size("tp")
    seq, tp = lax.axis_index("seq"), lax.axis_index("tp")
    chip, core = tp // 2, tp % 2
    mate, across = chip * 2 + 1 - core, (1 - chip) * 2 + core
    rows, half = full.shape[1], full.shape[2]
    width = half // 2
    channels = inner_w.shape[1]
    states = state_w.shape[1] // 2
    heads = step_w.shape[0]
    chunks = rows // ROWS
    tile = min(256, channels)
    tiles = channels // tile
    spans = channels // 128
    per_span = 128 // head_width
    share = states // seq_count
    piece = out_w.shape[1] // PIECES
    f32, bf16 = jnp.float32, jnp.bfloat16
    across_rows = (((1,), (1,)), ((), ()))

    def at_tp(index):
        return {"seq": seq, "tp": index}

    def at_seq(index):
        return {"seq": index, "tp": tp}

    def remote(src, dst, send, recv, device):
        return pltpu.make_async_remote_copy(
            src_ref=src, dst_ref=dst, send_sem=send, recv_sem=recv, device_id=device, device_id_type=MESH
        )

    barrier = pltpu.get_barrier_semaphore()
    for step in range(1, tp_count):
        pl.semaphore_signal(barrier, inc=1, device_id=at_tp((tp + step) % tp_count), device_id_type=MESH)
    for step in range(1, seq_count):
        pl.semaphore_signal(barrier, inc=1, device_id=at_seq((seq + step) % seq_count), device_id_type=MESH)

    mine = pl.ds(pl.multiple_of(core * width, width), width)
    theirs = pl.ds(pl.multiple_of((1 - core) * width, width), width)
    near_rows = pl.ds(pl.multiple_of(chip * half, half), half)
    far_rows = pl.ds(pl.multiple_of((1 - chip) * half, half), half)
    loads = [
        (tok_in, full.at[chip, :, mine]),
        (inner_in.at[near_rows], inner_w.at[near_rows]),
        (statew_in.at[near_rows], state_w.at[near_rows]),
        (stepw_in.at[:, near_rows], step_w.at[:, near_rows]),
        (inner_in.at[far_rows], inner_w.at[far_rows]),
        (statew_in.at[far_rows], state_w.at[far_rows]),
        (stepw_in.at[:, far_rows], step_w.at[:, far_rows]),
        (convi_in, conv_i),
        (convs_in, conv_s),
        (bias_in, bias),
        (rate_in, rate),
        (skip_in, skip),
        (gain_in, gain),
        (gate_in, gate_w),
        (outw_in, out_w),
    ]
    loads = [pltpu.make_async_copy(src, dst, local_sem.at[i]) for i, (src, dst) in enumerate(loads)]
    for load in loads:
        load.start()
    loads[0].wait()
    pl.semaphore_wait(barrier, tp_count - 1 + seq_count - 1)

    def crossing(c):
        part = full.at[chip, chunk_of(c), mine]
        return remote(part, part, x_send.at[c], x_recv.at[c], at_tp(across))

    def beside(c):
        part = full.at[chip, chunk_of(c), mine]
        return remote(part, part, d_send.at[c], d_recv.at[c], at_tp(mate))

    def forwarded(c):
        part = full.at[1 - chip, chunk_of(c), mine]
        return remote(part, part, f_send.at[c], f_recv.at[c], at_tp(mate))

    def arrived(side, columns, c, send, recv):
        part = full.at[side, chunk_of(c), columns]
        return remote(part, part, send.at[c], recv.at[c], at_tp(mate))

    order = [chunks - 1] + list(range(chunks - 1))
    for c in order:
        crossing(c).start()
        beside(c).start()

    for load in loads[1:4]:
        load.wait()
    for c in order:
        arrived(chip, theirs, c, d_send, d_recv).wait_recv()

    near = full.at[chip]

    def first(j, _):
        cols = tile_of(j, tile)
        raw[:, cols] = jnp.dot(near[...], inner_w[near_rows, cols], preferred_element_type=f32)
        return 0

    lax.fori_loop(0, tiles, first, 0)
    raw[:, channels:] = jnp.dot(near[...], state_w[near_rows, :], preferred_element_type=f32)
    step_acc[...] = lax.dot_general(near[...], step_w[:, near_rows], across_rows, preferred_element_type=f32)
    for load in loads[4:13]:
        load.wait()

    def rounded(value):
        return value.astype(bf16).astype(f32)

    def project_chunk(c):
        arrived(1 - chip, mine, c, x_send, x_recv).wait_recv()
        forwarded(c).start()
        arrived(1 - chip, theirs, c, f_send, f_recv).wait_recv()
        at = chunk_of(c)

        def second(j, _):
            cols = tile_of(j, tile)
            more = jnp.dot(full[1 - chip, at, :], inner_w[far_rows, cols], preferred_element_type=f32)
            raw[at, cols] = rounded(raw[at, cols] + more)
            return 0

        lax.fori_loop(0, tiles, second, 0)
        more = jnp.dot(full[1 - chip, at, :], state_w[far_rows, :], preferred_element_type=f32)
        raw[at, channels:] = rounded(raw[at, channels:] + more)
        more = lax.dot_general(
            full[1 - chip, at, :], step_w[:, far_rows], across_rows, preferred_element_type=f32
        )
        step_acc[at, :] += more

    t_row = lax.broadcasted_iota(jnp.int32, (ROWS, ROWS), 0)
    s_col = lax.broadcasted_iota(jnp.int32, (ROWS, ROWS), 1)
    causal = s_col <= t_row

    def mix_chunk(c):
        at = chunk_of(c)
        time_step = softplus(step_acc[at, :] + bias[...])
        decay = -time_step * rate[...]
        cum = jnp.dot(causal.astype(f32), decay, preferred_element_type=f32, precision=HIGHEST)
        ending = cum[ROWS - 1 :, :]
        tail = jnp.exp(ending - cum) * time_step
        cum_ref[at, :] = cum
        step_ref[at, :] = time_step
        ends[c] = jnp.broadcast_to(ending, ends.shape[1:])
        before = pl.ds(pl.multiple_of(jnp.maximum(c * ROWS - 8, 0), 8), 8)

        def conv(span, kernel):
            edge = jnp.where(c == 0, halo[:, span], raw[before, span])
            padded = jnp.concatenate([edge, raw[at, span]], axis=0)
            taps = kernel.shape[0]
            total = padded * kernel[taps - 1 : taps]
            for tap in range(taps - 1):
                total = total + pltpu.roll(padded, taps - 1 - tap, 0) * kernel[tap : tap + 1]
            return silu(total[8:]).astype(bf16)

        for p in range(2 * states // 128):
            span = slice(p * 128, (p + 1) * 128)
            bc_ref[at, span] = conv(slice(channels + p * 128, channels + (p + 1) * 128), conv_s[:, span])
        for p in range(spans):
            span = slice(p * 128, (p + 1) * 128)
            x = conv(span, conv_i[:, span])
            x_ref[at, span] = x
            weight = per_head(tail, p * per_span, per_span, head_width, 128)
            scaled[:, span] = (x.astype(f32) * weight).astype(bf16)
        starts[c] = state[...].astype(bf16)
        inject = bc_ref[at, :states]
        grown = jnp.exp(ending)
        for j in range(tiles):
            cols = slice(j * tile, (j + 1) * tile)
            add = lax.dot_general(
                inject, scaled[:, cols], (((0,), (0,)), ((), ())), preferred_element_type=f32
            )
            heads_tile = tile // head_width
            weight = per_head(grown, j * heads_tile, heads_tile, head_width, tile)
            state[:, cols] = state[:, cols] * weight + add

    state[...] = jnp.zeros_like(state)
    last = chunks - 1
    project_chunk(last)
    tail_rows = raw.at[rows - 8 :, :]

    def to_next():
        return remote(tail_rows, halo, halo_send, halo_recv, at_seq(jnp.minimum(seq + 1, seq_count - 1)))

    @pl.when(seq < seq_count - 1)
    def _():
        to_next().start()

    @pl.when(seq == 0)
    def _():
        halo[...] = jnp.zeros_like(halo)

    def step_chunk(c, _):
        project_chunk(c)

        @pl.when((c == 0) & (seq > 0))
        def _():
            remote(tail_rows, halo, halo_send, halo_recv, at_seq(jnp.maximum(seq - 1, 0))).wait_recv()

        mix_chunk(c)
        return 0

    lax.fori_loop(0, last, step_chunk, 0)
    mix_chunk(last)

    def share_of(o):
        return pl.ds(pl.multiple_of(o * share, share), share)

    total_end = ends[0]
    for c in range(1, chunks):
        total_end = total_end + ends[c]
    decay_out[...] = jnp.concatenate(
        [total_end, jnp.zeros((8, 128 - heads), f32)], axis=1
    )
    state_out[...] = state[...].astype(bf16)

    def decay_copy(o):
        return remote(decay_out, decay_in.at[seq], decay_send.at[o], decay_recv.at[seq], at_seq(o))

    def state_copy(o):
        return remote(state_out.at[share_of(o)], owned.at[seq], state_send.at[o], state_recv.at[seq], at_seq(o))

    def back_copy(i):
        return remote(prefixes.at[i], carried.at[share_of(seq)], back_send.at[i], back_recv.at[seq], at_seq(i))

    for step in range(1, seq_count):
        o = (seq + step) % seq_count

        @pl.when(seq < seq_count - 1)
        def _():
            decay_copy(o).start()
            state_copy(o).start()

    @pl.when(seq < seq_count - 1)
    def _():
        decay_in[seq] = decay_out[...]
        owned[seq] = state_out[share_of(seq), :]

    def inside(c, _):
        at = chunk_of(c)
        cum = cum_ref[at, :]
        eye = (t_row == s_col).astype(f32)
        flip = (((0,), (0,)), ((), ()))
        cum_t = lax.dot_general(cum, eye, flip, preferred_element_type=f32, precision=HIGHEST)
        step_t = lax.dot_general(step_ref[at, :], eye, flip, preferred_element_type=f32, precision=HIGHEST)
        readout = bc_ref[at, states:]
        scores = lax.dot_general(
            readout, bc_ref[at, :states], (((1,), (1,)), ((), ())), preferred_element_type=f32
        )
        scores = jnp.where(causal, scores, 0.0)
        grown = jnp.exp(cum)
        lane = lax.broadcasted_iota(jnp.int32, (ROWS, 128), 1)
        for p in range(spans):
            span = slice(p * 128, (p + 1) * 128)
            x = x_ref[at, span]
            mixes, parts = [], []
            for k in range(per_span):
                h = p * per_span + k
                gaps = jnp.minimum(cum[:, h : h + 1] - cum_t[h : h + 1, :], 0.0)
                mixes.append((scores * jnp.exp(gaps) * step_t[h : h + 1, :]).astype(bf16))
                own = (lane >= k * head_width) & (lane < (k + 1) * head_width)
                parts.append(jnp.where(own, x, jnp.zeros_like(x)))
            total = jnp.dot(
                jnp.concatenate(mixes, axis=1), jnp.concatenate(parts, axis=0), preferred_element_type=f32
            )
            reads = jnp.dot(readout, starts[c, :, span], preferred_element_type=f32)
            weight = per_head(grown, p * per_span, per_span, head_width, 128)
            direct = per_head(skip[...], p * per_span, per_span, head_width, 128)
            y_ref[at, span] = total + reads * weight + direct * x.astype(f32)
        return 0

    lax.fori_loop(0, chunks, inside, 0)

    for j in range(seq_count - 1):

        @pl.when(seq != j)
        def _():
            remote(decay_out, decay_in.at[j], decay_send.at[j], decay_recv.at[j], at_seq(j)).wait_recv()
            remote(
                state_out.at[share_of(j)], owned.at[j], state_send.at[j], state_recv.at[j], at_seq(j)
            ).wait_recv()

    for p in range(tiles):
        cols = slice(p * tile, (p + 1) * tile)
        heads_tile = tile // head_width
        run = owned[0, :, cols].astype(f32)
        prefixes[0, :, cols] = jnp.zeros((share, tile), bf16)
        prefixes[1, :, cols] = run.astype(bf16)
        for i in range(2, seq_count):
            grown = jnp.exp(decay_in[i - 1][:1, :])
            run = run * per_head(grown, p * heads_tile, heads_tile, head_width, tile) + owned[i - 1, :, cols].astype(f32)
            prefixes[i, :, cols] = run.astype(bf16)
    for i in range(seq_count - 1, 0, -1):

        @pl.when(seq != i)
        def _():
            back_copy(i).start()

    carried[share_of(seq), :] = prefixes[seq]

    loads[13].wait()

    def gate_tile(j, _):
        cols = tile_of(j, tile)
        value = jnp.dot(full[0], gate_w[:half, cols], preferred_element_type=f32)
        value = value + jnp.dot(full[1], gate_w[half:, cols], preferred_element_type=f32)
        gate_ref[:, cols] = silu(rounded(value))
        return 0

    lax.fori_loop(0, tiles, gate_tile, 0)
    loads[14].wait()

    @pl.when(seq == 0)
    def _():
        carried[...] = jnp.zeros_like(carried)

    for o in range(seq_count):

        @pl.when((seq > 0) & (seq != o))
        def _():
            remote(
                prefixes.at[o], carried.at[share_of(o)], back_send.at[o], back_recv.at[o], at_seq(o)
            ).wait_recv()

    def gate_block(b):
        at = chunk_of(b)
        offset = jnp.zeros_like(ends[0])
        for c in range(chunks - 1):
            offset = offset + jnp.where(b > c, ends[c], jnp.zeros_like(ends[c]))
        grown = jnp.exp(cum_ref[at, :] + offset[:1, :])
        readout = bc_ref[at, states:]
        squares = jnp.zeros((ROWS, 128), f32)
        for p in range(spans):
            span = slice(p * 128, (p + 1) * 128)
            reads = jnp.dot(readout, carried[:, span], preferred_element_type=f32)
            weight = per_head(grown, p * per_span, per_span, head_width, 128)
            g = (y_ref[at, span] + reads * weight) * gate_ref[at, span]
            squares = squares + g * g
            gated[at, span] = (g * gain[p : p + 1, :]).astype(bf16)
        square_out[b] = lax.dot_general(
            jnp.ones((8, 128), f32), squares, (((1,), (1,)), ((), ())),
            preferred_element_type=f32, precision=HIGHEST,
        )

    def square_copy(b):
        return remote(square_out.at[b], square_in.at[tp], sq_send.at[b], sq_recv.at[tp], at_tp(b))

    def pair_of(side):
        return tile_of(side, 2 * ROWS)

    far_first = (1 - chip) * 2

    def gate_far(k, _):
        gate_block(far_first + k)
        return 0

    lax.fori_loop(0, 2, gate_far, 0)
    diagonal = (1 - chip) * 2 + 1 - core
    square_copy(across).start()
    square_copy(diagonal).start()

    def near_copy(p):
        return remote(near_out.at[p], near_in.at[p], near_send.at[p], near_recv.at[p], at_tp(mate))

    def far_copy(p):
        return remote(far_out.at[p], far_in.at[p], far_send.at[p], far_recv.at[p], at_tp(across))

    def own_copy(p):
        return remote(own_out.at[p], own_in.at[p], own_send.at[p], own_recv.at[p], at_tp(mate))

    def pass_on(p):
        near_copy(p).wait_recv()
        far_out[p] = (far_acc[p] + near_in[p].astype(f32)).astype(bf16)
        far_copy(p).start()

    def far_piece(p, _):
        cols = tile_of(p, piece)
        both[...] = jnp.dot(gated[pair_of(1 - chip), :], out_w[:, cols], preferred_element_type=f32)
        near_out[p] = both[chunk_of(1 - core), :].astype(bf16)
        near_copy(p).start()
        far_acc[p] = both[chunk_of(core), :]

        @pl.when(p > 0)
        def _():
            pass_on(jnp.maximum(p - 1, 0))

        return 0

    lax.fori_loop(0, PIECES, far_piece, 0)
    pass_on(PIECES - 1)

    def gate_near(k, _):
        gate_block(chip * 2 + k)
        return 0

    lax.fori_loop(0, 2, gate_near, 0)
    square_copy(mate).start()

    def own_piece(p, _):
        cols = tile_of(p, piece)
        both[...] = jnp.dot(gated[pair_of(chip), :], out_w[:, cols], preferred_element_type=f32)
        own_out[p] = both[chunk_of(1 - core), :].astype(bf16)
        own_copy(p).start()
        own_acc[p] = both[chunk_of(core), :]
        return 0

    lax.fori_loop(0, PIECES, own_piece, 0)

    square = square_out[tp]
    for step in range(1, tp_count):
        source = (tp + step) % tp_count
        remote(square_out.at[0], square_in.at[source], sq_send.at[0], sq_recv.at[source], at_tp(source)).wait_recv()
        square = square + square_in[source]
    mean = square[:1, :] / (channels * tp_count)
    spread = jnp.broadcast_to(lax.rsqrt(mean + 1e-05), (ROWS, ROWS))
    scale = jnp.sum(jnp.where(t_row == s_col, spread, 0.0), axis=1, keepdims=True)

    def finish(p, _):
        own_copy(p).wait_recv()
        far_copy(p).wait_recv()
        total = own_acc[p] + own_in[p].astype(f32) + far_in[p].astype(f32)
        out_ref[:, tile_of(p, piece)] = (total * scale).astype(bf16)
        return 0

    lax.fori_loop(0, PIECES, finish, 0)

    for c in range(chunks):
        crossing(c).wait_send()
        beside(c).wait_send()
        forwarded(c).wait_send()

    @pl.when(seq < seq_count - 1)
    def _():
        to_next().wait_send()

    for o in range(seq_count):

        @pl.when((seq < seq_count - 1) & (seq != o))
        def _():
            decay_copy(o).wait_send()
            state_copy(o).wait_send()

        if o > 0:

            @pl.when(seq != o)
            def _():
                back_copy(o).wait_send()

    for b in (across, diagonal, mate):
        square_copy(b).wait_send()
    for p in range(PIECES):
        near_copy(p).wait_send()
        far_copy(p).wait_send()
        own_copy(p).wait_send()


def fused(
    tokens, gate_weight, inner_weight, state_weight, step_weight, conv_inner, conv_state,
    step_bias, decay_rate, skip_gain, norm_gain, out_weight,
):
    rows, width = tokens.shape
    channels = inner_weight.shape[1]
    heads = step_weight.shape[1]
    head_width = channels // heads
    states = state_weight.shape[1] // 2
    depth, out_width = inner_weight.shape[0], out_weight.shape[1]
    seq_count, tp_count = lax.axis_size("seq"), lax.axis_size("tp")
    chunks = rows // ROWS
    share = states // seq_count
    piece = out_width // PIECES
    f32, bf16 = jnp.float32, jnp.bfloat16
    dma, vmem = pltpu.SemaphoreType.DMA, pltpu.VMEM
    args = (
        tokens, gate_weight, inner_weight, state_weight, step_weight.T, conv_inner, conv_state,
        step_bias[None, :], decay_rate[None, :], skip_gain[None, :], norm_gain.reshape(-1, 128), out_weight,
    )
    scratch = [
        vmem((2, rows, 2 * width), bf16),
        vmem((depth, channels), bf16),
        vmem((depth, channels), bf16),
        vmem((depth, 2 * states), bf16),
        vmem((heads, depth), bf16),
        vmem(conv_inner.shape, f32),
        vmem(conv_state.shape, f32),
        vmem((1, heads), f32),
        vmem((1, heads), f32),
        vmem((1, heads), f32),
        vmem((channels // 128, 128), f32),
        vmem((channels, out_width), bf16),
        vmem((rows, channels + 2 * states), f32),
        vmem((8, channels + 2 * states), f32),
        vmem((rows, heads), f32),
        vmem((rows, channels), bf16),
        vmem((rows, 2 * states), bf16),
        vmem((rows, channels), f32),
        vmem((rows, channels), f32),
        vmem((rows, channels), bf16),
        vmem((ROWS, channels), bf16),
        vmem((rows, heads), f32),
        vmem((rows, heads), f32),
        vmem((chunks, 8, heads), f32),
        vmem((states, channels), f32),
        vmem((chunks, states, channels), bf16),
        vmem((states, channels), bf16),
        vmem((seq_count, share, channels), bf16),
        vmem((seq_count, share, channels), bf16),
        vmem((states, channels), bf16),
        vmem((8, 128), f32),
        vmem((seq_count, 8, 128), f32),
        vmem((tp_count, 8, ROWS), f32),
        vmem((tp_count, 8, ROWS), f32),
    ]
    half_sums = vmem((PIECES, ROWS, piece), bf16)
    whole_sums = vmem((PIECES, ROWS, piece), f32)
    scratch += [half_sums, half_sums, whole_sums, half_sums, half_sums, half_sums, half_sums, whole_sums]
    scratch += [vmem((2 * ROWS, piece), f32)]
    scratch += [dma((15,))] + [dma((chunks,))] * 6 + [dma, dma] + [dma((seq_count,))] * 6
    scratch += [dma((tp_count,))] * 2 + [dma((PIECES,))] * 6
    anywhere = pl.BlockSpec(memory_space=pl.ANY)
    return pl.pallas_call(
        lambda *refs: layer_kernel(head_width, *refs),
        out_shape=pltpu.VMEM((rows // tp_count, out_width), bf16),
        in_specs=[anywhere] * len(args),
        out_specs=pl.BlockSpec(memory_space=pltpu.VMEM),
        scratch_shapes=scratch,
        compiler_params=pltpu.CompilerParams(
            collective_id=0, has_side_effects=True, vmem_limit_bytes=VMEM_LIMIT
        ),
        name="layer",
    )(*args)


def on_device(
    tokens,
    gate_weight,
    inner_weight,
    state_weight,
    step_weight,
    conv_inner,
    conv_state,
    step_bias,
    decay_rate,
    skip_gain,
    norm_gain,
    out_weight,
):
    tok_rows = tokens.shape[0]
    width_inner = inner_weight.shape[1]
    head_count = step_weight.shape[1]
    head_width = width_inner // head_count
    state_size = state_weight.shape[1] // 2
    blocks = tok_rows // GROUP
    size_tp = lax.axis_size("tp")
    me = lax.axis_index("tp")

    chunks = [None] * blocks
    for b in range(blocks - 1, -1, -1):
        chunks[b] = gather_features(tokens[b * GROUP : (b + 1) * GROUP])
    halo = shifted(chunks[-1][GROUP - HALO :], 1)
    chunks[0] = jnp.concatenate([halo, chunks[0]], axis=0)

    inner_raw, state_raw, step_raw = [None] * blocks, [None] * blocks, [None] * blocks
    for b in range(blocks - 1, -1, -1):
        i_b, s_b, t_b = project(chunks[b], inner_weight, state_weight, step_weight)
        inner_raw[b], state_raw[b] = i_b.astype(jnp.bfloat16), s_b.astype(jnp.bfloat16)
        step_raw[b] = t_b[HALO:] if b == 0 else t_b

    lanes = max(128, head_width)
    time_step = jax.nn.softplus(jnp.concatenate(step_raw, axis=0) + step_bias[None, :])
    log_decay = -time_step * decay_rate[None, :]
    grouped = log_decay.reshape(blocks, GROUP, head_count)
    cumulative = jnp.cumsum(grouped, axis=1)
    ending = cumulative[:, -1]
    tail = (jnp.exp(ending[:, None] - cumulative)).reshape(tok_rows, head_count) * time_step
    cumulative = cumulative.reshape(tok_rows, head_count)

    def cost(flops, count, exps):
        return pl.CostEstimate(flops=flops, bytes_accessed=count, transcendentals=exps)

    whole = tok_rows * width_inner
    x, bc, contribution = pl.pallas_call(
        lambda *refs: conv_kernel(blocks, head_width, lanes, *refs),
        out_shape=(
            jax.ShapeDtypeStruct((tok_rows, width_inner), jnp.bfloat16),
            jax.ShapeDtypeStruct((tok_rows, 2 * state_size), jnp.bfloat16),
            jax.ShapeDtypeStruct((blocks, width_inner, state_size), jnp.float32),
        ),
        cost_estimate=cost(2 * whole * state_size, 6 * whole, whole),
        name="conv",
    )(*inner_raw, *state_raw, conv_inner, conv_state, tail)
    contribution = contribution.reshape(blocks, head_count, head_width, state_size)
    local_state = jnp.zeros((head_count, head_width, state_size), jnp.float32)
    for b in range(blocks):
        local_state = jnp.exp(ending[b])[:, None, None] * local_state + contribution[b]

    def by_rows(width):
        return pl.BlockSpec((GROUP, width), lambda b: (b, 0))

    def by_columns(height):
        return pl.BlockSpec((height, GROUP), lambda b: (0, b))

    def fixed(width):
        return pl.BlockSpec((1, width), lambda b: (0, 0))

    intra = pl.pallas_call(
        lambda *refs: intra_kernel(head_width, lanes, *refs),
        grid=(blocks,),
        in_specs=[
            by_rows(width_inner),
            by_rows(2 * state_size),
            by_rows(head_count),
            by_columns(head_count),
            by_columns(head_count),
            fixed(width_inner),
        ],
        out_specs=by_rows(width_inner),
        out_shape=jax.ShapeDtypeStruct((tok_rows, width_inner), jnp.float32),
        cost_estimate=cost(4 * whole * GROUP, 6 * whole, GROUP * tok_rows * head_count),
        name="intra",
    )(x, bc, cumulative, cumulative.T, time_step.T, jnp.repeat(skip_gain, head_width)[None, :])

    gate = jnp.concatenate(
        [
            jnp.dot(c[c.shape[0] - GROUP :], gate_weight, preferred_element_type=jnp.float32).astype(jnp.bfloat16)
            for c in chunks
        ],
        axis=0,
    )

    carried, intra = earlier_state(
        local_state.astype(jnp.bfloat16).reshape(width_inner, state_size),
        jnp.sum(ending, axis=0),
        head_width,
        intra,
    )
    carried = carried.astype(jnp.float32).reshape(head_count, head_width, state_size)
    states = []
    for b in range(blocks):
        states.append(carried.astype(jnp.bfloat16).reshape(1, width_inner, state_size))
        carried = jnp.exp(ending[b])[:, None, None] * carried + contribution[b]

    gated, squares = pl.pallas_call(
        lambda *refs: gate_kernel(head_width, lanes, *refs),
        grid=(blocks,),
        in_specs=[
            by_rows(width_inner),
            by_rows(2 * state_size),
            by_rows(head_count),
            by_rows(width_inner),
            fixed(width_inner),
            pl.BlockSpec((1, width_inner, state_size), lambda b: (b, 0, 0)),
        ],
        out_specs=(by_rows(width_inner), by_rows(1)),
        out_shape=(
            jax.ShapeDtypeStruct((tok_rows, width_inner), jnp.bfloat16),
            jax.ShapeDtypeStruct((tok_rows, 1), jnp.float32),
        ),
        cost_estimate=cost(2 * whole * state_size, 8 * whole, whole),
        name="gate",
    )(intra, bc, cumulative, gate, norm_gain[None, :], jnp.concatenate(states, axis=0))

    square_total = sum_over_tp(squares[:, 0])
    share = tok_rows // size_tp
    mean_square = lax.dynamic_slice(square_total, (me * share,), (share,)) / (width_inner * size_tp)
    scale = lax.rsqrt(mean_square + 1e-05)[:, None]

    if size_tp != 4:
        part = jnp.dot(gated, out_weight, preferred_element_type=jnp.float32).astype(jnp.bfloat16)
        total = lax.psum_scatter(part, "tp", scatter_dimension=0, tiled=True)
        return (total.astype(jnp.float32) * scale).astype(jnp.bfloat16)

    side = me // 2

    def reduced(chip, weight):
        rows = lax.dynamic_slice(gated, (chip * 2 * share, 0), (2 * share, width_inner))
        both = jnp.dot(rows, weight, preferred_element_type=jnp.float32).astype(jnp.bfloat16)
        shape = (share, weight.shape[1])
        away = lax.dynamic_slice(both, ((1 - me % 2) * share, 0), shape)
        own = lax.dynamic_slice(both, ((me % 2) * share, 0), shape)
        return own.astype(jnp.float32) + swapped(away, 1).astype(jnp.float32)

    cuts = 2
    width_out = out_weight.shape[1] // cuts
    weights = [out_weight[:, c * width_out : (c + 1) * width_out] for c in range(cuts)]
    arrived = [swapped(reduced(side ^ 1, w).astype(jnp.bfloat16), 2) for w in weights]
    results = []
    for w, other in zip(weights, arrived):
        total = reduced(side, w) + other.astype(jnp.float32)
        results.append((total * scale).astype(jnp.bfloat16))
    return jnp.concatenate(results, axis=1)


def solution(mesh):
    in_specs = (
        P("seq", "tp"),
        P(None, "tp"),
        P(None, "tp"),
        P(),
        P(None, "tp"),
        P(None, "tp"),
        P(),
        P("tp"),
        P("tp"),
        P("tp"),
        P("tp"),
        P("tp", None),
    )
    out_specs = P(("seq", "tp"), None)
    quick = mesh.shape["tp"] == 4 and mesh.shape["seq"] == 8
    return jax.shard_map(
        fused if quick else on_device, mesh=mesh, in_specs=in_specs, out_specs=out_specs, check_vma=False
    )
```

```python
import jax
import jax.numpy as jnp
from jax import lax
from jax.experimental import pallas as pl
from jax.experimental.pallas import tpu as pltpu
from jax.sharding import PartitionSpec as P

GROUP = 256
HALO = 16


def swapped(shard, by):
    size = lax.axis_size("tp")
    return lax.ppermute(shard, "tp", [(i, i ^ by) for i in range(size)])


def shifted(shard, by):
    size = lax.axis_size("seq")
    return lax.ppermute(shard, "seq", [(i, i + by) for i in range(size - by)])


def gather_features(rows):
    size = lax.axis_size("tp")
    me = lax.axis_index("tp")
    width = rows.shape[1]
    held = [(0, rows)]
    step = size // 2
    while step >= 1:
        held = held + [(code ^ step, swapped(part, step)) for code, part in held]
        step //= 2
    parts = dict(held)
    full = jnp.zeros((rows.shape[0], width * size), rows.dtype)
    for code in range(size):
        full = lax.dynamic_update_slice(full, parts[code], (0, (me ^ code) * width))
    return full


def sum_over_tp(part):
    size = lax.axis_size("tp")
    step = 1
    while step < size:
        part = part + swapped(part, step)
        step *= 2
    return part


def prefix_kernel(mine_ref, decay_ref, owner_ref, out_ref):
    owner = owner_ref[...]
    carried = jnp.zeros(mine_ref.shape[1:], jnp.float32)
    for i in range(mine_ref.shape[0]):
        out_ref[i] = carried.astype(jnp.bfloat16)
        log_row = jnp.sum(owner * decay_ref[i : i + 1, :], axis=1, keepdims=True)
        carried = carried * jnp.exp(log_row) + mine_ref[i].astype(jnp.float32)


def earlier_state(local_state, decay_total, head_width, cover):
    size = lax.axis_size("seq")
    rows, states = local_state.shape
    share = rows // size
    me = lax.axis_index("seq")
    heads = decay_total.shape[0]
    wide = jnp.pad(decay_total, (0, -heads % 128))
    wide = jnp.broadcast_to(wide[None, None, :], (size, 1, wide.shape[0]))
    decay_all = lax.all_to_all(wide, "seq", 0, 0, tiled=True)[:, 0, :heads]
    blocks = local_state.reshape(size, share, states)
    blocks, decay_all = lax.optimization_barrier((blocks, decay_all))
    mine = lax.all_to_all(blocks, "seq", 0, 0, tiled=True)
    mine, cover = lax.optimization_barrier((mine, cover))
    row_head = (me * share + jnp.arange(share)) // head_width
    owner = (row_head[:, None] == jnp.arange(decay_total.shape[0])[None, :]).astype(jnp.float32)
    prefixes = pl.pallas_call(
        prefix_kernel,
        out_shape=jax.ShapeDtypeStruct(mine.shape, jnp.bfloat16),
        cost_estimate=pl.CostEstimate(flops=0, bytes_accessed=4 * mine.size, transcendentals=0),
    )(mine, decay_all, owner)
    return lax.all_to_all(prefixes, "seq", 0, 0, tiled=True).reshape(rows, states), cover


def per_head(table, first, count, width, lanes):
    lane = lax.broadcasted_iota(jnp.int32, (table.shape[0], lanes), 1)
    spread = jnp.broadcast_to(table[:, first : first + 1], (table.shape[0], lanes))
    for k in range(1, count):
        spread = jnp.where(lane >= k * width, table[:, first + k : first + k + 1], spread)
    return spread


def silu(value):
    return value * (0.5 * jnp.tanh(0.5 * value) + 0.5)


def conv_kernel(blocks, head_width, lanes, *refs):
    inner_refs, state_refs = refs[:blocks], refs[blocks : 2 * blocks]
    tap_inner, tap_state, tail_ref = refs[2 * blocks : 2 * blocks + 3]
    x_ref, bc_ref, contribution_ref = refs[2 * blocks + 3 :]
    taps = tap_inner.shape[0]
    heads_per = lanes // head_width

    def mixed(chunk_refs, b, span, kernel):
        if b == 0:
            padded = chunk_refs[0][:, span].astype(jnp.float32)
        else:
            last = chunk_refs[b - 1].shape[0] - HALO
            edge = chunk_refs[b - 1][last:, span].astype(jnp.float32)
            padded = jnp.concatenate([edge, chunk_refs[b][:, span].astype(jnp.float32)], axis=0)
        total = padded * kernel[taps - 1 : taps]
        for tap in range(taps - 1):
            total = total + pltpu.roll(padded, taps - 1 - tap, 0) * kernel[tap : tap + 1]
        return silu(total[HALO:]).astype(jnp.bfloat16)

    for b in range(blocks):
        rows = slice(b * GROUP, (b + 1) * GROUP)
        bc = mixed(state_refs, b, slice(None), tap_state[...])
        bc_ref[rows] = bc
        inject = bc[:, : bc.shape[1] // 2]
        tail = tail_ref[rows]
        for p in range(x_ref.shape[1] // lanes):
            span = slice(p * lanes, (p + 1) * lanes)
            x = mixed(inner_refs, b, span, tap_inner[:, span])
            x_ref[rows, span] = x
            weight = per_head(tail, p * heads_per, heads_per, head_width, lanes)
            scaled = (x.astype(jnp.float32) * weight).astype(jnp.bfloat16)
            contribution_ref[b, span] = lax.dot_general(
                scaled, inject, (((0,), (0,)), ((), ())), preferred_element_type=jnp.float32
            )


def intra_kernel(head_width, lanes, x_ref, bc_ref, cum_ref, cum_t_ref, step_t_ref, skip_ref, out_ref):
    states = bc_ref.shape[1] // 2
    heads_per = lanes // head_width
    scores = lax.dot_general(
        bc_ref[:, states:], bc_ref[:, :states], (((1,), (1,)), ((), ())),
        preferred_element_type=jnp.float32,
    )
    t = lax.broadcasted_iota(jnp.int32, scores.shape, 0)
    s = lax.broadcasted_iota(jnp.int32, scores.shape, 1)
    scores = jnp.where(s <= t, scores, 0.0)
    lane = lax.broadcasted_iota(jnp.int32, (x_ref.shape[0], lanes), 1)
    for p in range(x_ref.shape[1] // lanes):
        span = slice(p * lanes, (p + 1) * lanes)
        x = x_ref[:, span]
        total = None
        for k in range(heads_per):
            h = p * heads_per + k
            gaps = jnp.minimum(cum_ref[:, h : h + 1] - cum_t_ref[h : h + 1, :], 0.0)
            mixing = (scores * jnp.exp(gaps) * step_t_ref[h : h + 1, :]).astype(jnp.bfloat16)
            part = jnp.dot(mixing, x, preferred_element_type=jnp.float32)
            total = part if k == 0 else jnp.where(lane >= k * head_width, part, total)
        out_ref[:, span] = total + skip_ref[:, span] * x.astype(jnp.float32)


def gate_kernel(head_width, lanes, intra_ref, bc_ref, cum_ref, gate_ref, gain_ref, state_ref, out_ref, square_ref):
    states = bc_ref.shape[1] // 2
    heads_per = lanes // head_width
    readout = bc_ref[:, states:]
    grown = jnp.exp(cum_ref[...])
    squares = jnp.zeros((readout.shape[0], lanes), jnp.float32)
    for p in range(intra_ref.shape[1] // lanes):
        span = slice(p * lanes, (p + 1) * lanes)
        reads = lax.dot_general(
            readout, state_ref[0, span], (((1,), (1,)), ((), ())), preferred_element_type=jnp.float32
        )
        weight = per_head(grown, p * heads_per, heads_per, head_width, lanes)
        g = (intra_ref[:, span] + reads * weight) * silu(gate_ref[:, span].astype(jnp.float32))
        squares = squares + g * g
        out_ref[:, span] = (g * gain_ref[:, span]).astype(jnp.bfloat16)
    square_ref[...] = jnp.sum(squares, axis=1, keepdims=True)


def project(rows, *weights):
    return [jnp.dot(rows, weight, preferred_element_type=jnp.float32) for weight in weights]


ROWS = 128
PIECES = 10
VMEM_LIMIT = 56 * 1024 * 1024
MESH = pl.DeviceIdType.MESH
HIGHEST = lax.Precision.HIGHEST


def softplus(value):
    return jnp.maximum(value, 0.0) + jnp.log1p(jnp.exp(-jnp.abs(value)))


def chunk_of(index):
    return pl.ds(pl.multiple_of(index * ROWS, ROWS), ROWS)


def tile_of(index, width):
    return pl.ds(pl.multiple_of(index * width, width), width)


def layer_kernel(
    head_width,
    tok_in, gate_in, inner_in, statew_in, stepw_in, convi_in, convs_in, bias_in, rate_in, skip_in, gain_in, outw_in,
    out_ref,
    full, gate_w, inner_w, state_w, step_w, conv_i, conv_s, bias, rate, skip, gain, out_w,
    raw, halo, halo_out, step_acc, x_ref, bc_ref, y_ref, gate_ref, gated,
    cum_ref, step_ref, reach, ends, state, starts, state_out, owned, parts_ref, sums_out, sums_in, back, carried,
    decay_out, decay_in, square_acc,
    square_out, square_in, near_out, near_in, far_acc, far_out, far_in, own_out, own_in, own_acc, both,
    local_sem, x_send, x_recv, f_send, f_recv, d_send, d_recv, halo_send, halo_recv,
    state_send, state_recv, back_send, back_recv, decay_send, decay_recv, sums_send, sums_recv,
    sq_send, sq_recv, near_send, near_recv, far_send, far_recv, own_send, own_recv,
):
    seq_count, tp_count = lax.axis_size("seq"), lax.axis_size("tp")
    seq, tp = lax.axis_index("seq"), lax.axis_index("tp")
    chip, core = tp // 2, tp % 2
    mate, across = chip * 2 + 1 - core, (1 - chip) * 2 + core
    rows, half = full.shape[1], full.shape[2]
    width = half // 2
    channels = inner_w.shape[1]
    states = state_w.shape[1] // 2
    heads = step_w.shape[0]
    chunks = rows // ROWS
    tile = min(256, channels)
    tiles = channels // tile
    spans = channels // 128
    per_span = 128 // head_width
    quarter = seq_count // 2
    side, place = seq // quarter, seq % quarter
    share = states // quarter
    heads_tile = tile // head_width
    piece = out_w.shape[1] // PIECES
    f32, bf16 = jnp.float32, jnp.bfloat16
    across_rows = (((1,), (1,)), ((), ()))

    def at_tp(index):
        return {"seq": seq, "tp": index}

    def at_seq(index):
        return {"seq": index, "tp": tp}

    def remote(src, dst, send, recv, device):
        return pltpu.make_async_remote_copy(
            src_ref=src, dst_ref=dst, send_sem=send, recv_sem=recv, device_id=device, device_id_type=MESH
        )

    barrier = pltpu.get_barrier_semaphore()
    for step in range(1, tp_count):
        pl.semaphore_signal(barrier, inc=1, device_id=at_tp((tp + step) % tp_count), device_id_type=MESH)
    for step in range(1, seq_count):
        pl.semaphore_signal(barrier, inc=1, device_id=at_seq((seq + step) % seq_count), device_id_type=MESH)

    mine = pl.ds(pl.multiple_of(core * width, width), width)
    theirs = pl.ds(pl.multiple_of((1 - core) * width, width), width)
    near_rows = pl.ds(pl.multiple_of(chip * half, half), half)
    far_rows = pl.ds(pl.multiple_of((1 - chip) * half, half), half)
    loads = [
        (tok_in, full.at[chip, :, mine]),
        (inner_in.at[near_rows], inner_w.at[near_rows]),
        (statew_in.at[near_rows], state_w.at[near_rows]),
        (stepw_in.at[:, near_rows], step_w.at[:, near_rows]),
        (inner_in.at[far_rows], inner_w.at[far_rows]),
        (statew_in.at[far_rows], state_w.at[far_rows]),
        (stepw_in.at[:, far_rows], step_w.at[:, far_rows]),
        (convi_in, conv_i),
        (convs_in, conv_s),
        (bias_in, bias),
        (rate_in, rate),
        (skip_in, skip),
        (gain_in, gain),
        (gate_in, gate_w),
        (outw_in, out_w),
    ]
    loads = [pltpu.make_async_copy(src, dst, local_sem.at[i]) for i, (src, dst) in enumerate(loads)]
    for load in loads:
        load.start()
    loads[0].wait()
    pl.semaphore_wait(barrier, tp_count - 1 + seq_count - 1)

    order = [(rows - 16, 16)] + [(c * ROWS, ROWS) for c in range(chunks - 1)]
    order += [(rows - ROWS, ROWS // 2), (rows - ROWS // 2, ROWS // 2 - 16)]

    def crossing(i):
        part = full.at[chip, pl.ds(*order[i]), mine]
        return remote(part, part, x_send.at[i], x_recv.at[i], at_tp(across))

    def beside(columns):
        part = full.at[chip, :, columns]
        return remote(part, part, d_send, d_recv, at_tp(mate))

    def forwarded(i, columns):
        part = full.at[1 - chip, pl.ds(*order[i]), columns]
        return remote(part, part, f_send.at[i], f_recv.at[i], at_tp(mate))

    def receive(i):
        part = full.at[1 - chip, pl.ds(*order[i]), mine]
        remote(part, part, x_send.at[i], x_recv.at[i], at_tp(across)).wait_recv()
        forwarded(i, mine).start()
        forwarded(i, theirs).wait_recv()

    for i in range(len(order)):
        crossing(i).start()
    beside(mine).start()

    for load in loads[1:4]:
        load.wait()
    beside(theirs).wait_recv()

    near = full.at[chip]

    def first(j, _):
        cols = tile_of(j, tile)
        raw[:, cols] = jnp.dot(near[...], inner_w[near_rows, cols], preferred_element_type=f32)
        return 0

    lax.fori_loop(0, tiles, first, 0)
    raw[:, channels:] = jnp.dot(near[...], state_w[near_rows, :], preferred_element_type=f32)
    step_acc[...] = lax.dot_general(near[...], step_w[:, near_rows], across_rows, preferred_element_type=f32)
    for load in loads[4:13]:
        load.wait()

    def rounded(value):
        return value.astype(bf16).astype(f32)

    far = full.at[1 - chip]

    def project(at):
        for j in range(tiles):
            cols = slice(j * tile, (j + 1) * tile)
            more = jnp.dot(far[at, :], inner_w[far_rows, cols], preferred_element_type=f32)
            raw[at, cols] = rounded(raw[at, cols] + more)
        more = jnp.dot(far[at, :], state_w[far_rows, :], preferred_element_type=f32)
        raw[at, channels:] = rounded(raw[at, channels:] + more)
        more = lax.dot_general(far[at, :], step_w[:, far_rows], across_rows, preferred_element_type=f32)
        step_acc[at, :] += more

    t_row = lax.broadcasted_iota(jnp.int32, (ROWS, ROWS), 0)
    s_col = lax.broadcasted_iota(jnp.int32, (ROWS, ROWS), 1)
    causal = s_col <= t_row

    def mix_chunk(c, final):
        at = chunk_of(c)
        time_step = softplus(step_acc[at, :] + bias[...])
        decay = -time_step * rate[...]
        cum = jnp.dot(causal.astype(f32), decay, preferred_element_type=f32, precision=HIGHEST)
        ending = cum[ROWS - 1 :, :]
        tail = jnp.exp(ending - cum) * time_step
        cum_ref[at, :] = cum
        step_ref[at, :] = time_step
        ends[c] = jnp.broadcast_to(ending, ends.shape[1:])
        if final:
            total = ends[0]
            for k in range(1, chunks):
                total = total + ends[k]
            decay_out[...] = jnp.concatenate([total, jnp.zeros((8, 128 - heads), f32)], axis=1)
            for step in range(1, quarter):
                decay_copy((place + step) % quarter).start()
            decay_in[place] = decay_out[...]
        before = pl.ds(pl.multiple_of(jnp.maximum(c * ROWS - 8, 0), 8), 8)

        def conv(span, kernel):
            edge = jnp.where(c == 0, halo[:, span], raw[before, span])
            padded = jnp.concatenate([edge, raw[at, span]], axis=0)
            taps = kernel.shape[0]
            total = padded * kernel[taps - 1 : taps]
            for tap in range(taps - 1):
                total = total + pltpu.roll(padded, taps - 1 - tap, 0) * kernel[tap : tap + 1]
            return silu(total[8:]).astype(bf16)

        for p in range(2 * states // 128):
            span = slice(p * 128, (p + 1) * 128)
            bc_ref[at, span] = conv(slice(channels + p * 128, channels + (p + 1) * 128), conv_s[:, span])
        inject = bc_ref[at, :states]
        grown = jnp.exp(ending)
        for j in range(tiles):
            pieces = []
            for p in range(j * tile // 128, (j + 1) * tile // 128):
                span = slice(p * 128, (p + 1) * 128)
                x = conv(span, conv_i[:, span])
                x_ref[at, span] = x
                weight = per_head(tail, p * per_span, per_span, head_width, 128)
                pieces.append((x.astype(f32) * weight).astype(bf16))
            add = lax.dot_general(
                inject, jnp.concatenate(pieces, axis=1), (((0,), (0,)), ((), ())), preferred_element_type=f32
            )
            starts[c, j] = state[j].astype(bf16)
            weight = per_head(grown, j * heads_tile, heads_tile, head_width, tile)
            if final:
                state_out[j] = (state[j] * weight + add).astype(bf16)
                for step in range(1, quarter):
                    state_copy(j, (place + step) % quarter).start()
                owned[j, place] = state_out[j, share_of(place), :]
            else:
                state[j] = state[j] * weight + add

    def share_of(o):
        return pl.ds(pl.multiple_of(o * share, share), share)

    def at_place(o):
        return at_seq(side * quarter + o)

    def decay_copy(o):
        return remote(decay_out, decay_in.at[place], decay_send.at[o], decay_recv.at[place], at_place(o))

    def state_copy(j, o):
        return remote(
            state_out.at[j, share_of(o)], owned.at[j, place], state_send.at[j, o], state_recv.at[j, place], at_place(o)
        )

    def sums_copy(j):
        return remote(
            sums_out.at[j], sums_in.at[j], sums_send.at[j], sums_recv.at[j], at_seq((seq + quarter) % seq_count)
        )

    def back_copy(j, i):
        return remote(
            back.at[j, i], carried.at[j, share_of(place)], back_send.at[j, i], back_recv.at[j, place], at_place(i)
        )

    def combine(j):
        for step in range(1, quarter):
            o = (place + step) % quarter
            if j == 0:
                remote(decay_out, decay_in.at[o], decay_send.at[o], decay_recv.at[o], at_place(o)).wait_recv()
            remote(
                state_out.at[j, share_of(o)], owned.at[j, o], state_send.at[j, o], state_recv.at[j, o], at_place(o)
            ).wait_recv()
        run = owned[j, 0].astype(f32)
        parts_ref[j, 0] = jnp.zeros((share, tile), f32)
        for i in range(1, quarter):
            parts_ref[j, i] = run
            grown = per_head(jnp.exp(decay_in[i][:1, :]), j * heads_tile, heads_tile, head_width, tile)
            run = run * grown + owned[j, i].astype(f32)
        sums_out[j] = run.astype(bf16)
        sums_copy(j).start()

    def finalize(j):
        sums_copy(j).wait_recv()
        before = jnp.where(side > 0, sums_in[j].astype(f32), jnp.zeros((share, tile), f32))
        total = jnp.zeros((8, 128), f32)
        for i in range(quarter):
            grown = per_head(jnp.exp(total[:1, :]), j * heads_tile, heads_tile, head_width, tile)
            back[j, i] = (parts_ref[j, i] + before * grown).astype(bf16)
            total = total + decay_in[i]
        for step in range(1, quarter):
            back_copy(j, (place + step) % quarter).start()
        carried[j, share_of(place), :] = back[j, place]

    def await_carried(j):
        for step in range(1, quarter):
            o = (place + step) % quarter
            remote(
                back.at[j, o], carried.at[j, share_of(o)], back_send.at[j, o], back_recv.at[j, o], at_place(o)
            ).wait_recv()

    state[...] = jnp.zeros_like(state)

    receive(0)
    end_rows = far[rows - 16 :, :]
    for j in range(tiles):
        cols = slice(j * tile, (j + 1) * tile)
        more = jnp.dot(end_rows, inner_w[far_rows, cols], preferred_element_type=f32)
        halo_out[:, cols] = rounded(raw[rows - 8 :, cols] + more[8:])
    more = jnp.dot(end_rows, state_w[far_rows, :], preferred_element_type=f32)
    halo_out[:, channels:] = rounded(raw[rows - 8 :, channels:] + more[8:])

    def to_next():
        return remote(halo_out, halo, halo_send, halo_recv, at_seq(jnp.minimum(seq + 1, seq_count - 1)))

    @pl.when(seq < seq_count - 1)
    def _():
        to_next().start()

    @pl.when(seq == 0)
    def _():
        halo[...] = jnp.zeros_like(halo)

    last = chunks - 1
    for c in range(last):
        receive(1 + c)
        project(chunk_of(c))
        if c == 0:

            @pl.when(seq > 0)
            def _():
                remote(halo_out, halo, halo_send, halo_recv, at_seq(jnp.maximum(seq - 1, 0))).wait_recv()

        mix_chunk(c, False)
    receive(chunks)
    project(pl.ds(rows - ROWS, ROWS // 2))
    receive(chunks + 1)
    project(pl.ds(rows - ROWS // 2, ROWS // 2))
    mix_chunk(last, True)

    def inside(c, _):
        at = chunk_of(c)
        cum = cum_ref[at, :]
        eye = (t_row == s_col).astype(f32)
        flip = (((0,), (0,)), ((), ()))
        cum_t = lax.dot_general(cum, eye, flip, preferred_element_type=f32, precision=HIGHEST)
        step_t = lax.dot_general(step_ref[at, :], eye, flip, preferred_element_type=f32, precision=HIGHEST)
        readout = bc_ref[at, states:]
        scores = lax.dot_general(
            readout, bc_ref[at, :states], (((1,), (1,)), ((), ())), preferred_element_type=f32
        )
        scores = jnp.where(causal, scores, 0.0)
        grown = jnp.exp(cum)
        lane = lax.broadcasted_iota(jnp.int32, (ROWS, 128), 1)
        for p in range(spans):
            span = slice(p * 128, (p + 1) * 128)
            x = x_ref[at, span]
            mixes, parts = [], []
            for k in range(per_span):
                h = p * per_span + k
                gaps = jnp.minimum(cum[:, h : h + 1] - cum_t[h : h + 1, :], 0.0)
                mixes.append((scores * jnp.exp(gaps) * step_t[h : h + 1, :]).astype(bf16))
                own = (lane >= k * head_width) & (lane < (k + 1) * head_width)
                parts.append(jnp.where(own, x, jnp.zeros_like(x)))
            total = jnp.dot(
                jnp.concatenate(mixes, axis=1), jnp.concatenate(parts, axis=0), preferred_element_type=f32
            )
            lanes = slice(p * 128 % tile, p * 128 % tile + 128)
            reads = jnp.dot(readout, starts[c, p * 128 // tile, :, lanes], preferred_element_type=f32)
            weight = per_head(grown, p * per_span, per_span, head_width, 128)
            direct = per_head(skip[...], p * per_span, per_span, head_width, 128)
            y_ref[at, span] = total + reads * weight + direct * x.astype(f32)
        return 0

    lax.fori_loop(0, chunks - 1, inside, 0)
    loads[13].wait()

    def gate_tile(j):
        cols = slice(j * tile, (j + 1) * tile)
        value = jnp.dot(full[0], gate_w[:half, cols], preferred_element_type=f32)
        value = value + jnp.dot(full[1], gate_w[half:, cols], preferred_element_type=f32)
        gate_ref[:, cols] = silu(rounded(value))

    lag = 3
    for j in range(tiles):
        combine(j)
        gate_tile(j)
        if j >= lag:
            finalize(j - lag)
    finished = max(tiles - lag, 0)
    for j in range(finished, tiles - 1):
        finalize(j)
        finished = j + 1
    inside(last, 0)
    offset = jnp.zeros_like(ends[0])
    for c in range(chunks):
        reach[chunk_of(c), :] = jnp.exp(cum_ref[chunk_of(c), :] + offset[:1, :])
        offset = offset + ends[c]
    for j in range(finished, tiles):
        finalize(j)
    loads[14].wait()

    def gate_pair(b, j):
        cols = slice(j * tile, (j + 1) * tile)
        for k in range(2):
            at = chunk_of(b * 2 + k)
            reads = jnp.dot(bc_ref[at, states:], carried[j], preferred_element_type=f32)
            weight = per_head(reach[at, :], j * heads_tile, heads_tile, head_width, tile)
            g = (y_ref[at, cols] + reads * weight) * gate_ref[at, cols]
            squares = jnp.zeros((ROWS, 128), f32)
            for q in range(tile // 128):
                p = j * tile // 128 + q
                part = g[:, q * 128 : (q + 1) * 128]
                squares = squares + part * part
                gated[at, p * 128 : (p + 1) * 128] = (part * gain[p : p + 1, :]).astype(bf16)
            square_acc[k] = squares if j == 0 else square_acc[k] + squares

    def close_pair(b):
        for k in range(2):
            square_out[b * 2 + k] = lax.dot_general(
                jnp.ones((8, 128), f32), square_acc[k], across_rows,
                preferred_element_type=f32, precision=HIGHEST,
            )

    def square_copy(b):
        return remote(square_out.at[b], square_in.at[tp], sq_send.at[b], sq_recv.at[tp], at_tp(b))

    def pair_of(b):
        return tile_of(b, 2 * ROWS)

    for j in range(tiles):
        await_carried(j)
        gate_pair(1 - chip, j)
    close_pair(1 - chip)
    diagonal = (1 - chip) * 2 + 1 - core
    square_copy(across).start()
    square_copy(diagonal).start()

    def near_copy(p):
        return remote(near_out.at[p], near_in.at[p], near_send.at[p], near_recv.at[p], at_tp(mate))

    def far_copy(p):
        return remote(far_out.at[p], far_in.at[p], far_send.at[p], far_recv.at[p], at_tp(across))

    def own_copy(p):
        return remote(own_out.at[p], own_in.at[p], own_send.at[p], own_recv.at[p], at_tp(mate))

    def pass_on(p):
        near_copy(p).wait_recv()
        far_out[p] = (far_acc[p] + near_in[p].astype(f32)).astype(bf16)
        far_copy(p).start()

    def far_piece(p, _):
        cols = tile_of(p, piece)
        both[...] = jnp.dot(gated[pair_of(1 - chip), :], out_w[:, cols], preferred_element_type=f32)
        near_out[p] = both[chunk_of(1 - core), :].astype(bf16)
        near_copy(p).start()
        far_acc[p] = both[chunk_of(core), :]

        @pl.when(p > 0)
        def _():
            pass_on(jnp.maximum(p - 1, 0))

        return 0

    lax.fori_loop(0, PIECES, far_piece, 0)
    pass_on(PIECES - 1)

    for j in range(tiles):
        gate_pair(chip, j)
    close_pair(chip)
    square_copy(mate).start()

    def own_piece(p, _):
        cols = tile_of(p, piece)
        both[...] = jnp.dot(gated[pair_of(chip), :], out_w[:, cols], preferred_element_type=f32)
        own_out[p] = both[chunk_of(1 - core), :].astype(bf16)
        own_copy(p).start()
        own_acc[p] = both[chunk_of(core), :]
        return 0

    lax.fori_loop(0, PIECES, own_piece, 0)

    square = square_out[tp]
    for step in range(1, tp_count):
        source = (tp + step) % tp_count
        remote(square_out.at[0], square_in.at[source], sq_send.at[0], sq_recv.at[source], at_tp(source)).wait_recv()
        square = square + square_in[source]
    mean = square[:1, :] / (channels * tp_count)
    spread = jnp.broadcast_to(lax.rsqrt(mean + 1e-05), (ROWS, ROWS))
    scale = jnp.sum(jnp.where(t_row == s_col, spread, 0.0), axis=1, keepdims=True)

    def finish(p, _):
        own_copy(p).wait_recv()
        far_copy(p).wait_recv()
        total = own_acc[p] + own_in[p].astype(f32) + far_in[p].astype(f32)
        out_ref[:, tile_of(p, piece)] = (total * scale).astype(bf16)
        return 0

    lax.fori_loop(0, PIECES, finish, 0)

    for i in range(len(order)):
        crossing(i).wait_send()
        forwarded(i, mine).wait_send()
    beside(mine).wait_send()

    @pl.when(seq < seq_count - 1)
    def _():
        to_next().wait_send()

    for step in range(1, quarter):
        o = (place + step) % quarter
        decay_copy(o).wait_send()
        for j in range(tiles):
            state_copy(j, o).wait_send()
            back_copy(j, o).wait_send()
    for j in range(tiles):
        sums_copy(j).wait_send()
    for b in (across, diagonal, mate):
        square_copy(b).wait_send()
    for p in range(PIECES):
        near_copy(p).wait_send()
        far_copy(p).wait_send()
        own_copy(p).wait_send()


def fused(
    tokens, gate_weight, inner_weight, state_weight, step_weight, conv_inner, conv_state,
    step_bias, decay_rate, skip_gain, norm_gain, out_weight,
):
    rows, width = tokens.shape
    channels = inner_weight.shape[1]
    heads = step_weight.shape[1]
    head_width = channels // heads
    states = state_weight.shape[1] // 2
    depth, out_width = inner_weight.shape[0], out_weight.shape[1]
    seq_count, tp_count = lax.axis_size("seq"), lax.axis_size("tp")
    chunks = rows // ROWS
    quarter = seq_count // 2
    share = states // quarter
    tile = min(256, channels)
    tiles = channels // tile
    arrivals = chunks + 2
    piece = out_width // PIECES
    f32, bf16 = jnp.float32, jnp.bfloat16
    dma, vmem = pltpu.SemaphoreType.DMA, pltpu.VMEM
    args = (
        tokens, gate_weight, inner_weight, state_weight, step_weight.T, conv_inner, conv_state,
        step_bias[None, :], decay_rate[None, :], skip_gain[None, :], norm_gain.reshape(-1, 128), out_weight,
    )
    scratch = [
        vmem((2, rows, 2 * width), bf16),
        vmem((depth, channels), bf16),
        vmem((depth, channels), bf16),
        vmem((depth, 2 * states), bf16),
        vmem((heads, depth), bf16),
        vmem(conv_inner.shape, f32),
        vmem(conv_state.shape, f32),
        vmem((1, heads), f32),
        vmem((1, heads), f32),
        vmem((1, heads), f32),
        vmem((channels // 128, 128), f32),
        vmem((channels, out_width), bf16),
        vmem((rows, channels + 2 * states), f32),
        vmem((8, channels + 2 * states), f32),
        vmem((8, channels + 2 * states), f32),
        vmem((rows, heads), f32),
        vmem((rows, channels), bf16),
        vmem((rows, 2 * states), bf16),
        vmem((rows, channels), f32),
        vmem((rows, channels), f32),
        vmem((rows, channels), bf16),
        vmem((rows, heads), f32),
        vmem((rows, heads), f32),
        vmem((rows, heads), f32),
        vmem((chunks, 8, heads), f32),
        vmem((tiles, states, tile), f32),
        vmem((chunks, tiles, states, tile), bf16),
        vmem((tiles, states, tile), bf16),
        vmem((tiles, quarter, share, tile), bf16),
        vmem((tiles, quarter, share, tile), f32),
        vmem((tiles, share, tile), bf16),
        vmem((tiles, share, tile), bf16),
        vmem((tiles, quarter, share, tile), bf16),
        vmem((tiles, states, tile), bf16),
        vmem((8, 128), f32),
        vmem((quarter, 8, 128), f32),
        vmem((2, ROWS, 128), f32),
        vmem((tp_count, 8, ROWS), f32),
        vmem((tp_count, 8, ROWS), f32),
    ]
    half_sums = vmem((PIECES, ROWS, piece), bf16)
    whole_sums = vmem((PIECES, ROWS, piece), f32)
    scratch += [half_sums, half_sums, whole_sums, half_sums, half_sums, half_sums, half_sums, whole_sums]
    scratch += [vmem((2 * ROWS, piece), f32)]
    scratch += [dma((15,))] + [dma((arrivals,))] * 4 + [dma] * 4
    scratch += [dma((tiles, quarter))] * 4 + [dma((quarter,))] * 2 + [dma((tiles,))] * 2
    scratch += [dma((tp_count,))] * 2 + [dma((PIECES,))] * 6
    anywhere = pl.BlockSpec(memory_space=pl.ANY)
    return pl.pallas_call(
        lambda *refs: layer_kernel(head_width, *refs),
        out_shape=pltpu.VMEM((rows // tp_count, out_width), bf16),
        in_specs=[anywhere] * len(args),
        out_specs=pl.BlockSpec(memory_space=pltpu.VMEM),
        scratch_shapes=scratch,
        compiler_params=pltpu.CompilerParams(
            collective_id=0, has_side_effects=True, vmem_limit_bytes=VMEM_LIMIT
        ),
        name="layer",
    )(*args)


def on_device(
    tokens,
    gate_weight,
    inner_weight,
    state_weight,
    step_weight,
    conv_inner,
    conv_state,
    step_bias,
    decay_rate,
    skip_gain,
    norm_gain,
    out_weight,
):
    tok_rows = tokens.shape[0]
    width_inner = inner_weight.shape[1]
    head_count = step_weight.shape[1]
    head_width = width_inner // head_count
    state_size = state_weight.shape[1] // 2
    blocks = tok_rows // GROUP
    size_tp = lax.axis_size("tp")
    me = lax.axis_index("tp")

    chunks = [None] * blocks
    for b in range(blocks - 1, -1, -1):
        chunks[b] = gather_features(tokens[b * GROUP : (b + 1) * GROUP])
    halo = shifted(chunks[-1][GROUP - HALO :], 1)
    chunks[0] = jnp.concatenate([halo, chunks[0]], axis=0)

    inner_raw, state_raw, step_raw = [None] * blocks, [None] * blocks, [None] * blocks
    for b in range(blocks - 1, -1, -1):
        i_b, s_b, t_b = project(chunks[b], inner_weight, state_weight, step_weight)
        inner_raw[b], state_raw[b] = i_b.astype(jnp.bfloat16), s_b.astype(jnp.bfloat16)
        step_raw[b] = t_b[HALO:] if b == 0 else t_b

    lanes = max(128, head_width)
    time_step = jax.nn.softplus(jnp.concatenate(step_raw, axis=0) + step_bias[None, :])
    log_decay = -time_step * decay_rate[None, :]
    grouped = log_decay.reshape(blocks, GROUP, head_count)
    cumulative = jnp.cumsum(grouped, axis=1)
    ending = cumulative[:, -1]
    tail = (jnp.exp(ending[:, None] - cumulative)).reshape(tok_rows, head_count) * time_step
    cumulative = cumulative.reshape(tok_rows, head_count)

    def cost(flops, count, exps):
        return pl.CostEstimate(flops=flops, bytes_accessed=count, transcendentals=exps)

    whole = tok_rows * width_inner
    x, bc, contribution = pl.pallas_call(
        lambda *refs: conv_kernel(blocks, head_width, lanes, *refs),
        out_shape=(
            jax.ShapeDtypeStruct((tok_rows, width_inner), jnp.bfloat16),
            jax.ShapeDtypeStruct((tok_rows, 2 * state_size), jnp.bfloat16),
            jax.ShapeDtypeStruct((blocks, width_inner, state_size), jnp.float32),
        ),
        cost_estimate=cost(2 * whole * state_size, 6 * whole, whole),
        name="conv",
    )(*inner_raw, *state_raw, conv_inner, conv_state, tail)
    contribution = contribution.reshape(blocks, head_count, head_width, state_size)
    local_state = jnp.zeros((head_count, head_width, state_size), jnp.float32)
    for b in range(blocks):
        local_state = jnp.exp(ending[b])[:, None, None] * local_state + contribution[b]

    def by_rows(width):
        return pl.BlockSpec((GROUP, width), lambda b: (b, 0))

    def by_columns(height):
        return pl.BlockSpec((height, GROUP), lambda b: (0, b))

    def fixed(width):
        return pl.BlockSpec((1, width), lambda b: (0, 0))

    intra = pl.pallas_call(
        lambda *refs: intra_kernel(head_width, lanes, *refs),
        grid=(blocks,),
        in_specs=[
            by_rows(width_inner),
            by_rows(2 * state_size),
            by_rows(head_count),
            by_columns(head_count),
            by_columns(head_count),
            fixed(width_inner),
        ],
        out_specs=by_rows(width_inner),
        out_shape=jax.ShapeDtypeStruct((tok_rows, width_inner), jnp.float32),
        cost_estimate=cost(4 * whole * GROUP, 6 * whole, GROUP * tok_rows * head_count),
        name="intra",
    )(x, bc, cumulative, cumulative.T, time_step.T, jnp.repeat(skip_gain, head_width)[None, :])

    gate = jnp.concatenate(
        [
            jnp.dot(c[c.shape[0] - GROUP :], gate_weight, preferred_element_type=jnp.float32).astype(jnp.bfloat16)
            for c in chunks
        ],
        axis=0,
    )

    carried, intra = earlier_state(
        local_state.astype(jnp.bfloat16).reshape(width_inner, state_size),
        jnp.sum(ending, axis=0),
        head_width,
        intra,
    )
    carried = carried.astype(jnp.float32).reshape(head_count, head_width, state_size)
    states = []
    for b in range(blocks):
        states.append(carried.astype(jnp.bfloat16).reshape(1, width_inner, state_size))
        carried = jnp.exp(ending[b])[:, None, None] * carried + contribution[b]

    gated, squares = pl.pallas_call(
        lambda *refs: gate_kernel(head_width, lanes, *refs),
        grid=(blocks,),
        in_specs=[
            by_rows(width_inner),
            by_rows(2 * state_size),
            by_rows(head_count),
            by_rows(width_inner),
            fixed(width_inner),
            pl.BlockSpec((1, width_inner, state_size), lambda b: (b, 0, 0)),
        ],
        out_specs=(by_rows(width_inner), by_rows(1)),
        out_shape=(
            jax.ShapeDtypeStruct((tok_rows, width_inner), jnp.bfloat16),
            jax.ShapeDtypeStruct((tok_rows, 1), jnp.float32),
        ),
        cost_estimate=cost(2 * whole * state_size, 8 * whole, whole),
        name="gate",
    )(intra, bc, cumulative, gate, norm_gain[None, :], jnp.concatenate(states, axis=0))

    square_total = sum_over_tp(squares[:, 0])
    share = tok_rows // size_tp
    mean_square = lax.dynamic_slice(square_total, (me * share,), (share,)) / (width_inner * size_tp)
    scale = lax.rsqrt(mean_square + 1e-05)[:, None]

    if size_tp != 4:
        part = jnp.dot(gated, out_weight, preferred_element_type=jnp.float32).astype(jnp.bfloat16)
        total = lax.psum_scatter(part, "tp", scatter_dimension=0, tiled=True)
        return (total.astype(jnp.float32) * scale).astype(jnp.bfloat16)

    side = me // 2

    def reduced(chip, weight):
        rows = lax.dynamic_slice(gated, (chip * 2 * share, 0), (2 * share, width_inner))
        both = jnp.dot(rows, weight, preferred_element_type=jnp.float32).astype(jnp.bfloat16)
        shape = (share, weight.shape[1])
        away = lax.dynamic_slice(both, ((1 - me % 2) * share, 0), shape)
        own = lax.dynamic_slice(both, ((me % 2) * share, 0), shape)
        return own.astype(jnp.float32) + swapped(away, 1).astype(jnp.float32)

    cuts = 2
    width_out = out_weight.shape[1] // cuts
    weights = [out_weight[:, c * width_out : (c + 1) * width_out] for c in range(cuts)]
    arrived = [swapped(reduced(side ^ 1, w).astype(jnp.bfloat16), 2) for w in weights]
    results = []
    for w, other in zip(weights, arrived):
        total = reduced(side, w) + other.astype(jnp.float32)
        results.append((total * scale).astype(jnp.bfloat16))
    return jnp.concatenate(results, axis=1)


def solution(mesh):
    in_specs = (
        P("seq", "tp"),
        P(None, "tp"),
        P(None, "tp"),
        P(),
        P(None, "tp"),
        P(None, "tp"),
        P(),
        P("tp"),
        P("tp"),
        P("tp"),
        P("tp"),
        P("tp", None),
    )
    out_specs = P(("seq", "tp"), None)
    quick = mesh.shape["tp"] == 4 and mesh.shape["seq"] == 8
    return jax.shard_map(
        fused if quick else on_device, mesh=mesh, in_specs=in_specs, out_specs=out_specs, check_vma=False
    )
```

```python
import jax
import jax.numpy as jnp
from jax import lax
from jax.experimental import pallas as pl
from jax.experimental.pallas import tpu as pltpu
from jax.sharding import PartitionSpec as P

GROUP = 256
HALO = 16


def swapped(shard, by):
    size = lax.axis_size("tp")
    return lax.ppermute(shard, "tp", [(i, i ^ by) for i in range(size)])


def shifted(shard, by):
    size = lax.axis_size("seq")
    return lax.ppermute(shard, "seq", [(i, i + by) for i in range(size - by)])


def gather_features(rows):
    size = lax.axis_size("tp")
    me = lax.axis_index("tp")
    width = rows.shape[1]
    held = [(0, rows)]
    step = size // 2
    while step >= 1:
        held = held + [(code ^ step, swapped(part, step)) for code, part in held]
        step //= 2
    parts = dict(held)
    full = jnp.zeros((rows.shape[0], width * size), rows.dtype)
    for code in range(size):
        full = lax.dynamic_update_slice(full, parts[code], (0, (me ^ code) * width))
    return full


def sum_over_tp(part):
    size = lax.axis_size("tp")
    step = 1
    while step < size:
        part = part + swapped(part, step)
        step *= 2
    return part


def prefix_kernel(mine_ref, decay_ref, owner_ref, out_ref):
    owner = owner_ref[...]
    carried = jnp.zeros(mine_ref.shape[1:], jnp.float32)
    for i in range(mine_ref.shape[0]):
        out_ref[i] = carried.astype(jnp.bfloat16)
        log_row = jnp.sum(owner * decay_ref[i : i + 1, :], axis=1, keepdims=True)
        carried = carried * jnp.exp(log_row) + mine_ref[i].astype(jnp.float32)


def earlier_state(local_state, decay_total, head_width, cover):
    size = lax.axis_size("seq")
    rows, states = local_state.shape
    share = rows // size
    me = lax.axis_index("seq")
    heads = decay_total.shape[0]
    wide = jnp.pad(decay_total, (0, -heads % 128))
    wide = jnp.broadcast_to(wide[None, None, :], (size, 1, wide.shape[0]))
    decay_all = lax.all_to_all(wide, "seq", 0, 0, tiled=True)[:, 0, :heads]
    blocks = local_state.reshape(size, share, states)
    blocks, decay_all = lax.optimization_barrier((blocks, decay_all))
    mine = lax.all_to_all(blocks, "seq", 0, 0, tiled=True)
    mine, cover = lax.optimization_barrier((mine, cover))
    row_head = (me * share + jnp.arange(share)) // head_width
    owner = (row_head[:, None] == jnp.arange(decay_total.shape[0])[None, :]).astype(jnp.float32)
    prefixes = pl.pallas_call(
        prefix_kernel,
        out_shape=jax.ShapeDtypeStruct(mine.shape, jnp.bfloat16),
        cost_estimate=pl.CostEstimate(flops=0, bytes_accessed=4 * mine.size, transcendentals=0),
    )(mine, decay_all, owner)
    return lax.all_to_all(prefixes, "seq", 0, 0, tiled=True).reshape(rows, states), cover


def per_head(table, first, count, width, lanes):
    lane = lax.broadcasted_iota(jnp.int32, (table.shape[0], lanes), 1)
    spread = jnp.broadcast_to(table[:, first : first + 1], (table.shape[0], lanes))
    for k in range(1, count):
        spread = jnp.where(lane >= k * width, table[:, first + k : first + k + 1], spread)
    return spread


def silu(value):
    return value * (0.5 * jnp.tanh(0.5 * value) + 0.5)


def conv_kernel(blocks, head_width, lanes, *refs):
    inner_refs, state_refs = refs[:blocks], refs[blocks : 2 * blocks]
    tap_inner, tap_state, tail_ref = refs[2 * blocks : 2 * blocks + 3]
    x_ref, bc_ref, contribution_ref = refs[2 * blocks + 3 :]
    taps = tap_inner.shape[0]
    heads_per = lanes // head_width

    def mixed(chunk_refs, b, span, kernel):
        if b == 0:
            padded = chunk_refs[0][:, span].astype(jnp.float32)
        else:
            last = chunk_refs[b - 1].shape[0] - HALO
            edge = chunk_refs[b - 1][last:, span].astype(jnp.float32)
            padded = jnp.concatenate([edge, chunk_refs[b][:, span].astype(jnp.float32)], axis=0)
        total = padded * kernel[taps - 1 : taps]
        for tap in range(taps - 1):
            total = total + pltpu.roll(padded, taps - 1 - tap, 0) * kernel[tap : tap + 1]
        return silu(total[HALO:]).astype(jnp.bfloat16)

    for b in range(blocks):
        rows = slice(b * GROUP, (b + 1) * GROUP)
        bc = mixed(state_refs, b, slice(None), tap_state[...])
        bc_ref[rows] = bc
        inject = bc[:, : bc.shape[1] // 2]
        tail = tail_ref[rows]
        for p in range(x_ref.shape[1] // lanes):
            span = slice(p * lanes, (p + 1) * lanes)
            x = mixed(inner_refs, b, span, tap_inner[:, span])
            x_ref[rows, span] = x
            weight = per_head(tail, p * heads_per, heads_per, head_width, lanes)
            scaled = (x.astype(jnp.float32) * weight).astype(jnp.bfloat16)
            contribution_ref[b, span] = lax.dot_general(
                scaled, inject, (((0,), (0,)), ((), ())), preferred_element_type=jnp.float32
            )


def intra_kernel(head_width, lanes, x_ref, bc_ref, cum_ref, cum_t_ref, step_t_ref, skip_ref, out_ref):
    states = bc_ref.shape[1] // 2
    heads_per = lanes // head_width
    scores = lax.dot_general(
        bc_ref[:, states:], bc_ref[:, :states], (((1,), (1,)), ((), ())),
        preferred_element_type=jnp.float32,
    )
    t = lax.broadcasted_iota(jnp.int32, scores.shape, 0)
    s = lax.broadcasted_iota(jnp.int32, scores.shape, 1)
    scores = jnp.where(s <= t, scores, 0.0)
    lane = lax.broadcasted_iota(jnp.int32, (x_ref.shape[0], lanes), 1)
    for p in range(x_ref.shape[1] // lanes):
        span = slice(p * lanes, (p + 1) * lanes)
        x = x_ref[:, span]
        total = None
        for k in range(heads_per):
            h = p * heads_per + k
            gaps = jnp.minimum(cum_ref[:, h : h + 1] - cum_t_ref[h : h + 1, :], 0.0)
            mixing = (scores * jnp.exp(gaps) * step_t_ref[h : h + 1, :]).astype(jnp.bfloat16)
            part = jnp.dot(mixing, x, preferred_element_type=jnp.float32)
            total = part if k == 0 else jnp.where(lane >= k * head_width, part, total)
        out_ref[:, span] = total + skip_ref[:, span] * x.astype(jnp.float32)


def gate_kernel(head_width, lanes, intra_ref, bc_ref, cum_ref, gate_ref, gain_ref, state_ref, out_ref, square_ref):
    states = bc_ref.shape[1] // 2
    heads_per = lanes // head_width
    readout = bc_ref[:, states:]
    grown = jnp.exp(cum_ref[...])
    squares = jnp.zeros((readout.shape[0], lanes), jnp.float32)
    for p in range(intra_ref.shape[1] // lanes):
        span = slice(p * lanes, (p + 1) * lanes)
        reads = lax.dot_general(
            readout, state_ref[0, span], (((1,), (1,)), ((), ())), preferred_element_type=jnp.float32
        )
        weight = per_head(grown, p * heads_per, heads_per, head_width, lanes)
        g = (intra_ref[:, span] + reads * weight) * silu(gate_ref[:, span].astype(jnp.float32))
        squares = squares + g * g
        out_ref[:, span] = (g * gain_ref[:, span]).astype(jnp.bfloat16)
    square_ref[...] = jnp.sum(squares, axis=1, keepdims=True)


def project(rows, *weights):
    return [jnp.dot(rows, weight, preferred_element_type=jnp.float32) for weight in weights]


ROWS = 128
PIECES = 10
VMEM_LIMIT = 56 * 1024 * 1024
MESH = pl.DeviceIdType.MESH
HIGHEST = lax.Precision.HIGHEST


def softplus(value):
    return jnp.maximum(value, 0.0) + jnp.log1p(jnp.exp(-jnp.abs(value)))


def chunk_of(index):
    return pl.ds(pl.multiple_of(index * ROWS, ROWS), ROWS)


def tile_of(index, width):
    return pl.ds(pl.multiple_of(index * width, width), width)


def layer_kernel(
    head_width,
    tok_in, gate_in, inner_in, statew_in, stepw_in, convi_in, convs_in, bias_in, rate_in, skip_in, gain_in, outw_in,
    out_ref,
    full, gate_w, inner_w, state_w, step_w, conv_i, conv_s, bias, rate, skip, gain, out_w,
    raw, halo, halo_out, step_acc, x_ref, bc_ref, y_ref, gate_ref, gated,
    cum_ref, step_ref, reach, ends, state, starts, state_out, owned, parts_ref, sums_out, sums_in, back, carried,
    decay_out, decay_in, square_acc,
    square_out, square_in, near_out, near_in, far_acc, far_out, far_in, own_out, own_in, own_acc, both,
    ready, local_sem, x_send, x_recv, f_send, f_recv, d_send, d_recv, halo_send, halo_recv,
    state_send, state_recv, back_send, back_recv, decay_send, decay_recv, sums_send, sums_recv,
    sq_send, sq_recv, near_send, near_recv, far_send, far_recv, own_send, own_recv,
):
    seq_count, tp_count = lax.axis_size("seq"), lax.axis_size("tp")
    seq, tp = lax.axis_index("seq"), lax.axis_index("tp")
    chip, core = tp // 2, tp % 2
    mate, across = chip * 2 + 1 - core, (1 - chip) * 2 + core
    rows, half = full.shape[1], full.shape[2]
    width = half // 2
    channels = inner_w.shape[1]
    states = state_w.shape[1] // 2
    heads = step_w.shape[0]
    chunks = rows // ROWS
    tile = min(256, channels)
    tiles = channels // tile
    spans = channels // 128
    per_span = 128 // head_width
    quarter = seq_count // 2
    side, place = seq // quarter, seq % quarter
    share = states // quarter
    heads_tile = tile // head_width
    piece = out_w.shape[1] // PIECES
    f32, bf16 = jnp.float32, jnp.bfloat16
    across_rows = (((1,), (1,)), ((), ()))

    def at_tp(index):
        return {"seq": seq, "tp": index}

    def at_seq(index):
        return {"seq": index, "tp": tp}

    def remote(src, dst, send, recv, device):
        return pltpu.make_async_remote_copy(
            src_ref=src, dst_ref=dst, send_sem=send, recv_sem=recv, device_id=device, device_id_type=MESH
        )

    barrier = pltpu.get_barrier_semaphore()
    for step in range(1, tp_count):
        pl.semaphore_signal(barrier, inc=1, device_id=at_tp((tp + step) % tp_count), device_id_type=MESH)
    def related(low, high):
        return (low < high) & ((low // quarter == high // quarter) | (high == low + quarter) | (high == low + 1))

    for d in range(seq_count):

        @pl.when(related(seq, d))
        def _():
            pl.semaphore_signal(barrier, inc=1, device_id=at_seq(d), device_id_type=MESH)

    lower = sum(jnp.where(related(d, seq), 1, 0) for d in range(seq_count))
    higher = sum(jnp.where(related(seq, d), 1, 0) for d in range(seq_count))

    mine = pl.ds(pl.multiple_of(core * width, width), width)
    theirs = pl.ds(pl.multiple_of((1 - core) * width, width), width)
    near_rows = pl.ds(pl.multiple_of(chip * half, half), half)
    far_rows = pl.ds(pl.multiple_of((1 - chip) * half, half), half)
    loads = [
        (tok_in, full.at[chip, :, mine]),
        (inner_in.at[near_rows], inner_w.at[near_rows]),
        (statew_in.at[near_rows], state_w.at[near_rows]),
        (stepw_in.at[:, near_rows], step_w.at[:, near_rows]),
        (inner_in.at[far_rows], inner_w.at[far_rows]),
        (statew_in.at[far_rows], state_w.at[far_rows]),
        (stepw_in.at[:, far_rows], step_w.at[:, far_rows]),
        (convi_in, conv_i),
        (convs_in, conv_s),
        (bias_in, bias),
        (rate_in, rate),
        (skip_in, skip),
        (gain_in, gain),
        (gate_in, gate_w),
        (outw_in, out_w),
    ]
    loads = [pltpu.make_async_copy(src, dst, local_sem.at[i]) for i, (src, dst) in enumerate(loads)]
    for load in loads[:13]:
        load.start()
    loads[0].wait()
    pl.semaphore_wait(barrier, tp_count - 1 + lower)
    for d in range(seq_count):

        @pl.when(related(d, seq))
        def _():
            pl.semaphore_signal(ready, inc=1, device_id=at_seq(d), device_id_type=MESH)


    order = [(rows - 16, 16)] + [(c * ROWS, ROWS) for c in range(chunks - 1)]
    order += [(rows - ROWS, ROWS // 2), (rows - ROWS // 2, ROWS // 2 - 16)]

    def crossing(i):
        part = full.at[chip, pl.ds(*order[i]), mine]
        return remote(part, part, x_send.at[i], x_recv.at[i], at_tp(across))

    def beside(columns):
        part = full.at[chip, :, columns]
        return remote(part, part, d_send, d_recv, at_tp(mate))

    def forwarded(i, columns):
        part = full.at[1 - chip, pl.ds(*order[i]), columns]
        return remote(part, part, f_send.at[i], f_recv.at[i], at_tp(mate))

    def relay(i):
        part = full.at[1 - chip, pl.ds(*order[i]), mine]
        remote(part, part, x_send.at[i], x_recv.at[i], at_tp(across)).wait_recv()
        forwarded(i, mine).start()

    def settle(i):
        forwarded(i, theirs).wait_recv()

    for i in range(len(order)):
        crossing(i).start()
    beside(mine).start()

    for load in loads[1:4]:
        load.wait()
    beside(theirs).wait_recv()

    near = full.at[chip]

    def first(j, _):
        cols = tile_of(j, tile)
        raw[:, cols] = jnp.dot(near[...], inner_w[near_rows, cols], preferred_element_type=f32)
        return 0

    early = min(3, tiles)
    lax.fori_loop(0, early, first, 0)
    relay(0)
    lax.fori_loop(early, tiles, first, 0)
    raw[:, channels:] = jnp.dot(near[...], state_w[near_rows, :], preferred_element_type=f32)
    step_acc[...] = lax.dot_general(near[...], step_w[:, near_rows], across_rows, preferred_element_type=f32)
    for load in loads[4:13]:
        load.wait()

    def rounded(value):
        return value.astype(bf16).astype(f32)

    far = full.at[1 - chip]

    def project(at):
        for j in range(tiles):
            cols = slice(j * tile, (j + 1) * tile)
            more = jnp.dot(far[at, :], inner_w[far_rows, cols], preferred_element_type=f32)
            raw[at, cols] = rounded(raw[at, cols] + more)
        more = jnp.dot(far[at, :], state_w[far_rows, :], preferred_element_type=f32)
        raw[at, channels:] = rounded(raw[at, channels:] + more)
        more = lax.dot_general(far[at, :], step_w[:, far_rows], across_rows, preferred_element_type=f32)
        step_acc[at, :] += more

    t_row = lax.broadcasted_iota(jnp.int32, (ROWS, ROWS), 0)
    s_col = lax.broadcasted_iota(jnp.int32, (ROWS, ROWS), 1)
    causal = s_col <= t_row

    def mix_chunk(c, final):
        at = chunk_of(c)
        time_step = softplus(step_acc[at, :] + bias[...])
        decay = -time_step * rate[...]
        cum = jnp.dot(causal.astype(f32), decay, preferred_element_type=f32, precision=HIGHEST)
        ending = cum[ROWS - 1 :, :]
        tail = jnp.exp(ending - cum) * time_step
        cum_ref[at, :] = cum
        step_ref[at, :] = time_step
        ends[c] = jnp.broadcast_to(ending, ends.shape[1:])
        if final:
            total = ends[0]
            for k in range(1, chunks):
                total = total + ends[k]
            decay_out[...] = jnp.concatenate([total, jnp.zeros((8, 128 - heads), f32)], axis=1)
            for step in range(1, quarter):
                decay_copy((place + step) % quarter).start()
            decay_in[place] = decay_out[...]
        before = pl.ds(pl.multiple_of(jnp.maximum(c * ROWS - 8, 0), 8), 8)

        def conv(span, kernel):
            edge = jnp.where(c == 0, halo[:, span], raw[before, span])
            padded = jnp.concatenate([edge, raw[at, span]], axis=0)
            taps = kernel.shape[0]
            total = padded * kernel[taps - 1 : taps]
            for tap in range(taps - 1):
                total = total + pltpu.roll(padded, taps - 1 - tap, 0) * kernel[tap : tap + 1]
            return silu(total[8:]).astype(bf16)

        for p in range(2 * states // 128):
            span = slice(p * 128, (p + 1) * 128)
            bc_ref[at, span] = conv(slice(channels + p * 128, channels + (p + 1) * 128), conv_s[:, span])
        inject = bc_ref[at, :states]
        grown = jnp.exp(ending)
        for j in range(tiles):
            pieces = []
            for p in range(j * tile // 128, (j + 1) * tile // 128):
                span = slice(p * 128, (p + 1) * 128)
                x = conv(span, conv_i[:, span])
                x_ref[at, span] = x
                weight = per_head(tail, p * per_span, per_span, head_width, 128)
                pieces.append((x.astype(f32) * weight).astype(bf16))
            add = lax.dot_general(
                inject, jnp.concatenate(pieces, axis=1), (((0,), (0,)), ((), ())), preferred_element_type=f32
            )
            starts[c, j] = state[j].astype(bf16)
            weight = per_head(grown, j * heads_tile, heads_tile, head_width, tile)
            if final:
                state_out[j] = (state[j] * weight + add).astype(bf16)
                for step in range(1, quarter):
                    state_copy(j, (place + step) % quarter).start()
                owned[j, place] = state_out[j, share_of(place), :]
            else:
                state[j] = state[j] * weight + add

    def share_of(o):
        return pl.ds(pl.multiple_of(o * share, share), share)

    def at_place(o):
        return at_seq(side * quarter + o)

    def decay_copy(o):
        return remote(decay_out, decay_in.at[place], decay_send.at[o], decay_recv.at[place], at_place(o))

    def state_copy(j, o):
        return remote(
            state_out.at[j, share_of(o)], owned.at[j, place], state_send.at[j, o], state_recv.at[j, place], at_place(o)
        )

    def sums_copy(j):
        return remote(
            sums_out.at[j], sums_in.at[j], sums_send.at[j], sums_recv.at[j], at_seq((seq + quarter) % seq_count)
        )

    def back_copy(j, i):
        return remote(
            back.at[j, i], carried.at[j, share_of(place)], back_send.at[j, i], back_recv.at[j, place], at_place(i)
        )

    def combine(j):
        for step in range(1, quarter):
            o = (place + step) % quarter
            if j == 0:
                remote(decay_out, decay_in.at[o], decay_send.at[o], decay_recv.at[o], at_place(o)).wait_recv()
            remote(
                state_out.at[j, share_of(o)], owned.at[j, o], state_send.at[j, o], state_recv.at[j, o], at_place(o)
            ).wait_recv()
        run = owned[j, 0].astype(f32)
        parts_ref[j, 0] = jnp.zeros((share, tile), f32)
        for i in range(1, quarter):
            parts_ref[j, i] = run
            grown = per_head(jnp.exp(decay_in[i][:1, :]), j * heads_tile, heads_tile, head_width, tile)
            run = run * grown + owned[j, i].astype(f32)

        @pl.when(side == 0)
        def _():
            sums_out[j] = run.astype(bf16)
            sums_copy(j).start()
            give_back(j, None)

    def give_back(j, before):
        total = jnp.zeros((8, 128), f32)
        for i in range(quarter):
            value = parts_ref[j, i]
            if before is not None:
                value = value + before * per_head(
                    jnp.exp(total[:1, :]), j * heads_tile, heads_tile, head_width, tile
                )
                total = total + decay_in[i]
            back[j, i] = value.astype(bf16)
        for step in range(1, quarter):
            back_copy(j, (place + step) % quarter).start()
        carried[j, share_of(place), :] = back[j, place]

    def finalize(j):
        @pl.when(side == 1)
        def _():
            sums_copy(j).wait_recv()
            give_back(j, sums_in[j].astype(f32))

    def await_carried(j):
        for step in range(1, quarter):
            o = (place + step) % quarter
            remote(
                back.at[j, o], carried.at[j, share_of(o)], back_send.at[j, o], back_recv.at[j, o], at_place(o)
            ).wait_recv()

    state[...] = jnp.zeros_like(state)

    settle(0)
    end_rows = far[rows - 16 :, :]
    for j in range(tiles):
        cols = slice(j * tile, (j + 1) * tile)
        more = jnp.dot(end_rows, inner_w[far_rows, cols], preferred_element_type=f32)
        halo_out[:, cols] = rounded(raw[rows - 8 :, cols] + more[8:])
    more = jnp.dot(end_rows, state_w[far_rows, :], preferred_element_type=f32)
    halo_out[:, channels:] = rounded(raw[rows - 8 :, channels:] + more[8:])

    def to_next():
        return remote(halo_out, halo, halo_send, halo_recv, at_seq(jnp.minimum(seq + 1, seq_count - 1)))

    @pl.when(seq < seq_count - 1)
    def _():
        pl.semaphore_wait(ready, higher)
        to_next().start()

    @pl.when(seq == 0)
    def _():
        halo[...] = jnp.zeros_like(halo)

    last = chunks - 1
    relay(1)
    settle(1)
    project(chunk_of(0))
    relay(2)

    @pl.when(seq > 0)
    def _():
        remote(halo_out, halo, halo_send, halo_recv, at_seq(jnp.maximum(seq - 1, 0))).wait_recv()

    for c in range(1, last):
        mix_chunk(c - 1, False)
        settle(1 + c)
        project(chunk_of(c))
        relay(2 + c)
    mix_chunk(last - 1, False)
    settle(chunks)
    relay(chunks + 1)
    project(pl.ds(rows - ROWS, ROWS // 2))
    settle(chunks + 1)
    project(pl.ds(rows - ROWS // 2, ROWS // 2))
    mix_chunk(last, True)

    def inside(c, _):
        at = chunk_of(c)
        cum = cum_ref[at, :]
        eye = (t_row == s_col).astype(f32)
        flip = (((0,), (0,)), ((), ()))
        cum_t = lax.dot_general(cum, eye, flip, preferred_element_type=f32, precision=HIGHEST)
        step_t = lax.dot_general(step_ref[at, :], eye, flip, preferred_element_type=f32, precision=HIGHEST)
        readout = bc_ref[at, states:]
        scores = lax.dot_general(
            readout, bc_ref[at, :states], (((1,), (1,)), ((), ())), preferred_element_type=f32
        )
        scores = jnp.where(causal, scores, 0.0)
        grown = jnp.exp(cum)
        lane = lax.broadcasted_iota(jnp.int32, (ROWS, 128), 1)
        for p in range(spans):
            span = slice(p * 128, (p + 1) * 128)
            x = x_ref[at, span]
            mixes, parts = [], []
            for k in range(per_span):
                h = p * per_span + k
                gaps = jnp.minimum(cum[:, h : h + 1] - cum_t[h : h + 1, :], 0.0)
                mixes.append((scores * jnp.exp(gaps) * step_t[h : h + 1, :]).astype(bf16))
                own = (lane >= k * head_width) & (lane < (k + 1) * head_width)
                parts.append(jnp.where(own, x, jnp.zeros_like(x)))
            total = jnp.dot(
                jnp.concatenate(mixes, axis=1), jnp.concatenate(parts, axis=0), preferred_element_type=f32
            )
            lanes = slice(p * 128 % tile, p * 128 % tile + 128)
            reads = jnp.dot(readout, starts[c, p * 128 // tile, :, lanes], preferred_element_type=f32)
            weight = per_head(grown, p * per_span, per_span, head_width, 128)
            direct = per_head(skip[...], p * per_span, per_span, head_width, 128)
            y_ref[at, span] = total + reads * weight + direct * x.astype(f32)
        return 0

    loads[13].start()
    loads[14].start()
    lax.fori_loop(0, chunks - 2, inside, 0)
    loads[13].wait()

    def gate_tile(j, _):
        cols = tile_of(j, tile)
        value = jnp.dot(full[0], gate_w[:half, cols], preferred_element_type=f32)
        value = value + jnp.dot(full[1], gate_w[half:, cols], preferred_element_type=f32)
        gate_ref[:, cols] = silu(rounded(value))
        return 0

    base = jnp.minimum(seq, 0)

    def run(body, index):
        lax.fori_loop(base + index, base + index + 1, body, 0)

    steps = [(combine, 0), (combine, 1), (run, 0), (combine, 2), (combine, 3), (run, 1), (combine, 4), (run, 2)]
    steps += [(finalize, 0), (run, 3), (finalize, 1), (finalize, 2)]
    steps += [(None, chunks - 2), (finalize, 3), (run, 4), (finalize, 4), (None, chunks - 1)]
    for action, index in steps:
        if action is None:
            run(inside, index)
        elif index < tiles and action is run:
            run(gate_tile, index)
        elif index < tiles and action is combine:
            action(index)
        elif index < tiles:
            action(index)
    offset = jnp.zeros_like(ends[0])
    for c in range(chunks):
        reach[chunk_of(c), :] = jnp.exp(cum_ref[chunk_of(c), :] + offset[:1, :])
        offset = offset + ends[c]
    loads[14].wait()

    def gate_pair(b, j):
        cols = slice(j * tile, (j + 1) * tile)
        for k in range(2):
            at = chunk_of(b * 2 + k)
            reads = jnp.dot(bc_ref[at, states:], carried[j], preferred_element_type=f32)
            weight = per_head(reach[at, :], j * heads_tile, heads_tile, head_width, tile)
            g = (y_ref[at, cols] + reads * weight) * gate_ref[at, cols]
            squares = jnp.zeros((ROWS, 128), f32)
            for q in range(tile // 128):
                p = j * tile // 128 + q
                part = g[:, q * 128 : (q + 1) * 128]
                squares = squares + part * part
                gated[at, p * 128 : (p + 1) * 128] = (part * gain[p : p + 1, :]).astype(bf16)
            square_acc[k] = squares if j == 0 else square_acc[k] + squares

    def close_pair(b):
        for k in range(2):
            square_out[b * 2 + k] = lax.dot_general(
                jnp.ones((8, 128), f32), square_acc[k], across_rows,
                preferred_element_type=f32, precision=HIGHEST,
            )

    def square_copy(b):
        return remote(square_out.at[b], square_in.at[tp], sq_send.at[b], sq_recv.at[tp], at_tp(b))

    def pair_of(b):
        return tile_of(b, 2 * ROWS)

    for j in range(tiles):
        await_carried(j)
        gate_pair(1 - chip, j)
    diagonal = (1 - chip) * 2 + 1 - core

    def near_copy(p):
        return remote(near_out.at[p], near_in.at[p], near_send.at[p], near_recv.at[p], at_tp(mate))

    def far_copy(p):
        return remote(far_out.at[p], far_in.at[p], far_send.at[p], far_recv.at[p], at_tp(across))

    def own_copy(p):
        return remote(own_out.at[p], own_in.at[p], own_send.at[p], own_recv.at[p], at_tp(mate))

    def pass_on(p):
        near_copy(p).wait_recv()
        far_out[p] = (far_acc[p] + near_in[p].astype(f32)).astype(bf16)
        far_copy(p).start()

    def far_piece(p, _):
        cols = tile_of(p, piece)
        both[...] = jnp.dot(gated[pair_of(1 - chip), :], out_w[:, cols], preferred_element_type=f32)
        near_out[p] = both[chunk_of(1 - core), :].astype(bf16)
        near_copy(p).start()
        far_acc[p] = both[chunk_of(core), :]

        @pl.when(p > 0)
        def _():
            pass_on(jnp.maximum(p - 1, 0))

        return 0

    lax.fori_loop(base, base + 1, far_piece, 0)
    close_pair(1 - chip)
    square_copy(across).start()
    square_copy(diagonal).start()
    lax.fori_loop(1, PIECES, far_piece, 0)
    pass_on(PIECES - 1)
    for j in range(tiles):
        gate_pair(chip, j)
    close_pair(chip)
    square_copy(mate).start()

    def own_piece(p, _):
        cols = tile_of(p, piece)
        both[...] = jnp.dot(gated[pair_of(chip), :], out_w[:, cols], preferred_element_type=f32)
        own_out[p] = both[chunk_of(1 - core), :].astype(bf16)
        own_copy(p).start()
        own_acc[p] = both[chunk_of(core), :]
        return 0

    lax.fori_loop(0, PIECES, own_piece, 0)

    square = square_out[tp]
    for step in range(1, tp_count):
        source = (tp + step) % tp_count
        remote(square_out.at[0], square_in.at[source], sq_send.at[0], sq_recv.at[source], at_tp(source)).wait_recv()
        square = square + square_in[source]
    mean = square[:1, :] / (channels * tp_count)
    spread = jnp.broadcast_to(lax.rsqrt(mean + 1e-05), (ROWS, ROWS))
    scale = jnp.sum(jnp.where(t_row == s_col, spread, 0.0), axis=1, keepdims=True)

    def finish(p, _):
        own_copy(p).wait_recv()
        far_copy(p).wait_recv()
        total = own_acc[p] + own_in[p].astype(f32) + far_in[p].astype(f32)
        out_ref[:, tile_of(p, piece)] = (total * scale).astype(bf16)
        return 0

    lax.fori_loop(0, PIECES, finish, 0)

    for i in range(len(order)):
        crossing(i).wait_send()
        forwarded(i, mine).wait_send()
    beside(mine).wait_send()

    @pl.when(seq < seq_count - 1)
    def _():
        to_next().wait_send()

    for step in range(1, quarter):
        o = (place + step) % quarter
        decay_copy(o).wait_send()
        for j in range(tiles):
            state_copy(j, o).wait_send()
            back_copy(j, o).wait_send()
    @pl.when(side == 0)
    def _():
        for j in range(tiles):
            sums_copy(j).wait_send()

    for b in (across, diagonal, mate):
        square_copy(b).wait_send()
    for p in range(PIECES):
        near_copy(p).wait_send()
        far_copy(p).wait_send()
        own_copy(p).wait_send()


def fused(
    tokens, gate_weight, inner_weight, state_weight, step_weight, conv_inner, conv_state,
    step_bias, decay_rate, skip_gain, norm_gain, out_weight,
):
    rows, width = tokens.shape
    channels = inner_weight.shape[1]
    heads = step_weight.shape[1]
    if channels > 5 * 256 or rows < 3 * ROWS:
        return on_device(
            tokens, gate_weight, inner_weight, state_weight, step_weight, conv_inner, conv_state,
            step_bias, decay_rate, skip_gain, norm_gain, out_weight,
        )
    head_width = channels // heads
    states = state_weight.shape[1] // 2
    depth, out_width = inner_weight.shape[0], out_weight.shape[1]
    seq_count, tp_count = lax.axis_size("seq"), lax.axis_size("tp")
    chunks = rows // ROWS
    quarter = seq_count // 2
    share = states // quarter
    tile = min(256, channels)
    tiles = channels // tile
    arrivals = chunks + 2
    piece = out_width // PIECES
    f32, bf16 = jnp.float32, jnp.bfloat16
    dma, vmem = pltpu.SemaphoreType.DMA, pltpu.VMEM
    args = (
        tokens, gate_weight, inner_weight, state_weight, step_weight.T, conv_inner, conv_state,
        step_bias[None, :], decay_rate[None, :], skip_gain[None, :], norm_gain.reshape(-1, 128), out_weight,
    )
    scratch = [
        vmem((2, rows, 2 * width), bf16),
        vmem((depth, channels), bf16),
        vmem((depth, channels), bf16),
        vmem((depth, 2 * states), bf16),
        vmem((heads, depth), bf16),
        vmem(conv_inner.shape, f32),
        vmem(conv_state.shape, f32),
        vmem((1, heads), f32),
        vmem((1, heads), f32),
        vmem((1, heads), f32),
        vmem((channels // 128, 128), f32),
        vmem((channels, out_width), bf16),
        vmem((rows, channels + 2 * states), f32),
        vmem((8, channels + 2 * states), f32),
        vmem((8, channels + 2 * states), f32),
        vmem((rows, heads), f32),
        vmem((rows, channels), bf16),
        vmem((rows, 2 * states), bf16),
        vmem((rows, channels), f32),
        vmem((rows, channels), f32),
        vmem((rows, channels), bf16),
        vmem((rows, heads), f32),
        vmem((rows, heads), f32),
        vmem((rows, heads), f32),
        vmem((chunks, 8, heads), f32),
        vmem((tiles, states, tile), f32),
        vmem((chunks, tiles, states, tile), bf16),
        vmem((tiles, states, tile), bf16),
        vmem((tiles, quarter, share, tile), bf16),
        vmem((tiles, quarter, share, tile), f32),
        vmem((tiles, share, tile), bf16),
        vmem((tiles, share, tile), bf16),
        vmem((tiles, quarter, share, tile), bf16),
        vmem((tiles, states, tile), bf16),
        vmem((8, 128), f32),
        vmem((quarter, 8, 128), f32),
        vmem((2, ROWS, 128), f32),
        vmem((tp_count, 8, ROWS), f32),
        vmem((tp_count, 8, ROWS), f32),
    ]
    half_sums = vmem((PIECES, ROWS, piece), bf16)
    whole_sums = vmem((PIECES, ROWS, piece), f32)
    scratch += [half_sums, half_sums, whole_sums, half_sums, half_sums, half_sums, half_sums, whole_sums]
    scratch += [vmem((2 * ROWS, piece), f32)]
    scratch += [pltpu.SemaphoreType.REGULAR, dma((15,))] + [dma((arrivals,))] * 4 + [dma] * 4
    scratch += [dma((tiles, quarter))] * 4 + [dma((quarter,))] * 2 + [dma((tiles,))] * 2
    scratch += [dma((tp_count,))] * 2 + [dma((PIECES,))] * 6
    anywhere = pl.BlockSpec(memory_space=pl.ANY)
    return pl.pallas_call(
        lambda *refs: layer_kernel(head_width, *refs),
        out_shape=pltpu.VMEM((rows // tp_count, out_width), bf16),
        in_specs=[anywhere] * len(args),
        out_specs=pl.BlockSpec(memory_space=pltpu.VMEM),
        scratch_shapes=scratch,
        compiler_params=pltpu.CompilerParams(
            collective_id=0, has_side_effects=True, vmem_limit_bytes=VMEM_LIMIT
        ),
        name="layer",
    )(*args)


def on_device(
    tokens,
    gate_weight,
    inner_weight,
    state_weight,
    step_weight,
    conv_inner,
    conv_state,
    step_bias,
    decay_rate,
    skip_gain,
    norm_gain,
    out_weight,
):
    tok_rows = tokens.shape[0]
    width_inner = inner_weight.shape[1]
    head_count = step_weight.shape[1]
    head_width = width_inner // head_count
    state_size = state_weight.shape[1] // 2
    blocks = tok_rows // GROUP
    size_tp = lax.axis_size("tp")
    me = lax.axis_index("tp")

    chunks = [None] * blocks
    for b in range(blocks - 1, -1, -1):
        chunks[b] = gather_features(tokens[b * GROUP : (b + 1) * GROUP])
    halo = shifted(chunks[-1][GROUP - HALO :], 1)
    chunks[0] = jnp.concatenate([halo, chunks[0]], axis=0)

    inner_raw, state_raw, step_raw = [None] * blocks, [None] * blocks, [None] * blocks
    for b in range(blocks - 1, -1, -1):
        i_b, s_b, t_b = project(chunks[b], inner_weight, state_weight, step_weight)
        inner_raw[b], state_raw[b] = i_b.astype(jnp.bfloat16), s_b.astype(jnp.bfloat16)
        step_raw[b] = t_b[HALO:] if b == 0 else t_b

    lanes = max(128, head_width)
    time_step = jax.nn.softplus(jnp.concatenate(step_raw, axis=0) + step_bias[None, :])
    log_decay = -time_step * decay_rate[None, :]
    grouped = log_decay.reshape(blocks, GROUP, head_count)
    cumulative = jnp.cumsum(grouped, axis=1)
    ending = cumulative[:, -1]
    tail = (jnp.exp(ending[:, None] - cumulative)).reshape(tok_rows, head_count) * time_step
    cumulative = cumulative.reshape(tok_rows, head_count)

    def cost(flops, count, exps):
        return pl.CostEstimate(flops=flops, bytes_accessed=count, transcendentals=exps)

    whole = tok_rows * width_inner
    x, bc, contribution = pl.pallas_call(
        lambda *refs: conv_kernel(blocks, head_width, lanes, *refs),
        out_shape=(
            jax.ShapeDtypeStruct((tok_rows, width_inner), jnp.bfloat16),
            jax.ShapeDtypeStruct((tok_rows, 2 * state_size), jnp.bfloat16),
            jax.ShapeDtypeStruct((blocks, width_inner, state_size), jnp.float32),
        ),
        cost_estimate=cost(2 * whole * state_size, 6 * whole, whole),
        name="conv",
    )(*inner_raw, *state_raw, conv_inner, conv_state, tail)
    contribution = contribution.reshape(blocks, head_count, head_width, state_size)
    local_state = jnp.zeros((head_count, head_width, state_size), jnp.float32)
    for b in range(blocks):
        local_state = jnp.exp(ending[b])[:, None, None] * local_state + contribution[b]

    def by_rows(width):
        return pl.BlockSpec((GROUP, width), lambda b: (b, 0))

    def by_columns(height):
        return pl.BlockSpec((height, GROUP), lambda b: (0, b))

    def fixed(width):
        return pl.BlockSpec((1, width), lambda b: (0, 0))

    intra = pl.pallas_call(
        lambda *refs: intra_kernel(head_width, lanes, *refs),
        grid=(blocks,),
        in_specs=[
            by_rows(width_inner),
            by_rows(2 * state_size),
            by_rows(head_count),
            by_columns(head_count),
            by_columns(head_count),
            fixed(width_inner),
        ],
        out_specs=by_rows(width_inner),
        out_shape=jax.ShapeDtypeStruct((tok_rows, width_inner), jnp.float32),
        cost_estimate=cost(4 * whole * GROUP, 6 * whole, GROUP * tok_rows * head_count),
        name="intra",
    )(x, bc, cumulative, cumulative.T, time_step.T, jnp.repeat(skip_gain, head_width)[None, :])

    gate = jnp.concatenate(
        [
            jnp.dot(c[c.shape[0] - GROUP :], gate_weight, preferred_element_type=jnp.float32).astype(jnp.bfloat16)
            for c in chunks
        ],
        axis=0,
    )

    carried, intra = earlier_state(
        local_state.astype(jnp.bfloat16).reshape(width_inner, state_size),
        jnp.sum(ending, axis=0),
        head_width,
        intra,
    )
    carried = carried.astype(jnp.float32).reshape(head_count, head_width, state_size)
    states = []
    for b in range(blocks):
        states.append(carried.astype(jnp.bfloat16).reshape(1, width_inner, state_size))
        carried = jnp.exp(ending[b])[:, None, None] * carried + contribution[b]

    gated, squares = pl.pallas_call(
        lambda *refs: gate_kernel(head_width, lanes, *refs),
        grid=(blocks,),
        in_specs=[
            by_rows(width_inner),
            by_rows(2 * state_size),
            by_rows(head_count),
            by_rows(width_inner),
            fixed(width_inner),
            pl.BlockSpec((1, width_inner, state_size), lambda b: (b, 0, 0)),
        ],
        out_specs=(by_rows(width_inner), by_rows(1)),
        out_shape=(
            jax.ShapeDtypeStruct((tok_rows, width_inner), jnp.bfloat16),
            jax.ShapeDtypeStruct((tok_rows, 1), jnp.float32),
        ),
        cost_estimate=cost(2 * whole * state_size, 8 * whole, whole),
        name="gate",
    )(intra, bc, cumulative, gate, norm_gain[None, :], jnp.concatenate(states, axis=0))

    square_total = sum_over_tp(squares[:, 0])
    share = tok_rows // size_tp
    mean_square = lax.dynamic_slice(square_total, (me * share,), (share,)) / (width_inner * size_tp)
    scale = lax.rsqrt(mean_square + 1e-05)[:, None]

    if size_tp != 4:
        part = jnp.dot(gated, out_weight, preferred_element_type=jnp.float32).astype(jnp.bfloat16)
        total = lax.psum_scatter(part, "tp", scatter_dimension=0, tiled=True)
        return (total.astype(jnp.float32) * scale).astype(jnp.bfloat16)

    side = me // 2

    def reduced(chip, weight):
        rows = lax.dynamic_slice(gated, (chip * 2 * share, 0), (2 * share, width_inner))
        both = jnp.dot(rows, weight, preferred_element_type=jnp.float32).astype(jnp.bfloat16)
        shape = (share, weight.shape[1])
        away = lax.dynamic_slice(both, ((1 - me % 2) * share, 0), shape)
        own = lax.dynamic_slice(both, ((me % 2) * share, 0), shape)
        return own.astype(jnp.float32) + swapped(away, 1).astype(jnp.float32)

    cuts = 2
    width_out = out_weight.shape[1] // cuts
    weights = [out_weight[:, c * width_out : (c + 1) * width_out] for c in range(cuts)]
    arrived = [swapped(reduced(side ^ 1, w).astype(jnp.bfloat16), 2) for w in weights]
    results = []
    for w, other in zip(weights, arrived):
        total = reduced(side, w) + other.astype(jnp.float32)
        results.append((total * scale).astype(jnp.bfloat16))
    return jnp.concatenate(results, axis=1)


def solution(mesh):
    in_specs = (
        P("seq", "tp"),
        P(None, "tp"),
        P(None, "tp"),
        P(),
        P(None, "tp"),
        P(None, "tp"),
        P(),
        P("tp"),
        P("tp"),
        P("tp"),
        P("tp"),
        P("tp", None),
    )
    out_specs = P(("seq", "tp"), None)
    quick = mesh.shape["tp"] == 4 and mesh.shape["seq"] == 8
    return jax.shard_map(
        fused if quick else on_device, mesh=mesh, in_specs=in_specs, out_specs=out_specs, check_vma=False
    )
```

```python
import jax
import jax.numpy as jnp
from jax import lax
from jax.experimental import pallas as pl
from jax.experimental.pallas import tpu as pltpu
from jax.sharding import PartitionSpec as P

GROUP = 256
HALO = 16


def swapped(shard, by):
    size = lax.axis_size("tp")
    return lax.ppermute(shard, "tp", [(i, i ^ by) for i in range(size)])


def shifted(shard, by):
    size = lax.axis_size("seq")
    return lax.ppermute(shard, "seq", [(i, i + by) for i in range(size - by)])


def gather_features(rows):
    size = lax.axis_size("tp")
    me = lax.axis_index("tp")
    width = rows.shape[1]
    held = [(0, rows)]
    step = size // 2
    while step >= 1:
        held = held + [(code ^ step, swapped(part, step)) for code, part in held]
        step //= 2
    parts = dict(held)
    full = jnp.zeros((rows.shape[0], width * size), rows.dtype)
    for code in range(size):
        full = lax.dynamic_update_slice(full, parts[code], (0, (me ^ code) * width))
    return full


def sum_over_tp(part):
    size = lax.axis_size("tp")
    step = 1
    while step < size:
        part = part + swapped(part, step)
        step *= 2
    return part


def prefix_kernel(mine_ref, decay_ref, owner_ref, out_ref):
    owner = owner_ref[...]
    carried = jnp.zeros(mine_ref.shape[1:], jnp.float32)
    for i in range(mine_ref.shape[0]):
        out_ref[i] = carried.astype(jnp.bfloat16)
        log_row = jnp.sum(owner * decay_ref[i : i + 1, :], axis=1, keepdims=True)
        carried = carried * jnp.exp(log_row) + mine_ref[i].astype(jnp.float32)


def earlier_state(local_state, decay_total, head_width, cover):
    size = lax.axis_size("seq")
    rows, states = local_state.shape
    share = rows // size
    me = lax.axis_index("seq")
    heads = decay_total.shape[0]
    wide = jnp.pad(decay_total, (0, -heads % 128))
    wide = jnp.broadcast_to(wide[None, None, :], (size, 1, wide.shape[0]))
    decay_all = lax.all_to_all(wide, "seq", 0, 0, tiled=True)[:, 0, :heads]
    blocks = local_state.reshape(size, share, states)
    blocks, decay_all = lax.optimization_barrier((blocks, decay_all))
    mine = lax.all_to_all(blocks, "seq", 0, 0, tiled=True)
    mine, cover = lax.optimization_barrier((mine, cover))
    row_head = (me * share + jnp.arange(share)) // head_width
    owner = (row_head[:, None] == jnp.arange(decay_total.shape[0])[None, :]).astype(jnp.float32)
    prefixes = pl.pallas_call(
        prefix_kernel,
        out_shape=jax.ShapeDtypeStruct(mine.shape, jnp.bfloat16),
        cost_estimate=pl.CostEstimate(flops=0, bytes_accessed=4 * mine.size, transcendentals=0),
    )(mine, decay_all, owner)
    return lax.all_to_all(prefixes, "seq", 0, 0, tiled=True).reshape(rows, states), cover


def per_head(table, first, count, width, lanes):
    lane = lax.broadcasted_iota(jnp.int32, (table.shape[0], lanes), 1)
    spread = jnp.broadcast_to(table[:, first : first + 1], (table.shape[0], lanes))
    for k in range(1, count):
        spread = jnp.where(lane >= k * width, table[:, first + k : first + k + 1], spread)
    return spread


def silu(value):
    return value * (0.5 * jnp.tanh(0.5 * value) + 0.5)


def conv_kernel(blocks, head_width, lanes, *refs):
    inner_refs, state_refs = refs[:blocks], refs[blocks : 2 * blocks]
    tap_inner, tap_state, tail_ref = refs[2 * blocks : 2 * blocks + 3]
    x_ref, bc_ref, contribution_ref = refs[2 * blocks + 3 :]
    taps = tap_inner.shape[0]
    heads_per = lanes // head_width

    def mixed(chunk_refs, b, span, kernel):
        if b == 0:
            padded = chunk_refs[0][:, span].astype(jnp.float32)
        else:
            last = chunk_refs[b - 1].shape[0] - HALO
            edge = chunk_refs[b - 1][last:, span].astype(jnp.float32)
            padded = jnp.concatenate([edge, chunk_refs[b][:, span].astype(jnp.float32)], axis=0)
        total = padded * kernel[taps - 1 : taps]
        for tap in range(taps - 1):
            total = total + pltpu.roll(padded, taps - 1 - tap, 0) * kernel[tap : tap + 1]
        return silu(total[HALO:]).astype(jnp.bfloat16)

    for b in range(blocks):
        rows = slice(b * GROUP, (b + 1) * GROUP)
        bc = mixed(state_refs, b, slice(None), tap_state[...])
        bc_ref[rows] = bc
        inject = bc[:, : bc.shape[1] // 2]
        tail = tail_ref[rows]
        for p in range(x_ref.shape[1] // lanes):
            span = slice(p * lanes, (p + 1) * lanes)
            x = mixed(inner_refs, b, span, tap_inner[:, span])
            x_ref[rows, span] = x
            weight = per_head(tail, p * heads_per, heads_per, head_width, lanes)
            scaled = (x.astype(jnp.float32) * weight).astype(jnp.bfloat16)
            contribution_ref[b, span] = lax.dot_general(
                scaled, inject, (((0,), (0,)), ((), ())), preferred_element_type=jnp.float32
            )


def intra_kernel(head_width, lanes, x_ref, bc_ref, cum_ref, cum_t_ref, step_t_ref, skip_ref, out_ref):
    states = bc_ref.shape[1] // 2
    heads_per = lanes // head_width
    scores = lax.dot_general(
        bc_ref[:, states:], bc_ref[:, :states], (((1,), (1,)), ((), ())),
        preferred_element_type=jnp.float32,
    )
    t = lax.broadcasted_iota(jnp.int32, scores.shape, 0)
    s = lax.broadcasted_iota(jnp.int32, scores.shape, 1)
    scores = jnp.where(s <= t, scores, 0.0)
    lane = lax.broadcasted_iota(jnp.int32, (x_ref.shape[0], lanes), 1)
    for p in range(x_ref.shape[1] // lanes):
        span = slice(p * lanes, (p + 1) * lanes)
        x = x_ref[:, span]
        total = None
        for k in range(heads_per):
            h = p * heads_per + k
            gaps = jnp.minimum(cum_ref[:, h : h + 1] - cum_t_ref[h : h + 1, :], 0.0)
            mixing = (scores * jnp.exp(gaps) * step_t_ref[h : h + 1, :]).astype(jnp.bfloat16)
            part = jnp.dot(mixing, x, preferred_element_type=jnp.float32)
            total = part if k == 0 else jnp.where(lane >= k * head_width, part, total)
        out_ref[:, span] = total + skip_ref[:, span] * x.astype(jnp.float32)


def gate_kernel(head_width, lanes, intra_ref, bc_ref, cum_ref, gate_ref, gain_ref, state_ref, out_ref, square_ref):
    states = bc_ref.shape[1] // 2
    heads_per = lanes // head_width
    readout = bc_ref[:, states:]
    grown = jnp.exp(cum_ref[...])
    squares = jnp.zeros((readout.shape[0], lanes), jnp.float32)
    for p in range(intra_ref.shape[1] // lanes):
        span = slice(p * lanes, (p + 1) * lanes)
        reads = lax.dot_general(
            readout, state_ref[0, span], (((1,), (1,)), ((), ())), preferred_element_type=jnp.float32
        )
        weight = per_head(grown, p * heads_per, heads_per, head_width, lanes)
        g = (intra_ref[:, span] + reads * weight) * silu(gate_ref[:, span].astype(jnp.float32))
        squares = squares + g * g
        out_ref[:, span] = (g * gain_ref[:, span]).astype(jnp.bfloat16)
    square_ref[...] = jnp.sum(squares, axis=1, keepdims=True)


def project(rows, *weights):
    return [jnp.dot(rows, weight, preferred_element_type=jnp.float32) for weight in weights]


ROWS = 128
PIECES = 10
VMEM_LIMIT = 56 * 1024 * 1024
MESH = pl.DeviceIdType.MESH
HIGHEST = lax.Precision.HIGHEST


def softplus(value):
    return jnp.maximum(value, 0.0) + jnp.log1p(jnp.exp(-jnp.abs(value)))


def chunk_of(index):
    return pl.ds(pl.multiple_of(index * ROWS, ROWS), ROWS)


def tile_of(index, width):
    return pl.ds(pl.multiple_of(index * width, width), width)


def layer_kernel(
    head_width,
    tok_in, gate_in, inner_in, statew_in, stepw_in, convi_in, convs_in, bias_in, rate_in, skip_in, gain_in, outw_in,
    out_ref,
    full, gate_w, inner_w, state_w, step_w, conv_i, conv_s, bias, rate, skip, gain, out_w,
    raw, halo, halo_out, step_acc, x_ref, bc_ref, y_ref, gate_ref, gated,
    cum_ref, step_ref, reach, ends, state, starts, state_out, owned, parts_ref, sums_out, sums_in, back, carried,
    decay_out, decay_in, square_acc,
    square_out, square_in, near_out, near_in, far_acc, far_out, far_in, own_out, own_in, own_acc, both,
    ready, local_sem, x_send, x_recv, f_send, f_recv, d_send, d_recv, halo_send, halo_recv,
    state_send, state_recv, back_send, back_recv, decay_send, decay_recv, sums_send, sums_recv,
    sq_send, sq_recv, near_send, near_recv, far_send, far_recv, own_send, own_recv,
):
    seq_count, tp_count = lax.axis_size("seq"), lax.axis_size("tp")
    seq, tp = lax.axis_index("seq"), lax.axis_index("tp")
    chip, core = tp // 2, tp % 2
    mate, across = chip * 2 + 1 - core, (1 - chip) * 2 + core
    rows, half = full.shape[1], full.shape[2]
    width = half // 2
    channels = inner_w.shape[1]
    states = state_w.shape[1] // 2
    heads = step_w.shape[0]
    chunks = rows // ROWS
    tile = min(256, channels)
    tiles = channels // tile
    spans = channels // 128
    per_span = 128 // head_width
    quarter = seq_count // 2
    side, place = seq // quarter, seq % quarter
    share = states // quarter
    heads_tile = tile // head_width
    piece = out_w.shape[1] // PIECES
    f32, bf16 = jnp.float32, jnp.bfloat16
    across_rows = (((1,), (1,)), ((), ()))

    def at_tp(index):
        return {"seq": seq, "tp": index}

    def at_seq(index):
        return {"seq": index, "tp": tp}

    def remote(src, dst, send, recv, device):
        return pltpu.make_async_remote_copy(
            src_ref=src, dst_ref=dst, send_sem=send, recv_sem=recv, device_id=device, device_id_type=MESH
        )

    barrier = pltpu.get_barrier_semaphore()
    for step in range(1, tp_count):
        pl.semaphore_signal(barrier, inc=1, device_id=at_tp((tp + step) % tp_count), device_id_type=MESH)
    def related(low, high):
        return (low < high) & ((low // quarter == high // quarter) | (high == low + quarter) | (high == low + 1))

    for d in range(seq_count):

        @pl.when(related(seq, d))
        def _():
            pl.semaphore_signal(barrier, inc=1, device_id=at_seq(d), device_id_type=MESH)

    lower = sum(jnp.where(related(d, seq), 1, 0) for d in range(seq_count))
    higher = sum(jnp.where(related(seq, d), 1, 0) for d in range(seq_count))

    mine = pl.ds(pl.multiple_of(core * width, width), width)
    theirs = pl.ds(pl.multiple_of((1 - core) * width, width), width)
    near_rows = pl.ds(pl.multiple_of(chip * half, half), half)
    far_rows = pl.ds(pl.multiple_of((1 - chip) * half, half), half)
    loads = [
        (tok_in, full.at[chip, :, mine]),
        (inner_in.at[near_rows], inner_w.at[near_rows]),
        (statew_in.at[near_rows], state_w.at[near_rows]),
        (stepw_in.at[:, near_rows], step_w.at[:, near_rows]),
        (inner_in.at[far_rows], inner_w.at[far_rows]),
        (statew_in.at[far_rows], state_w.at[far_rows]),
        (stepw_in.at[:, far_rows], step_w.at[:, far_rows]),
        (convi_in, conv_i),
        (convs_in, conv_s),
        (bias_in, bias),
        (rate_in, rate),
        (skip_in, skip),
        (gain_in, gain),
        (gate_in, gate_w),
        (outw_in, out_w),
    ]
    loads = [pltpu.make_async_copy(src, dst, local_sem.at[i]) for i, (src, dst) in enumerate(loads)]
    for load in loads:
        load.start()
    loads[0].wait()
    pl.semaphore_wait(barrier, tp_count - 1 + lower)
    for d in range(seq_count):

        @pl.when(related(d, seq))
        def _():
            pl.semaphore_signal(ready, inc=1, device_id=at_seq(d), device_id_type=MESH)


    order = [(rows - 16, 16)] + [(c * ROWS, ROWS) for c in range(chunks - 1)]
    order += [(rows - ROWS, ROWS // 2), (rows - ROWS // 2, ROWS // 2 - 16)]

    def crossing(i):
        part = full.at[chip, pl.ds(*order[i]), mine]
        return remote(part, part, x_send, x_recv.at[i], at_tp(across))

    def beside(columns):
        part = full.at[chip, :, columns]
        return remote(part, part, d_send, d_recv, at_tp(mate))

    def forwarded(i, columns):
        part = full.at[1 - chip, pl.ds(*order[i]), columns]
        return remote(part, part, f_send, f_recv.at[i], at_tp(mate))

    def relay(i):
        part = full.at[1 - chip, pl.ds(*order[i]), mine]
        remote(part, part, x_send, x_recv.at[i], at_tp(across)).wait_recv()
        forwarded(i, mine).start()

    def settle(i):
        forwarded(i, theirs).wait_recv()

    for i in range(len(order)):
        crossing(i).start()
    beside(mine).start()

    for load in loads[1:4]:
        load.wait()
    beside(theirs).wait_recv()

    near = full.at[chip]

    def first(j, _):
        cols = tile_of(j, tile)
        raw[:, cols] = jnp.dot(near[...], inner_w[near_rows, cols], preferred_element_type=f32)
        return 0

    early = min(3, tiles)
    lax.fori_loop(0, early, first, 0)
    relay(0)
    lax.fori_loop(early, tiles, first, 0)
    raw[:, channels:] = jnp.dot(near[...], state_w[near_rows, :], preferred_element_type=f32)
    step_acc[...] = lax.dot_general(near[...], step_w[:, near_rows], across_rows, preferred_element_type=f32)
    for load in loads[4:13]:
        load.wait()

    def rounded(value):
        return value.astype(bf16).astype(f32)

    far = full.at[1 - chip]

    def project(at):
        for j in range(tiles):
            cols = slice(j * tile, (j + 1) * tile)
            more = jnp.dot(far[at, :], inner_w[far_rows, cols], preferred_element_type=f32)
            raw[at, cols] = rounded(raw[at, cols] + more)
        more = jnp.dot(far[at, :], state_w[far_rows, :], preferred_element_type=f32)
        raw[at, channels:] = rounded(raw[at, channels:] + more)
        more = lax.dot_general(far[at, :], step_w[:, far_rows], across_rows, preferred_element_type=f32)
        step_acc[at, :] += more

    t_row = lax.broadcasted_iota(jnp.int32, (ROWS, ROWS), 0)
    s_col = lax.broadcasted_iota(jnp.int32, (ROWS, ROWS), 1)
    causal = s_col <= t_row

    def mix_chunk(c, final):
        at = chunk_of(c)
        time_step = softplus(step_acc[at, :] + bias[...])
        decay = -time_step * rate[...]
        cum = jnp.dot(causal.astype(f32), decay, preferred_element_type=f32, precision=HIGHEST)
        ending = cum[ROWS - 1 :, :]
        tail = jnp.exp(ending - cum) * time_step
        cum_ref[at, :] = cum
        step_ref[at, :] = time_step
        ends[c] = jnp.broadcast_to(ending, ends.shape[1:])
        if final:
            total = ends[0]
            for k in range(1, chunks):
                total = total + ends[k]
            decay_out[...] = jnp.concatenate([total, jnp.zeros((8, 128 - heads), f32)], axis=1)
            for step in range(1, quarter):
                decay_copy((place + step) % quarter).start()
            decay_in[place] = decay_out[...]
        before = pl.ds(pl.multiple_of(jnp.maximum(c * ROWS - 8, 0), 8), 8)

        def conv(span, kernel):
            edge = jnp.where(c == 0, halo[:, span], raw[before, span])
            padded = jnp.concatenate([edge, raw[at, span]], axis=0)
            taps = kernel.shape[0]
            total = padded * kernel[taps - 1 : taps]
            for tap in range(taps - 1):
                total = total + pltpu.roll(padded, taps - 1 - tap, 0) * kernel[tap : tap + 1]
            return silu(total[8:]).astype(bf16)

        for p in range(2 * states // 128):
            span = slice(p * 128, (p + 1) * 128)
            bc_ref[at, span] = conv(slice(channels + p * 128, channels + (p + 1) * 128), conv_s[:, span])
        inject = bc_ref[at, :states]
        grown = jnp.exp(ending)
        waiting = []
        for j in range(tiles):
            pieces = []
            for p in range(j * tile // 128, (j + 1) * tile // 128):
                span = slice(p * 128, (p + 1) * 128)
                x = conv(span, conv_i[:, span])
                x_ref[at, span] = x
                weight = per_head(tail, p * per_span, per_span, head_width, 128)
                pieces.append((x.astype(f32) * weight).astype(bf16))
            add = lax.dot_general(
                inject, jnp.concatenate(pieces, axis=1), (((0,), (0,)), ((), ())), preferred_element_type=f32
            )
            starts[c, j] = state[j].astype(bf16)
            weight = per_head(grown, j * heads_tile, heads_tile, head_width, tile)
            if final:
                state_out[j] = (state[j] * weight + add).astype(bf16)
                waiting.append(j)
                if j in (1, tiles - 1):
                    for k in waiting:
                        for step in range(1, quarter):
                            state_copy(k, (place + step) % quarter).start()
                        owned[k, place] = state_out[k, share_of(place), :]
                    waiting.clear()
            else:
                state[j] = state[j] * weight + add

    def share_of(o):
        return pl.ds(pl.multiple_of(o * share, share), share)

    def at_place(o):
        return at_seq(side * quarter + o)

    def decay_copy(o):
        return remote(decay_out, decay_in.at[place], decay_send, decay_recv, at_place(o))

    def state_copy(j, o):
        return remote(
            state_out.at[j, share_of(o)], owned.at[j, place], state_send, state_recv.at[j], at_place(o)
        )

    def sums_copy(j):
        return remote(
            sums_out.at[j], sums_in.at[j], sums_send, sums_recv.at[j], at_seq((seq + quarter) % seq_count)
        )

    def back_copy(j, i):
        return remote(
            back.at[j, i], carried.at[j, share_of(place)], back_send, back_recv.at[j], at_place(i)
        )

    others = pl.ds(0, quarter - 1)

    def every(ref, send, recv):
        return remote(ref, ref, send, recv, at_tp(mate))

    def combine(j):
        if j == 0:
            every(decay_in.at[others], decay_send, decay_recv).wait_recv()
        every(owned.at[j, others], state_send, state_recv.at[j]).wait_recv()
        run = owned[j, 0].astype(f32)
        parts_ref[j, 0] = jnp.zeros((share, tile), f32)
        for i in range(1, quarter):
            parts_ref[j, i] = run
            grown = per_head(jnp.exp(decay_in[i][:1, :]), j * heads_tile, heads_tile, head_width, tile)
            run = run * grown + owned[j, i].astype(f32)

        @pl.when(side == 0)
        def _():
            sums_out[j] = run.astype(bf16)
            sums_copy(j).start()
            give_back(j, None)

    def give_back(j, before):
        total = jnp.zeros((8, 128), f32)
        for i in range(quarter):
            value = parts_ref[j, i]
            if before is not None:
                value = value + before * per_head(
                    jnp.exp(total[:1, :]), j * heads_tile, heads_tile, head_width, tile
                )
                total = total + decay_in[i]
            back[j, i] = value.astype(bf16)
        for step in range(1, quarter):
            back_copy(j, (place + step) % quarter).start()
        carried[j, share_of(place), :] = back[j, place]

    def finalize(j):
        @pl.when(side == 1)
        def _():
            sums_copy(j).wait_recv()
            give_back(j, sums_in[j].astype(f32))

    def await_carried(j):
        every(back.at[j, others], back_send, back_recv.at[j]).wait_recv()

    state[...] = jnp.zeros_like(state)

    settle(0)
    end_rows = far[rows - 16 :, :]
    for j in range(tiles):
        cols = slice(j * tile, (j + 1) * tile)
        more = jnp.dot(end_rows, inner_w[far_rows, cols], preferred_element_type=f32)
        halo_out[:, cols] = rounded(raw[rows - 8 :, cols] + more[8:])
    more = jnp.dot(end_rows, state_w[far_rows, :], preferred_element_type=f32)
    halo_out[:, channels:] = rounded(raw[rows - 8 :, channels:] + more[8:])

    def to_next():
        return remote(halo_out, halo, halo_send, halo_recv, at_seq(jnp.minimum(seq + 1, seq_count - 1)))

    @pl.when(seq < seq_count - 1)
    def _():
        pl.semaphore_wait(ready, higher)
        to_next().start()

    @pl.when(seq == 0)
    def _():
        halo[...] = jnp.zeros_like(halo)

    last = chunks - 1
    relay(1)
    loads[13].wait()

    def gate_near(j, _):
        cols = tile_of(j, tile)
        gate_ref[:, cols] = jnp.dot(near[...], gate_w[near_rows, cols], preferred_element_type=f32)
        return 0

    few = min(2, tiles)
    lax.fori_loop(0, few, gate_near, 0)
    settle(1)
    project(chunk_of(0))
    lax.fori_loop(few, tiles, gate_near, 0)
    relay(2)

    @pl.when(seq > 0)
    def _():
        remote(halo_out, halo, halo_send, halo_recv, at_seq(jnp.maximum(seq - 1, 0))).wait_recv()

    for c in range(1, last):
        mix_chunk(c - 1, False)
        settle(1 + c)
        project(chunk_of(c))
        relay(2 + c)
    mix_chunk(last - 1, False)
    settle(chunks)
    relay(chunks + 1)
    project(pl.ds(rows - ROWS, ROWS // 2))
    settle(chunks + 1)
    project(pl.ds(rows - ROWS // 2, ROWS // 2))
    mix_chunk(last, True)

    def inside(c, _):
        at = chunk_of(c)
        cum = cum_ref[at, :]
        eye = (t_row == s_col).astype(f32)
        flip = (((0,), (0,)), ((), ()))
        cum_t = lax.dot_general(cum, eye, flip, preferred_element_type=f32, precision=HIGHEST)
        step_t = lax.dot_general(step_ref[at, :], eye, flip, preferred_element_type=f32, precision=HIGHEST)
        readout = bc_ref[at, states:]
        scores = lax.dot_general(
            readout, bc_ref[at, :states], (((1,), (1,)), ((), ())), preferred_element_type=f32
        )
        scores = jnp.where(causal, scores, 0.0)
        grown = jnp.exp(cum)
        lane = lax.broadcasted_iota(jnp.int32, (ROWS, 128), 1)
        for p in range(spans):
            span = slice(p * 128, (p + 1) * 128)
            x = x_ref[at, span]
            mixes, parts = [], []
            for k in range(per_span):
                h = p * per_span + k
                gaps = jnp.minimum(cum[:, h : h + 1] - cum_t[h : h + 1, :], 0.0)
                mixes.append((scores * jnp.exp(gaps) * step_t[h : h + 1, :]).astype(bf16))
                own = (lane >= k * head_width) & (lane < (k + 1) * head_width)
                parts.append(jnp.where(own, x, jnp.zeros_like(x)))
            total = jnp.dot(
                jnp.concatenate(mixes, axis=1), jnp.concatenate(parts, axis=0), preferred_element_type=f32
            )
            lanes = slice(p * 128 % tile, p * 128 % tile + 128)
            reads = jnp.dot(readout, starts[c, p * 128 // tile, :, lanes], preferred_element_type=f32)
            weight = per_head(grown, p * per_span, per_span, head_width, 128)
            direct = per_head(skip[...], p * per_span, per_span, head_width, 128)
            y_ref[at, span] = total + reads * weight + direct * x.astype(f32)
        return 0

    def gate_tile(j, _):
        cols = tile_of(j, tile)
        more = jnp.dot(far[...], gate_w[far_rows, cols], preferred_element_type=f32)
        gate_ref[:, cols] = silu(rounded(gate_ref[:, cols] + more))
        return 0

    base = jnp.minimum(seq, 0)

    def run(body, index):
        lax.fori_loop(base + index, base + index + 1, body, 0)

    steps = [(None, 0), (None, 1), (run, 0), (run, 1)] + [(combine, j) for j in range(3)]
    steps += [(run, 2), (combine, 3), (combine, 4), (run, 3), (finalize, 0), (run, 4), (finalize, 1), (finalize, 2)]
    steps += [(None, chunk) for chunk in range(2, chunks - 1)]
    steps += [(finalize, 3), (finalize, 4), (None, chunks - 1)]
    for action, index in steps:
        if action is None:
            run(inside, index)
        elif index < tiles and action is run:
            run(gate_tile, index)
        elif index < tiles and action is combine:
            action(index)
        elif index < tiles:
            action(index)
    offset = jnp.zeros_like(ends[0])
    for c in range(chunks):
        reach[chunk_of(c), :] = jnp.exp(cum_ref[chunk_of(c), :] + offset[:1, :])
        offset = offset + ends[c]
    loads[14].wait()

    def gate_pair(b, j):
        cols = slice(j * tile, (j + 1) * tile)
        for k in range(2):
            at = chunk_of(b * 2 + k)
            reads = jnp.dot(bc_ref[at, states:], carried[j], preferred_element_type=f32)
            weight = per_head(reach[at, :], j * heads_tile, heads_tile, head_width, tile)
            g = (y_ref[at, cols] + reads * weight) * gate_ref[at, cols]
            squares = jnp.zeros((ROWS, 128), f32)
            for q in range(tile // 128):
                p = j * tile // 128 + q
                part = g[:, q * 128 : (q + 1) * 128]
                squares = squares + part * part
                gated[at, p * 128 : (p + 1) * 128] = (part * gain[p : p + 1, :]).astype(bf16)
            square_acc[k] = squares if j == 0 else square_acc[k] + squares

    def close_pair(b):
        for k in range(2):
            square_out[b * 2 + k] = lax.dot_general(
                jnp.ones((8, 128), f32), square_acc[k], across_rows,
                preferred_element_type=f32, precision=HIGHEST,
            )

    def square_copy(b):
        return remote(square_out.at[b], square_in.at[tp], sq_send, sq_recv, at_tp(b))

    def pair_of(b):
        return tile_of(b, 2 * ROWS)

    for j in range(tiles):
        await_carried(j)
        gate_pair(1 - chip, j)
    diagonal = (1 - chip) * 2 + 1 - core

    def near_copy(p):
        return remote(near_out.at[p], near_in.at[p], near_send, near_recv.at[p], at_tp(mate))

    def far_copy(p):
        return remote(far_out.at[p], far_in.at[p], far_send, far_recv.at[p], at_tp(across))

    def own_copy(p):
        return remote(own_out.at[p], own_in.at[p], own_send, own_recv, at_tp(mate))

    def pass_on(p):
        near_copy(p).wait_recv()
        far_out[p] = (far_acc[p] + near_in[p].astype(f32)).astype(bf16)
        far_copy(p).start()

    def far_piece(p, _):
        cols = tile_of(p, piece)
        both[...] = jnp.dot(gated[pair_of(1 - chip), :], out_w[:, cols], preferred_element_type=f32)
        near_out[p] = both[chunk_of(1 - core), :].astype(bf16)
        near_copy(p).start()
        far_acc[p] = both[chunk_of(core), :]

        @pl.when(p > 0)
        def _():
            pass_on(jnp.maximum(p - 1, 0))

        return 0

    lax.fori_loop(base, base + 2, far_piece, 0)
    close_pair(1 - chip)
    square_copy(across).start()
    square_copy(diagonal).start()
    lax.fori_loop(2, PIECES, far_piece, 0)
    pass_on(PIECES - 1)
    for j in range(tiles):
        gate_pair(chip, j)
    close_pair(chip)
    square_copy(mate).start()

    def own_piece(p, _):
        cols = tile_of(p, piece)
        both[...] = jnp.dot(gated[pair_of(chip), :], out_w[:, cols], preferred_element_type=f32)
        own_out[p] = both[chunk_of(1 - core), :].astype(bf16)
        own_copy(p).start()
        own_acc[p] = both[chunk_of(core), :]
        return 0

    lax.fori_loop(0, PIECES, own_piece, 0)

    square = square_out[tp]
    every(square_in.at[pl.ds(0, tp_count - 1)], sq_send, sq_recv).wait_recv()
    for step in range(1, tp_count):
        square = square + square_in[(tp + step) % tp_count]
    mean = square[:1, :] / (channels * tp_count)
    spread = jnp.broadcast_to(lax.rsqrt(mean + 1e-05), (ROWS, ROWS))
    scale = jnp.sum(jnp.where(t_row == s_col, spread, 0.0), axis=1, keepdims=True)

    every(own_in, own_send, own_recv).wait_recv()

    def finish(p, _):
        far_copy(p).wait_recv()
        total = own_acc[p] + own_in[p].astype(f32) + far_in[p].astype(f32)
        out_ref[:, tile_of(p, piece)] = (total * scale).astype(bf16)
        return 0

    lax.fori_loop(0, PIECES, finish, 0)

    every(full.at[chip, :, mine], x_send, x_recv.at[0]).wait_send()
    every(full.at[1 - chip, :, mine], f_send, f_recv.at[0]).wait_send()
    beside(mine).wait_send()

    @pl.when(seq < seq_count - 1)
    def _():
        to_next().wait_send()

    @pl.when(side == 0)
    def _():
        every(sums_out, sums_send, sums_recv.at[0]).wait_send()

    every(decay_in.at[others], decay_send, decay_recv).wait_send()
    every(owned.at[:, others], state_send, state_recv.at[0]).wait_send()
    every(back.at[:, others], back_send, back_recv.at[0]).wait_send()
    every(square_in.at[pl.ds(0, tp_count - 1)], sq_send, sq_recv).wait_send()
    every(near_out, near_send, near_recv.at[0]).wait_send()
    every(far_out, far_send, far_recv.at[0]).wait_send()
    every(own_out, own_send, own_recv).wait_send()


def fused(
    tokens, gate_weight, inner_weight, state_weight, step_weight, conv_inner, conv_state,
    step_bias, decay_rate, skip_gain, norm_gain, out_weight,
):
    rows, width = tokens.shape
    channels = inner_weight.shape[1]
    heads = step_weight.shape[1]
    if channels > 5 * 256 or rows < 3 * ROWS:
        return on_device(
            tokens, gate_weight, inner_weight, state_weight, step_weight, conv_inner, conv_state,
            step_bias, decay_rate, skip_gain, norm_gain, out_weight,
        )
    head_width = channels // heads
    states = state_weight.shape[1] // 2
    depth, out_width = inner_weight.shape[0], out_weight.shape[1]
    seq_count, tp_count = lax.axis_size("seq"), lax.axis_size("tp")
    chunks = rows // ROWS
    quarter = seq_count // 2
    share = states // quarter
    tile = min(256, channels)
    tiles = channels // tile
    arrivals = chunks + 2
    piece = out_width // PIECES
    f32, bf16 = jnp.float32, jnp.bfloat16
    dma, vmem = pltpu.SemaphoreType.DMA, pltpu.VMEM
    args = (
        tokens, gate_weight, inner_weight, state_weight, step_weight.T, conv_inner, conv_state,
        step_bias[None, :], decay_rate[None, :], skip_gain[None, :], norm_gain.reshape(-1, 128), out_weight,
    )
    scratch = [
        vmem((2, rows, 2 * width), bf16),
        vmem((depth, channels), bf16),
        vmem((depth, channels), bf16),
        vmem((depth, 2 * states), bf16),
        vmem((heads, depth), bf16),
        vmem(conv_inner.shape, f32),
        vmem(conv_state.shape, f32),
        vmem((1, heads), f32),
        vmem((1, heads), f32),
        vmem((1, heads), f32),
        vmem((channels // 128, 128), f32),
        vmem((channels, out_width), bf16),
        vmem((rows, channels + 2 * states), f32),
        vmem((8, channels + 2 * states), f32),
        vmem((8, channels + 2 * states), f32),
        vmem((rows, heads), f32),
        vmem((rows, channels), bf16),
        vmem((rows, 2 * states), bf16),
        vmem((rows, channels), f32),
        vmem((rows, channels), f32),
        vmem((rows, channels), bf16),
        vmem((rows, heads), f32),
        vmem((rows, heads), f32),
        vmem((rows, heads), f32),
        vmem((chunks, 8, heads), f32),
        vmem((tiles, states, tile), f32),
        vmem((chunks, tiles, states, tile), bf16),
        vmem((tiles, states, tile), bf16),
        vmem((tiles, quarter, share, tile), bf16),
        vmem((tiles, quarter, share, tile), f32),
        vmem((tiles, share, tile), bf16),
        vmem((tiles, share, tile), bf16),
        vmem((tiles, quarter, share, tile), bf16),
        vmem((tiles, states, tile), bf16),
        vmem((8, 128), f32),
        vmem((quarter, 8, 128), f32),
        vmem((2, ROWS, 128), f32),
        vmem((tp_count, 8, ROWS), f32),
        vmem((tp_count, 8, ROWS), f32),
    ]
    half_sums = vmem((PIECES, ROWS, piece), bf16)
    whole_sums = vmem((PIECES, ROWS, piece), f32)
    scratch += [half_sums, half_sums, whole_sums, half_sums, half_sums, half_sums, half_sums, whole_sums]
    scratch += [vmem((2 * ROWS, piece), f32)]
    scratch += [pltpu.SemaphoreType.REGULAR, dma((15,))]
    scratch += [dma, dma((arrivals,)), dma, dma((arrivals,)), dma, dma, dma, dma]
    scratch += [dma, dma((tiles,)), dma, dma((tiles,)), dma, dma, dma, dma((tiles,))]
    scratch += [dma, dma, dma, dma((PIECES,)), dma, dma((PIECES,)), dma, dma]
    anywhere = pl.BlockSpec(memory_space=pl.ANY)
    return pl.pallas_call(
        lambda *refs: layer_kernel(head_width, *refs),
        out_shape=pltpu.VMEM((rows // tp_count, out_width), bf16),
        in_specs=[anywhere] * len(args),
        out_specs=pl.BlockSpec(memory_space=pltpu.VMEM),
        scratch_shapes=scratch,
        compiler_params=pltpu.CompilerParams(
            collective_id=0, has_side_effects=True, vmem_limit_bytes=VMEM_LIMIT
        ),
        name="layer",
    )(*args)


def on_device(
    tokens,
    gate_weight,
    inner_weight,
    state_weight,
    step_weight,
    conv_inner,
    conv_state,
    step_bias,
    decay_rate,
    skip_gain,
    norm_gain,
    out_weight,
):
    tok_rows = tokens.shape[0]
    width_inner = inner_weight.shape[1]
    head_count = step_weight.shape[1]
    head_width = width_inner // head_count
    state_size = state_weight.shape[1] // 2
    blocks = tok_rows // GROUP
    size_tp = lax.axis_size("tp")
    me = lax.axis_index("tp")

    chunks = [None] * blocks
    for b in range(blocks - 1, -1, -1):
        chunks[b] = gather_features(tokens[b * GROUP : (b + 1) * GROUP])
    halo = shifted(chunks[-1][GROUP - HALO :], 1)
    chunks[0] = jnp.concatenate([halo, chunks[0]], axis=0)

    inner_raw, state_raw, step_raw = [None] * blocks, [None] * blocks, [None] * blocks
    for b in range(blocks - 1, -1, -1):
        i_b, s_b, t_b = project(chunks[b], inner_weight, state_weight, step_weight)
        inner_raw[b], state_raw[b] = i_b.astype(jnp.bfloat16), s_b.astype(jnp.bfloat16)
        step_raw[b] = t_b[HALO:] if b == 0 else t_b

    lanes = max(128, head_width)
    time_step = jax.nn.softplus(jnp.concatenate(step_raw, axis=0) + step_bias[None, :])
    log_decay = -time_step * decay_rate[None, :]
    grouped = log_decay.reshape(blocks, GROUP, head_count)
    cumulative = jnp.cumsum(grouped, axis=1)
    ending = cumulative[:, -1]
    tail = (jnp.exp(ending[:, None] - cumulative)).reshape(tok_rows, head_count) * time_step
    cumulative = cumulative.reshape(tok_rows, head_count)

    def cost(flops, count, exps):
        return pl.CostEstimate(flops=flops, bytes_accessed=count, transcendentals=exps)

    whole = tok_rows * width_inner
    x, bc, contribution = pl.pallas_call(
        lambda *refs: conv_kernel(blocks, head_width, lanes, *refs),
        out_shape=(
            jax.ShapeDtypeStruct((tok_rows, width_inner), jnp.bfloat16),
            jax.ShapeDtypeStruct((tok_rows, 2 * state_size), jnp.bfloat16),
            jax.ShapeDtypeStruct((blocks, width_inner, state_size), jnp.float32),
        ),
        cost_estimate=cost(2 * whole * state_size, 6 * whole, whole),
        name="conv",
    )(*inner_raw, *state_raw, conv_inner, conv_state, tail)
    contribution = contribution.reshape(blocks, head_count, head_width, state_size)
    local_state = jnp.zeros((head_count, head_width, state_size), jnp.float32)
    for b in range(blocks):
        local_state = jnp.exp(ending[b])[:, None, None] * local_state + contribution[b]

    def by_rows(width):
        return pl.BlockSpec((GROUP, width), lambda b: (b, 0))

    def by_columns(height):
        return pl.BlockSpec((height, GROUP), lambda b: (0, b))

    def fixed(width):
        return pl.BlockSpec((1, width), lambda b: (0, 0))

    intra = pl.pallas_call(
        lambda *refs: intra_kernel(head_width, lanes, *refs),
        grid=(blocks,),
        in_specs=[
            by_rows(width_inner),
            by_rows(2 * state_size),
            by_rows(head_count),
            by_columns(head_count),
            by_columns(head_count),
            fixed(width_inner),
        ],
        out_specs=by_rows(width_inner),
        out_shape=jax.ShapeDtypeStruct((tok_rows, width_inner), jnp.float32),
        cost_estimate=cost(4 * whole * GROUP, 6 * whole, GROUP * tok_rows * head_count),
        name="intra",
    )(x, bc, cumulative, cumulative.T, time_step.T, jnp.repeat(skip_gain, head_width)[None, :])

    gate = jnp.concatenate(
        [
            jnp.dot(c[c.shape[0] - GROUP :], gate_weight, preferred_element_type=jnp.float32).astype(jnp.bfloat16)
            for c in chunks
        ],
        axis=0,
    )

    carried, intra = earlier_state(
        local_state.astype(jnp.bfloat16).reshape(width_inner, state_size),
        jnp.sum(ending, axis=0),
        head_width,
        intra,
    )
    carried = carried.astype(jnp.float32).reshape(head_count, head_width, state_size)
    states = []
    for b in range(blocks):
        states.append(carried.astype(jnp.bfloat16).reshape(1, width_inner, state_size))
        carried = jnp.exp(ending[b])[:, None, None] * carried + contribution[b]

    gated, squares = pl.pallas_call(
        lambda *refs: gate_kernel(head_width, lanes, *refs),
        grid=(blocks,),
        in_specs=[
            by_rows(width_inner),
            by_rows(2 * state_size),
            by_rows(head_count),
            by_rows(width_inner),
            fixed(width_inner),
            pl.BlockSpec((1, width_inner, state_size), lambda b: (b, 0, 0)),
        ],
        out_specs=(by_rows(width_inner), by_rows(1)),
        out_shape=(
            jax.ShapeDtypeStruct((tok_rows, width_inner), jnp.bfloat16),
            jax.ShapeDtypeStruct((tok_rows, 1), jnp.float32),
        ),
        cost_estimate=cost(2 * whole * state_size, 8 * whole, whole),
        name="gate",
    )(intra, bc, cumulative, gate, norm_gain[None, :], jnp.concatenate(states, axis=0))

    square_total = sum_over_tp(squares[:, 0])
    share = tok_rows // size_tp
    mean_square = lax.dynamic_slice(square_total, (me * share,), (share,)) / (width_inner * size_tp)
    scale = lax.rsqrt(mean_square + 1e-05)[:, None]

    if size_tp != 4:
        part = jnp.dot(gated, out_weight, preferred_element_type=jnp.float32).astype(jnp.bfloat16)
        total = lax.psum_scatter(part, "tp", scatter_dimension=0, tiled=True)
        return (total.astype(jnp.float32) * scale).astype(jnp.bfloat16)

    side = me // 2

    def reduced(chip, weight):
        rows = lax.dynamic_slice(gated, (chip * 2 * share, 0), (2 * share, width_inner))
        both = jnp.dot(rows, weight, preferred_element_type=jnp.float32).astype(jnp.bfloat16)
        shape = (share, weight.shape[1])
        away = lax.dynamic_slice(both, ((1 - me % 2) * share, 0), shape)
        own = lax.dynamic_slice(both, ((me % 2) * share, 0), shape)
        return own.astype(jnp.float32) + swapped(away, 1).astype(jnp.float32)

    cuts = 2
    width_out = out_weight.shape[1] // cuts
    weights = [out_weight[:, c * width_out : (c + 1) * width_out] for c in range(cuts)]
    arrived = [swapped(reduced(side ^ 1, w).astype(jnp.bfloat16), 2) for w in weights]
    results = []
    for w, other in zip(weights, arrived):
        total = reduced(side, w) + other.astype(jnp.float32)
        results.append((total * scale).astype(jnp.bfloat16))
    return jnp.concatenate(results, axis=1)


def solution(mesh):
    in_specs = (
        P("seq", "tp"),
        P(None, "tp"),
        P(None, "tp"),
        P(),
        P(None, "tp"),
        P(None, "tp"),
        P(),
        P("tp"),
        P("tp"),
        P("tp"),
        P("tp"),
        P("tp", None),
    )
    out_specs = P(("seq", "tp"), None)
    quick = mesh.shape["tp"] == 4 and mesh.shape["seq"] == 8
    return jax.shard_map(
        fused if quick else on_device, mesh=mesh, in_specs=in_specs, out_specs=out_specs, check_vma=False
    )
```

```python
import jax
import jax.numpy as jnp
from jax import lax
from jax.experimental import pallas as pl
from jax.experimental.pallas import tpu as pltpu
from jax.sharding import PartitionSpec as P

GROUP = 256
HALO = 16


def swapped(shard, by):
    size = lax.axis_size("tp")
    return lax.ppermute(shard, "tp", [(i, i ^ by) for i in range(size)])


def shifted(shard, by):
    size = lax.axis_size("seq")
    return lax.ppermute(shard, "seq", [(i, i + by) for i in range(size - by)])


def gather_features(rows):
    size = lax.axis_size("tp")
    me = lax.axis_index("tp")
    width = rows.shape[1]
    held = [(0, rows)]
    step = size // 2
    while step >= 1:
        held = held + [(code ^ step, swapped(part, step)) for code, part in held]
        step //= 2
    parts = dict(held)
    full = jnp.zeros((rows.shape[0], width * size), rows.dtype)
    for code in range(size):
        full = lax.dynamic_update_slice(full, parts[code], (0, (me ^ code) * width))
    return full


def sum_over_tp(part):
    size = lax.axis_size("tp")
    step = 1
    while step < size:
        part = part + swapped(part, step)
        step *= 2
    return part


def prefix_kernel(mine_ref, decay_ref, owner_ref, out_ref):
    owner = owner_ref[...]
    carried = jnp.zeros(mine_ref.shape[1:], jnp.float32)
    for i in range(mine_ref.shape[0]):
        out_ref[i] = carried.astype(jnp.bfloat16)
        log_row = jnp.sum(owner * decay_ref[i : i + 1, :], axis=1, keepdims=True)
        carried = carried * jnp.exp(log_row) + mine_ref[i].astype(jnp.float32)


def earlier_state(local_state, decay_total, head_width, cover):
    size = lax.axis_size("seq")
    rows, states = local_state.shape
    share = rows // size
    me = lax.axis_index("seq")
    heads = decay_total.shape[0]
    wide = jnp.pad(decay_total, (0, -heads % 128))
    wide = jnp.broadcast_to(wide[None, None, :], (size, 1, wide.shape[0]))
    decay_all = lax.all_to_all(wide, "seq", 0, 0, tiled=True)[:, 0, :heads]
    blocks = local_state.reshape(size, share, states)
    blocks, decay_all = lax.optimization_barrier((blocks, decay_all))
    mine = lax.all_to_all(blocks, "seq", 0, 0, tiled=True)
    mine, cover = lax.optimization_barrier((mine, cover))
    row_head = (me * share + jnp.arange(share)) // head_width
    owner = (row_head[:, None] == jnp.arange(decay_total.shape[0])[None, :]).astype(jnp.float32)
    prefixes = pl.pallas_call(
        prefix_kernel,
        out_shape=jax.ShapeDtypeStruct(mine.shape, jnp.bfloat16),
        cost_estimate=pl.CostEstimate(flops=0, bytes_accessed=4 * mine.size, transcendentals=0),
    )(mine, decay_all, owner)
    return lax.all_to_all(prefixes, "seq", 0, 0, tiled=True).reshape(rows, states), cover


def per_head(table, first, count, width, lanes):
    lane = lax.broadcasted_iota(jnp.int32, (table.shape[0], lanes), 1)
    spread = jnp.broadcast_to(table[:, first : first + 1], (table.shape[0], lanes))
    for k in range(1, count):
        spread = jnp.where(lane >= k * width, table[:, first + k : first + k + 1], spread)
    return spread


def silu(value):
    return value * (0.5 * jnp.tanh(0.5 * value) + 0.5)


def conv_kernel(blocks, head_width, lanes, *refs):
    inner_refs, state_refs = refs[:blocks], refs[blocks : 2 * blocks]
    tap_inner, tap_state, tail_ref = refs[2 * blocks : 2 * blocks + 3]
    x_ref, bc_ref, contribution_ref = refs[2 * blocks + 3 :]
    taps = tap_inner.shape[0]
    heads_per = lanes // head_width

    def mixed(chunk_refs, b, span, kernel):
        if b == 0:
            padded = chunk_refs[0][:, span].astype(jnp.float32)
        else:
            last = chunk_refs[b - 1].shape[0] - HALO
            edge = chunk_refs[b - 1][last:, span].astype(jnp.float32)
            padded = jnp.concatenate([edge, chunk_refs[b][:, span].astype(jnp.float32)], axis=0)
        total = padded * kernel[taps - 1 : taps]
        for tap in range(taps - 1):
            total = total + pltpu.roll(padded, taps - 1 - tap, 0) * kernel[tap : tap + 1]
        return silu(total[HALO:]).astype(jnp.bfloat16)

    for b in range(blocks):
        rows = slice(b * GROUP, (b + 1) * GROUP)
        bc = mixed(state_refs, b, slice(None), tap_state[...])
        bc_ref[rows] = bc
        inject = bc[:, : bc.shape[1] // 2]
        tail = tail_ref[rows]
        for p in range(x_ref.shape[1] // lanes):
            span = slice(p * lanes, (p + 1) * lanes)
            x = mixed(inner_refs, b, span, tap_inner[:, span])
            x_ref[rows, span] = x
            weight = per_head(tail, p * heads_per, heads_per, head_width, lanes)
            scaled = (x.astype(jnp.float32) * weight).astype(jnp.bfloat16)
            contribution_ref[b, span] = lax.dot_general(
                scaled, inject, (((0,), (0,)), ((), ())), preferred_element_type=jnp.float32
            )


def intra_kernel(head_width, lanes, x_ref, bc_ref, cum_ref, cum_t_ref, step_t_ref, skip_ref, out_ref):
    states = bc_ref.shape[1] // 2
    heads_per = lanes // head_width
    scores = lax.dot_general(
        bc_ref[:, states:], bc_ref[:, :states], (((1,), (1,)), ((), ())),
        preferred_element_type=jnp.float32,
    )
    t = lax.broadcasted_iota(jnp.int32, scores.shape, 0)
    s = lax.broadcasted_iota(jnp.int32, scores.shape, 1)
    scores = jnp.where(s <= t, scores, 0.0)
    lane = lax.broadcasted_iota(jnp.int32, (x_ref.shape[0], lanes), 1)
    for p in range(x_ref.shape[1] // lanes):
        span = slice(p * lanes, (p + 1) * lanes)
        x = x_ref[:, span]
        total = None
        for k in range(heads_per):
            h = p * heads_per + k
            gaps = jnp.minimum(cum_ref[:, h : h + 1] - cum_t_ref[h : h + 1, :], 0.0)
            mixing = (scores * jnp.exp(gaps) * step_t_ref[h : h + 1, :]).astype(jnp.bfloat16)
            part = jnp.dot(mixing, x, preferred_element_type=jnp.float32)
            total = part if k == 0 else jnp.where(lane >= k * head_width, part, total)
        out_ref[:, span] = total + skip_ref[:, span] * x.astype(jnp.float32)


def gate_kernel(head_width, lanes, intra_ref, bc_ref, cum_ref, gate_ref, gain_ref, state_ref, out_ref, square_ref):
    states = bc_ref.shape[1] // 2
    heads_per = lanes // head_width
    readout = bc_ref[:, states:]
    grown = jnp.exp(cum_ref[...])
    squares = jnp.zeros((readout.shape[0], lanes), jnp.float32)
    for p in range(intra_ref.shape[1] // lanes):
        span = slice(p * lanes, (p + 1) * lanes)
        reads = lax.dot_general(
            readout, state_ref[0, span], (((1,), (1,)), ((), ())), preferred_element_type=jnp.float32
        )
        weight = per_head(grown, p * heads_per, heads_per, head_width, lanes)
        g = (intra_ref[:, span] + reads * weight) * silu(gate_ref[:, span].astype(jnp.float32))
        squares = squares + g * g
        out_ref[:, span] = (g * gain_ref[:, span]).astype(jnp.bfloat16)
    square_ref[...] = jnp.sum(squares, axis=1, keepdims=True)


def project(rows, *weights):
    return [jnp.dot(rows, weight, preferred_element_type=jnp.float32) for weight in weights]


ROWS = 128
PIECES = 10
VMEM_LIMIT = 56 * 1024 * 1024
MESH = pl.DeviceIdType.MESH
HIGHEST = lax.Precision.HIGHEST


def softplus(value):
    return jnp.maximum(value, 0.0) + jnp.log1p(jnp.exp(-jnp.abs(value)))


def chunk_of(index):
    return pl.ds(pl.multiple_of(index * ROWS, ROWS), ROWS)


def tile_of(index, width):
    return pl.ds(pl.multiple_of(index * width, width), width)


def layer_kernel(
    head_width,
    tok_in, gate_in, inner_in, statew_in, stepw_in, convi_in, convs_in, bias_in, rate_in, skip_in, gain_in, outw_in,
    out_ref,
    full, gate_w, inner_w, state_w, step_w, conv_i, conv_s, bias, rate, skip, gain, out_w,
    raw, halo, halo_out, step_acc, x_ref, bc_ref, y_ref, gate_ref, gated,
    cum_ref, step_ref, reach, ends, state, starts, state_out, owned, parts_ref, sums_out, sums_in, back, carried,
    decay_out, decay_in, square_acc,
    square_out, square_in, near_out, near_in, far_acc, far_out, far_in, own_out, own_in, own_acc, both,
    ready, local_sem, x_send, x_recv, f_send, f_recv, d_send, d_recv, halo_send, halo_recv,
    state_send, state_recv, back_send, back_recv, decay_send, decay_recv, sums_send, sums_recv,
    sq_send, sq_recv, near_send, near_recv, far_send, far_recv, own_send, own_recv,
):
    seq_count, tp_count = lax.axis_size("seq"), lax.axis_size("tp")
    seq, tp = lax.axis_index("seq"), lax.axis_index("tp")
    chip, core = tp // 2, tp % 2
    mate, across = chip * 2 + 1 - core, (1 - chip) * 2 + core
    rows, half = full.shape[1], full.shape[2]
    width = half // 2
    channels = inner_w.shape[1]
    states = state_w.shape[1] // 2
    heads = step_w.shape[0]
    chunks = rows // ROWS
    tile = min(256, channels)
    tiles = channels // tile
    spans = channels // 128
    per_span = 128 // head_width
    quarter = seq_count // 2
    side, place = seq // quarter, seq % quarter
    share = states // quarter
    heads_tile = tile // head_width
    piece = out_w.shape[1] // PIECES
    f32, bf16 = jnp.float32, jnp.bfloat16
    across_rows = (((1,), (1,)), ((), ()))

    def at_tp(index):
        return {"seq": seq, "tp": index}

    def at_seq(index):
        return {"seq": index, "tp": tp}

    def remote(src, dst, send, recv, device):
        return pltpu.make_async_remote_copy(
            src_ref=src, dst_ref=dst, send_sem=send, recv_sem=recv, device_id=device, device_id_type=MESH
        )

    barrier = pltpu.get_barrier_semaphore()
    for step in range(1, tp_count):
        pl.semaphore_signal(barrier, inc=1, device_id=at_tp((tp + step) % tp_count), device_id_type=MESH)
    def related(low, high):
        return (low < high) & ((low // quarter == high // quarter) | (high == low + quarter) | (high == low + 1))

    for d in range(seq_count):

        @pl.when(related(seq, d))
        def _():
            pl.semaphore_signal(barrier, inc=1, device_id=at_seq(d), device_id_type=MESH)

    lower = sum(jnp.where(related(d, seq), 1, 0) for d in range(seq_count))
    higher = sum(jnp.where(related(seq, d), 1, 0) for d in range(seq_count))

    mine = pl.ds(pl.multiple_of(core * width, width), width)
    theirs = pl.ds(pl.multiple_of((1 - core) * width, width), width)
    near_rows = pl.ds(pl.multiple_of(chip * half, half), half)
    far_rows = pl.ds(pl.multiple_of((1 - chip) * half, half), half)
    loads = [
        (tok_in, full.at[chip, :, mine]),
        (inner_in.at[near_rows], inner_w.at[near_rows]),
        (statew_in.at[near_rows], state_w.at[near_rows]),
        (stepw_in.at[:, near_rows], step_w.at[:, near_rows]),
        (inner_in.at[far_rows], inner_w.at[far_rows]),
        (statew_in.at[far_rows], state_w.at[far_rows]),
        (stepw_in.at[:, far_rows], step_w.at[:, far_rows]),
        (convi_in, conv_i),
        (convs_in, conv_s),
        (bias_in, bias),
        (rate_in, rate),
        (skip_in, skip),
        (gain_in, gain),
        (gate_in, gate_w),
        (outw_in, out_w),
    ]
    loads = [pltpu.make_async_copy(src, dst, local_sem.at[i]) for i, (src, dst) in enumerate(loads)]
    for load in loads:
        load.start()
    loads[0].wait()
    pl.semaphore_wait(barrier, tp_count - 1 + lower)
    for d in range(seq_count):

        @pl.when(related(d, seq))
        def _():
            pl.semaphore_signal(ready, inc=1, device_id=at_seq(d), device_id_type=MESH)


    order = [(rows - 16, 16)] + [(c * ROWS, ROWS) for c in range(chunks - 1)]
    order += [(rows - ROWS, ROWS // 2), (rows - ROWS // 2, ROWS // 2 - 16)]

    def crossing(i):
        part = full.at[chip, pl.ds(*order[i]), mine]
        return remote(part, part, x_send, x_recv.at[i], at_tp(across))

    def beside(columns):
        part = full.at[chip, :, columns]
        return remote(part, part, d_send, d_recv, at_tp(mate))

    def forwarded(i, columns):
        part = full.at[1 - chip, pl.ds(*order[i]), columns]
        return remote(part, part, f_send, f_recv.at[i], at_tp(mate))

    def relay(i):
        part = full.at[1 - chip, pl.ds(*order[i]), mine]
        remote(part, part, x_send, x_recv.at[i], at_tp(across)).wait_recv()
        forwarded(i, mine).start()

    def settle(i):
        forwarded(i, theirs).wait_recv()

    for i in range(len(order)):
        crossing(i).start()
    beside(mine).start()

    for load in loads[1:4]:
        load.wait()
    beside(theirs).wait_recv()

    near = full.at[chip]

    def first(j, _):
        cols = tile_of(j, tile)
        raw[:, cols] = jnp.dot(near[...], inner_w[near_rows, cols], preferred_element_type=f32)
        return 0

    early = min(3, tiles)
    lax.fori_loop(0, early, first, 0)
    relay(0)
    lax.fori_loop(early, tiles, first, 0)
    raw[:, channels:] = jnp.dot(near[...], state_w[near_rows, :], preferred_element_type=f32)
    step_acc[...] = lax.dot_general(near[...], step_w[:, near_rows], across_rows, preferred_element_type=f32)
    for load in loads[4:13]:
        load.wait()

    def rounded(value):
        return value.astype(bf16).astype(f32)

    far = full.at[1 - chip]

    def project_tile(at, j):
        cols = slice(j * tile, (j + 1) * tile)
        more = jnp.dot(far[at, :], inner_w[far_rows, cols], preferred_element_type=f32)
        raw[at, cols] = rounded(raw[at, cols] + more)

    def project_rest(at):
        more = jnp.dot(far[at, :], state_w[far_rows, :], preferred_element_type=f32)
        raw[at, channels:] = rounded(raw[at, channels:] + more)
        more = lax.dot_general(far[at, :], step_w[:, far_rows], across_rows, preferred_element_type=f32)
        step_acc[at, :] += more

    def project(at):
        for j in range(tiles):
            project_tile(at, j)
        project_rest(at)

    t_row = lax.broadcasted_iota(jnp.int32, (ROWS, ROWS), 0)
    s_col = lax.broadcasted_iota(jnp.int32, (ROWS, ROWS), 1)
    causal = s_col <= t_row

    def mix_chunk(c, final):
        at = chunk_of(c)
        time_step = softplus(step_acc[at, :] + bias[...])
        decay = -time_step * rate[...]
        cum = jnp.dot(causal.astype(f32), decay, preferred_element_type=f32, precision=HIGHEST)
        ending = cum[ROWS - 1 :, :]
        tail = jnp.exp(ending - cum) * time_step
        cum_ref[at, :] = cum
        step_ref[at, :] = time_step
        ends[c] = jnp.broadcast_to(ending, ends.shape[1:])
        if final is not None:
            final(0)
            total = ends[0]
            for k in range(1, chunks):
                total = total + ends[k]
            decay_out[...] = jnp.concatenate([total, jnp.zeros((8, 128 - heads), f32)], axis=1)
            for step in range(1, quarter):
                decay_copy((place + step) % quarter).start()
            decay_in[place] = decay_out[...]
        before = pl.ds(pl.multiple_of(jnp.maximum(c * ROWS - 8, 0), 8), 8)

        def conv(span, kernel):
            edge = jnp.where(c == 0, halo[:, span], raw[before, span])
            padded = jnp.concatenate([edge, raw[at, span]], axis=0)
            taps = kernel.shape[0]
            total = padded * kernel[taps - 1 : taps]
            for tap in range(taps - 1):
                total = total + pltpu.roll(padded, taps - 1 - tap, 0) * kernel[tap : tap + 1]
            return silu(total[8:]).astype(bf16)

        for p in range(2 * states // 128):
            span = slice(p * 128, (p + 1) * 128)
            bc_ref[at, span] = conv(slice(channels + p * 128, channels + (p + 1) * 128), conv_s[:, span])
        inject = bc_ref[at, :states]
        grown = jnp.exp(ending)
        waiting = []
        for j in range(tiles):
            pieces = []
            if final is not None and j + 1 < tiles:
                final(j + 1)
            for p in range(j * tile // 128, (j + 1) * tile // 128):
                span = slice(p * 128, (p + 1) * 128)
                x = conv(span, conv_i[:, span])
                x_ref[at, span] = x
                weight = per_head(tail, p * per_span, per_span, head_width, 128)
                pieces.append((x.astype(f32) * weight).astype(bf16))
            add = lax.dot_general(
                inject, jnp.concatenate(pieces, axis=1), (((0,), (0,)), ((), ())), preferred_element_type=f32
            )
            starts[c, j] = state[j].astype(bf16)
            weight = per_head(grown, j * heads_tile, heads_tile, head_width, tile)
            if final is not None:
                state_out[j] = (state[j] * weight + add).astype(bf16)
                waiting.append(j)
                if j in (1, tiles - 1):
                    for k in waiting:
                        for step in range(1, quarter):
                            state_copy(k, (place + step) % quarter).start()
                        owned[k, place] = state_out[k, share_of(place), :]
                    waiting.clear()
            else:
                state[j] = state[j] * weight + add

    def share_of(o):
        return pl.ds(pl.multiple_of(o * share, share), share)

    def at_place(o):
        return at_seq(side * quarter + o)

    def decay_copy(o):
        return remote(decay_out, decay_in.at[place], decay_send, decay_recv, at_place(o))

    def state_copy(j, o):
        return remote(
            state_out.at[j, share_of(o)], owned.at[j, place], state_send, state_recv.at[j], at_place(o)
        )

    def sums_copy(j):
        return remote(
            sums_out.at[j], sums_in.at[j], sums_send, sums_recv.at[j], at_seq((seq + quarter) % seq_count)
        )

    def back_copy(j, i):
        return remote(
            back.at[j, i], carried.at[j, share_of(place)], back_send, back_recv.at[j], at_place(i)
        )

    others = pl.ds(0, quarter - 1)

    def every(ref, send, recv):
        return remote(ref, ref, send, recv, at_tp(mate))

    def combine(j):
        if j == 0:
            every(decay_in.at[others], decay_send, decay_recv).wait_recv()
        every(owned.at[j, others], state_send, state_recv.at[j]).wait_recv()
        run = owned[j, 0].astype(f32)
        parts_ref[j, 0] = jnp.zeros((share, tile), f32)
        for i in range(1, quarter):
            parts_ref[j, i] = run
            grown = per_head(jnp.exp(decay_in[i][:1, :]), j * heads_tile, heads_tile, head_width, tile)
            run = run * grown + owned[j, i].astype(f32)

        @pl.when(side == 0)
        def _():
            sums_out[j] = run.astype(bf16)
            sums_copy(j).start()
            give_back(j, None)

    def give_back(j, before):
        total = jnp.zeros((8, 128), f32)
        for i in range(quarter):
            value = parts_ref[j, i]
            if before is not None:
                value = value + before * per_head(
                    jnp.exp(total[:1, :]), j * heads_tile, heads_tile, head_width, tile
                )
                total = total + decay_in[i]
            back[j, i] = value.astype(bf16)
        for step in range(1, quarter):
            back_copy(j, (place + step) % quarter).start()
        carried[j, share_of(place), :] = back[j, place]

    def finalize(j):
        @pl.when(side == 1)
        def _():
            sums_copy(j).wait_recv()
            give_back(j, sums_in[j].astype(f32))

    def await_carried(j):
        every(back.at[j, others], back_send, back_recv.at[j]).wait_recv()

    state[...] = jnp.zeros_like(state)

    settle(0)
    end_rows = far[rows - 16 :, :]
    for j in range(tiles):
        cols = slice(j * tile, (j + 1) * tile)
        more = jnp.dot(end_rows, inner_w[far_rows, cols], preferred_element_type=f32)
        halo_out[:, cols] = rounded(raw[rows - 8 :, cols] + more[8:])
    more = jnp.dot(end_rows, state_w[far_rows, :], preferred_element_type=f32)
    halo_out[:, channels:] = rounded(raw[rows - 8 :, channels:] + more[8:])

    def to_next():
        return remote(halo_out, halo, halo_send, halo_recv, at_seq(jnp.minimum(seq + 1, seq_count - 1)))

    @pl.when(seq < seq_count - 1)
    def _():
        pl.semaphore_wait(ready, higher)
        to_next().start()

    @pl.when(seq == 0)
    def _():
        halo[...] = jnp.zeros_like(halo)

    last = chunks - 1
    relay(1)
    loads[13].wait()

    def gate_near(j, _):
        cols = tile_of(j, tile)
        gate_ref[:, cols] = jnp.dot(near[...], gate_w[near_rows, cols], preferred_element_type=f32)
        return 0

    few = min(2, tiles)
    lax.fori_loop(0, few, gate_near, 0)
    settle(1)
    project(chunk_of(0))
    lax.fori_loop(few, tiles, gate_near, 0)
    relay(2)

    @pl.when(seq > 0)
    def _():
        remote(halo_out, halo, halo_send, halo_recv, at_seq(jnp.maximum(seq - 1, 0))).wait_recv()

    for c in range(1, last):
        mix_chunk(c - 1, None)
        settle(1 + c)
        project(chunk_of(c))
        relay(2 + c)
    mix_chunk(last - 1, None)
    settle(chunks)
    relay(chunks + 1)
    project(pl.ds(rows - ROWS, ROWS // 2))
    settle(chunks + 1)
    rest = pl.ds(rows - ROWS // 2, ROWS // 2)
    project_rest(rest)
    mix_chunk(last, lambda j: project_tile(rest, j))

    def inside(c, _):
        at = chunk_of(c)
        cum = cum_ref[at, :]
        eye = (t_row == s_col).astype(f32)
        flip = (((0,), (0,)), ((), ()))
        cum_t = lax.dot_general(cum, eye, flip, preferred_element_type=f32, precision=HIGHEST)
        step_t = lax.dot_general(step_ref[at, :], eye, flip, preferred_element_type=f32, precision=HIGHEST)
        readout = bc_ref[at, states:]
        scores = lax.dot_general(
            readout, bc_ref[at, :states], (((1,), (1,)), ((), ())), preferred_element_type=f32
        )
        scores = jnp.where(causal, scores, 0.0)
        grown = jnp.exp(cum)
        lane = lax.broadcasted_iota(jnp.int32, (ROWS, 128), 1)
        for p in range(spans):
            span = slice(p * 128, (p + 1) * 128)
            x = x_ref[at, span]
            mixes, parts = [], []
            for k in range(per_span):
                h = p * per_span + k
                gaps = jnp.minimum(cum[:, h : h + 1] - cum_t[h : h + 1, :], 0.0)
                mixes.append((scores * jnp.exp(gaps) * step_t[h : h + 1, :]).astype(bf16))
                own = (lane >= k * head_width) & (lane < (k + 1) * head_width)
                parts.append(jnp.where(own, x, jnp.zeros_like(x)))
            total = jnp.dot(
                jnp.concatenate(mixes, axis=1), jnp.concatenate(parts, axis=0), preferred_element_type=f32
            )
            lanes = slice(p * 128 % tile, p * 128 % tile + 128)
            reads = jnp.dot(readout, starts[c, p * 128 // tile, :, lanes], preferred_element_type=f32)
            weight = per_head(grown, p * per_span, per_span, head_width, 128)
            direct = per_head(skip[...], p * per_span, per_span, head_width, 128)
            y_ref[at, span] = total + reads * weight + direct * x.astype(f32)
        return 0

    def gate_tile(j, _):
        cols = tile_of(j, tile)
        more = jnp.dot(far[...], gate_w[far_rows, cols], preferred_element_type=f32)
        gate_ref[:, cols] = silu(rounded(gate_ref[:, cols] + more))
        return 0

    base = jnp.minimum(seq, 0)

    def run(body, index):
        lax.fori_loop(base + index, base + index + 1, body, 0)

    steps = [(None, 0), (None, 1), (run, 0), (run, 1)] + [(combine, j) for j in range(3)]
    steps += [(run, 2), (combine, 3), (combine, 4), (run, 3), (finalize, 0), (run, 4), (finalize, 1), (finalize, 2)]
    steps += [(None, chunk) for chunk in range(2, chunks - 1)]
    steps += [(finalize, 3), (finalize, 4), (None, chunks - 1)]
    for action, index in steps:
        if action is None:
            run(inside, index)
        elif index < tiles and action is run:
            run(gate_tile, index)
        elif index < tiles and action is combine:
            action(index)
        elif index < tiles:
            action(index)
    offset = jnp.zeros_like(ends[0])
    for c in range(chunks):
        reach[chunk_of(c), :] = jnp.exp(cum_ref[chunk_of(c), :] + offset[:1, :])
        offset = offset + ends[c]
    loads[14].wait()

    def gate_pair(b, j):
        cols = slice(j * tile, (j + 1) * tile)
        for k in range(2):
            at = chunk_of(b * 2 + k)
            reads = jnp.dot(bc_ref[at, states:], carried[j], preferred_element_type=f32)
            weight = per_head(reach[at, :], j * heads_tile, heads_tile, head_width, tile)
            g = (y_ref[at, cols] + reads * weight) * gate_ref[at, cols]
            squares = jnp.zeros((ROWS, 128), f32)
            for q in range(tile // 128):
                p = j * tile // 128 + q
                part = g[:, q * 128 : (q + 1) * 128]
                squares = squares + part * part
                gated[at, p * 128 : (p + 1) * 128] = (part * gain[p : p + 1, :]).astype(bf16)
            square_acc[k] = squares if j == 0 else square_acc[k] + squares

    def close_pair(b):
        for k in range(2):
            square_out[b * 2 + k] = lax.dot_general(
                jnp.ones((8, 128), f32), square_acc[k], across_rows,
                preferred_element_type=f32, precision=HIGHEST,
            )

    def square_copy(b):
        return remote(square_out.at[b], square_in.at[tp], sq_send, sq_recv, at_tp(b))

    def pair_of(b):
        return tile_of(b, 2 * ROWS)

    most = channels - tile
    for j in range(tiles):
        if j == tiles - 1 and most:
            both[...] = jnp.dot(gated[pair_of(1 - chip), :most], out_w[:most, :piece], preferred_element_type=f32)
        await_carried(j)
        gate_pair(1 - chip, j)
    diagonal = (1 - chip) * 2 + 1 - core

    def near_copy(p):
        return remote(near_out.at[p], near_in.at[p], near_send, near_recv.at[p], at_tp(mate))

    def far_copy(p):
        return remote(far_out.at[p], far_in.at[p], far_send, far_recv.at[p], at_tp(across))

    def own_copy(p):
        return remote(own_out.at[p], own_in.at[p], own_send, own_recv, at_tp(mate))

    def pass_on(p):
        near_copy(p).wait_recv()
        far_out[p] = (far_acc[p] + near_in[p].astype(f32)).astype(bf16)
        far_copy(p).start()

    def far_piece(p, _):
        cols = tile_of(p, piece)
        both[...] = jnp.dot(gated[pair_of(1 - chip), :], out_w[:, cols], preferred_element_type=f32)
        near_out[p] = both[chunk_of(1 - core), :].astype(bf16)
        near_copy(p).start()
        far_acc[p] = both[chunk_of(core), :]

        pass_on(p - 1)
        return 0

    whole = jnp.dot(gated[pair_of(1 - chip), most:], out_w[most:, :piece], preferred_element_type=f32)
    both[...] = both[...] + whole if most else whole
    near_out[0] = both[chunk_of(1 - core), :].astype(bf16)
    near_copy(0).start()
    far_acc[0] = both[chunk_of(core), :]
    lax.fori_loop(base + 1, base + 2, far_piece, 0)
    close_pair(1 - chip)
    square_copy(across).start()
    square_copy(diagonal).start()
    lax.fori_loop(2, PIECES, far_piece, 0)
    pass_on(PIECES - 1)
    for j in range(tiles):
        gate_pair(chip, j)
    close_pair(chip)
    square_copy(mate).start()

    def own_piece(p, _):
        cols = tile_of(p, piece)
        both[...] = jnp.dot(gated[pair_of(chip), :], out_w[:, cols], preferred_element_type=f32)
        own_out[p] = both[chunk_of(1 - core), :].astype(bf16)
        own_copy(p).start()
        own_acc[p] = both[chunk_of(core), :]
        return 0

    lax.fori_loop(0, PIECES, own_piece, 0)

    square = square_out[tp]
    every(square_in.at[pl.ds(0, tp_count - 1)], sq_send, sq_recv).wait_recv()
    for step in range(1, tp_count):
        square = square + square_in[(tp + step) % tp_count]
    mean = square[:1, :] / (channels * tp_count)
    spread = jnp.broadcast_to(lax.rsqrt(mean + 1e-05), (ROWS, ROWS))
    scale = jnp.sum(jnp.where(t_row == s_col, spread, 0.0), axis=1, keepdims=True)

    every(own_in, own_send, own_recv).wait_recv()

    def finish(p, _):
        far_copy(p).wait_recv()
        total = own_acc[p] + own_in[p].astype(f32) + far_in[p].astype(f32)
        out_ref[:, tile_of(p, piece)] = (total * scale).astype(bf16)
        return 0

    lax.fori_loop(0, PIECES, finish, 0)

    every(full.at[chip, :, mine], x_send, x_recv.at[0]).wait_send()
    every(full.at[1 - chip, :, mine], f_send, f_recv.at[0]).wait_send()
    beside(mine).wait_send()

    @pl.when(seq < seq_count - 1)
    def _():
        to_next().wait_send()

    @pl.when(side == 0)
    def _():
        every(sums_out, sums_send, sums_recv.at[0]).wait_send()

    every(decay_in.at[others], decay_send, decay_recv).wait_send()
    every(owned.at[:, others], state_send, state_recv.at[0]).wait_send()
    every(back.at[:, others], back_send, back_recv.at[0]).wait_send()
    every(square_in.at[pl.ds(0, tp_count - 1)], sq_send, sq_recv).wait_send()
    every(near_out, near_send, near_recv.at[0]).wait_send()
    every(far_out, far_send, far_recv.at[0]).wait_send()
    every(own_out, own_send, own_recv).wait_send()


def fused(
    tokens, gate_weight, inner_weight, state_weight, step_weight, conv_inner, conv_state,
    step_bias, decay_rate, skip_gain, norm_gain, out_weight,
):
    rows, width = tokens.shape
    channels = inner_weight.shape[1]
    heads = step_weight.shape[1]
    if channels > 5 * 256 or rows < 3 * ROWS:
        return on_device(
            tokens, gate_weight, inner_weight, state_weight, step_weight, conv_inner, conv_state,
            step_bias, decay_rate, skip_gain, norm_gain, out_weight,
        )
    head_width = channels // heads
    states = state_weight.shape[1] // 2
    depth, out_width = inner_weight.shape[0], out_weight.shape[1]
    seq_count, tp_count = lax.axis_size("seq"), lax.axis_size("tp")
    chunks = rows // ROWS
    quarter = seq_count // 2
    share = states // quarter
    tile = min(256, channels)
    tiles = channels // tile
    arrivals = chunks + 2
    piece = out_width // PIECES
    f32, bf16 = jnp.float32, jnp.bfloat16
    dma, vmem = pltpu.SemaphoreType.DMA, pltpu.VMEM
    args = (
        tokens, gate_weight, inner_weight, state_weight, step_weight.T, conv_inner, conv_state,
        step_bias[None, :], decay_rate[None, :], skip_gain[None, :], norm_gain.reshape(-1, 128), out_weight,
    )
    scratch = [
        vmem((2, rows, 2 * width), bf16),
        vmem((depth, channels), bf16),
        vmem((depth, channels), bf16),
        vmem((depth, 2 * states), bf16),
        vmem((heads, depth), bf16),
        vmem(conv_inner.shape, f32),
        vmem(conv_state.shape, f32),
        vmem((1, heads), f32),
        vmem((1, heads), f32),
        vmem((1, heads), f32),
        vmem((channels // 128, 128), f32),
        vmem((channels, out_width), bf16),
        vmem((rows, channels + 2 * states), f32),
        vmem((8, channels + 2 * states), f32),
        vmem((8, channels + 2 * states), f32),
        vmem((rows, heads), f32),
        vmem((rows, channels), bf16),
        vmem((rows, 2 * states), bf16),
        vmem((rows, channels), f32),
        vmem((rows, channels), f32),
        vmem((rows, channels), bf16),
        vmem((rows, heads), f32),
        vmem((rows, heads), f32),
        vmem((rows, heads), f32),
        vmem((chunks, 8, heads), f32),
        vmem((tiles, states, tile), f32),
        vmem((chunks, tiles, states, tile), bf16),
        vmem((tiles, states, tile), bf16),
        vmem((tiles, quarter, share, tile), bf16),
        vmem((tiles, quarter, share, tile), f32),
        vmem((tiles, share, tile), bf16),
        vmem((tiles, share, tile), bf16),
        vmem((tiles, quarter, share, tile), bf16),
        vmem((tiles, states, tile), bf16),
        vmem((8, 128), f32),
        vmem((quarter, 8, 128), f32),
        vmem((2, ROWS, 128), f32),
        vmem((tp_count, 8, ROWS), f32),
        vmem((tp_count, 8, ROWS), f32),
    ]
    half_sums = vmem((PIECES, ROWS, piece), bf16)
    whole_sums = vmem((PIECES, ROWS, piece), f32)
    scratch += [half_sums, half_sums, whole_sums, half_sums, half_sums, half_sums, half_sums, whole_sums]
    scratch += [vmem((2 * ROWS, piece), f32)]
    scratch += [pltpu.SemaphoreType.REGULAR, dma((15,))]
    scratch += [dma, dma((arrivals,)), dma, dma((arrivals,)), dma, dma, dma, dma]
    scratch += [dma, dma((tiles,)), dma, dma((tiles,)), dma, dma, dma, dma((tiles,))]
    scratch += [dma, dma, dma, dma((PIECES,)), dma, dma((PIECES,)), dma, dma]
    anywhere = pl.BlockSpec(memory_space=pl.ANY)
    return pl.pallas_call(
        lambda *refs: layer_kernel(head_width, *refs),
        out_shape=pltpu.VMEM((rows // tp_count, out_width), bf16),
        in_specs=[anywhere] * len(args),
        out_specs=pl.BlockSpec(memory_space=pltpu.VMEM),
        scratch_shapes=scratch,
        compiler_params=pltpu.CompilerParams(
            collective_id=0, has_side_effects=True, vmem_limit_bytes=VMEM_LIMIT
        ),
        name="layer",
    )(*args)


def on_device(
    tokens,
    gate_weight,
    inner_weight,
    state_weight,
    step_weight,
    conv_inner,
    conv_state,
    step_bias,
    decay_rate,
    skip_gain,
    norm_gain,
    out_weight,
):
    tok_rows = tokens.shape[0]
    width_inner = inner_weight.shape[1]
    head_count = step_weight.shape[1]
    head_width = width_inner // head_count
    state_size = state_weight.shape[1] // 2
    blocks = tok_rows // GROUP
    size_tp = lax.axis_size("tp")
    me = lax.axis_index("tp")

    chunks = [None] * blocks
    for b in range(blocks - 1, -1, -1):
        chunks[b] = gather_features(tokens[b * GROUP : (b + 1) * GROUP])
    halo = shifted(chunks[-1][GROUP - HALO :], 1)
    chunks[0] = jnp.concatenate([halo, chunks[0]], axis=0)

    inner_raw, state_raw, step_raw = [None] * blocks, [None] * blocks, [None] * blocks
    for b in range(blocks - 1, -1, -1):
        i_b, s_b, t_b = project(chunks[b], inner_weight, state_weight, step_weight)
        inner_raw[b], state_raw[b] = i_b.astype(jnp.bfloat16), s_b.astype(jnp.bfloat16)
        step_raw[b] = t_b[HALO:] if b == 0 else t_b

    lanes = max(128, head_width)
    time_step = jax.nn.softplus(jnp.concatenate(step_raw, axis=0) + step_bias[None, :])
    log_decay = -time_step * decay_rate[None, :]
    grouped = log_decay.reshape(blocks, GROUP, head_count)
    cumulative = jnp.cumsum(grouped, axis=1)
    ending = cumulative[:, -1]
    tail = (jnp.exp(ending[:, None] - cumulative)).reshape(tok_rows, head_count) * time_step
    cumulative = cumulative.reshape(tok_rows, head_count)

    def cost(flops, count, exps):
        return pl.CostEstimate(flops=flops, bytes_accessed=count, transcendentals=exps)

    whole = tok_rows * width_inner
    x, bc, contribution = pl.pallas_call(
        lambda *refs: conv_kernel(blocks, head_width, lanes, *refs),
        out_shape=(
            jax.ShapeDtypeStruct((tok_rows, width_inner), jnp.bfloat16),
            jax.ShapeDtypeStruct((tok_rows, 2 * state_size), jnp.bfloat16),
            jax.ShapeDtypeStruct((blocks, width_inner, state_size), jnp.float32),
        ),
        cost_estimate=cost(2 * whole * state_size, 6 * whole, whole),
        name="conv",
    )(*inner_raw, *state_raw, conv_inner, conv_state, tail)
    contribution = contribution.reshape(blocks, head_count, head_width, state_size)
    local_state = jnp.zeros((head_count, head_width, state_size), jnp.float32)
    for b in range(blocks):
        local_state = jnp.exp(ending[b])[:, None, None] * local_state + contribution[b]

    def by_rows(width):
        return pl.BlockSpec((GROUP, width), lambda b: (b, 0))

    def by_columns(height):
        return pl.BlockSpec((height, GROUP), lambda b: (0, b))

    def fixed(width):
        return pl.BlockSpec((1, width), lambda b: (0, 0))

    intra = pl.pallas_call(
        lambda *refs: intra_kernel(head_width, lanes, *refs),
        grid=(blocks,),
        in_specs=[
            by_rows(width_inner),
            by_rows(2 * state_size),
            by_rows(head_count),
            by_columns(head_count),
            by_columns(head_count),
            fixed(width_inner),
        ],
        out_specs=by_rows(width_inner),
        out_shape=jax.ShapeDtypeStruct((tok_rows, width_inner), jnp.float32),
        cost_estimate=cost(4 * whole * GROUP, 6 * whole, GROUP * tok_rows * head_count),
        name="intra",
    )(x, bc, cumulative, cumulative.T, time_step.T, jnp.repeat(skip_gain, head_width)[None, :])

    gate = jnp.concatenate(
        [
            jnp.dot(c[c.shape[0] - GROUP :], gate_weight, preferred_element_type=jnp.float32).astype(jnp.bfloat16)
            for c in chunks
        ],
        axis=0,
    )

    carried, intra = earlier_state(
        local_state.astype(jnp.bfloat16).reshape(width_inner, state_size),
        jnp.sum(ending, axis=0),
        head_width,
        intra,
    )
    carried = carried.astype(jnp.float32).reshape(head_count, head_width, state_size)
    states = []
    for b in range(blocks):
        states.append(carried.astype(jnp.bfloat16).reshape(1, width_inner, state_size))
        carried = jnp.exp(ending[b])[:, None, None] * carried + contribution[b]

    gated, squares = pl.pallas_call(
        lambda *refs: gate_kernel(head_width, lanes, *refs),
        grid=(blocks,),
        in_specs=[
            by_rows(width_inner),
            by_rows(2 * state_size),
            by_rows(head_count),
            by_rows(width_inner),
            fixed(width_inner),
            pl.BlockSpec((1, width_inner, state_size), lambda b: (b, 0, 0)),
        ],
        out_specs=(by_rows(width_inner), by_rows(1)),
        out_shape=(
            jax.ShapeDtypeStruct((tok_rows, width_inner), jnp.bfloat16),
            jax.ShapeDtypeStruct((tok_rows, 1), jnp.float32),
        ),
        cost_estimate=cost(2 * whole * state_size, 8 * whole, whole),
        name="gate",
    )(intra, bc, cumulative, gate, norm_gain[None, :], jnp.concatenate(states, axis=0))

    square_total = sum_over_tp(squares[:, 0])
    share = tok_rows // size_tp
    mean_square = lax.dynamic_slice(square_total, (me * share,), (share,)) / (width_inner * size_tp)
    scale = lax.rsqrt(mean_square + 1e-05)[:, None]

    if size_tp != 4:
        part = jnp.dot(gated, out_weight, preferred_element_type=jnp.float32).astype(jnp.bfloat16)
        total = lax.psum_scatter(part, "tp", scatter_dimension=0, tiled=True)
        return (total.astype(jnp.float32) * scale).astype(jnp.bfloat16)

    side = me // 2

    def reduced(chip, weight):
        rows = lax.dynamic_slice(gated, (chip * 2 * share, 0), (2 * share, width_inner))
        both = jnp.dot(rows, weight, preferred_element_type=jnp.float32).astype(jnp.bfloat16)
        shape = (share, weight.shape[1])
        away = lax.dynamic_slice(both, ((1 - me % 2) * share, 0), shape)
        own = lax.dynamic_slice(both, ((me % 2) * share, 0), shape)
        return own.astype(jnp.float32) + swapped(away, 1).astype(jnp.float32)

    cuts = 2
    width_out = out_weight.shape[1] // cuts
    weights = [out_weight[:, c * width_out : (c + 1) * width_out] for c in range(cuts)]
    arrived = [swapped(reduced(side ^ 1, w).astype(jnp.bfloat16), 2) for w in weights]
    results = []
    for w, other in zip(weights, arrived):
        total = reduced(side, w) + other.astype(jnp.float32)
        results.append((total * scale).astype(jnp.bfloat16))
    return jnp.concatenate(results, axis=1)


def solution(mesh):
    in_specs = (
        P("seq", "tp"),
        P(None, "tp"),
        P(None, "tp"),
        P(),
        P(None, "tp"),
        P(None, "tp"),
        P(),
        P("tp"),
        P("tp"),
        P("tp"),
        P("tp"),
        P("tp", None),
    )
    out_specs = P(("seq", "tp"), None)
    quick = mesh.shape["tp"] == 4 and mesh.shape["seq"] == 8
    return jax.shard_map(
        fused if quick else on_device, mesh=mesh, in_specs=in_specs, out_specs=out_specs, check_vma=False
    )
```

```python
import jax
import jax.numpy as jnp
from jax import lax
from jax.experimental import pallas as pl
from jax.experimental.pallas import tpu as pltpu
from jax.sharding import PartitionSpec as P

GROUP = 256
HALO = 16


def swapped(shard, by):
    size = lax.axis_size("tp")
    return lax.ppermute(shard, "tp", [(i, i ^ by) for i in range(size)])


def shifted(shard, by):
    size = lax.axis_size("seq")
    return lax.ppermute(shard, "seq", [(i, i + by) for i in range(size - by)])


def gather_features(rows):
    size = lax.axis_size("tp")
    me = lax.axis_index("tp")
    width = rows.shape[1]
    held = [(0, rows)]
    step = size // 2
    while step >= 1:
        held = held + [(code ^ step, swapped(part, step)) for code, part in held]
        step //= 2
    parts = dict(held)
    full = jnp.zeros((rows.shape[0], width * size), rows.dtype)
    for code in range(size):
        full = lax.dynamic_update_slice(full, parts[code], (0, (me ^ code) * width))
    return full


def sum_over_tp(part):
    size = lax.axis_size("tp")
    step = 1
    while step < size:
        part = part + swapped(part, step)
        step *= 2
    return part


def prefix_kernel(mine_ref, decay_ref, owner_ref, out_ref):
    owner = owner_ref[...]
    carried = jnp.zeros(mine_ref.shape[1:], jnp.float32)
    for i in range(mine_ref.shape[0]):
        out_ref[i] = carried.astype(jnp.bfloat16)
        log_row = jnp.sum(owner * decay_ref[i : i + 1, :], axis=1, keepdims=True)
        carried = carried * jnp.exp(log_row) + mine_ref[i].astype(jnp.float32)


def earlier_state(local_state, decay_total, head_width, cover):
    size = lax.axis_size("seq")
    rows, states = local_state.shape
    share = rows // size
    me = lax.axis_index("seq")
    heads = decay_total.shape[0]
    wide = jnp.pad(decay_total, (0, -heads % 128))
    wide = jnp.broadcast_to(wide[None, None, :], (size, 1, wide.shape[0]))
    decay_all = lax.all_to_all(wide, "seq", 0, 0, tiled=True)[:, 0, :heads]
    blocks = local_state.reshape(size, share, states)
    blocks, decay_all = lax.optimization_barrier((blocks, decay_all))
    mine = lax.all_to_all(blocks, "seq", 0, 0, tiled=True)
    mine, cover = lax.optimization_barrier((mine, cover))
    row_head = (me * share + jnp.arange(share)) // head_width
    owner = (row_head[:, None] == jnp.arange(decay_total.shape[0])[None, :]).astype(jnp.float32)
    prefixes = pl.pallas_call(
        prefix_kernel,
        out_shape=jax.ShapeDtypeStruct(mine.shape, jnp.bfloat16),
        cost_estimate=pl.CostEstimate(flops=0, bytes_accessed=4 * mine.size, transcendentals=0),
    )(mine, decay_all, owner)
    return lax.all_to_all(prefixes, "seq", 0, 0, tiled=True).reshape(rows, states), cover


def per_head(table, first, count, width, lanes):
    lane = lax.broadcasted_iota(jnp.int32, (table.shape[0], lanes), 1)
    spread = jnp.broadcast_to(table[:, first : first + 1], (table.shape[0], lanes))
    for k in range(1, count):
        spread = jnp.where(lane >= k * width, table[:, first + k : first + k + 1], spread)
    return spread


def silu(value):
    return value * (0.5 * jnp.tanh(0.5 * value) + 0.5)


def conv_kernel(blocks, head_width, lanes, *refs):
    inner_refs, state_refs = refs[:blocks], refs[blocks : 2 * blocks]
    tap_inner, tap_state, tail_ref = refs[2 * blocks : 2 * blocks + 3]
    x_ref, bc_ref, contribution_ref = refs[2 * blocks + 3 :]
    taps = tap_inner.shape[0]
    heads_per = lanes // head_width

    def mixed(chunk_refs, b, span, kernel):
        if b == 0:
            padded = chunk_refs[0][:, span].astype(jnp.float32)
        else:
            last = chunk_refs[b - 1].shape[0] - HALO
            edge = chunk_refs[b - 1][last:, span].astype(jnp.float32)
            padded = jnp.concatenate([edge, chunk_refs[b][:, span].astype(jnp.float32)], axis=0)
        total = padded * kernel[taps - 1 : taps]
        for tap in range(taps - 1):
            total = total + pltpu.roll(padded, taps - 1 - tap, 0) * kernel[tap : tap + 1]
        return silu(total[HALO:]).astype(jnp.bfloat16)

    for b in range(blocks):
        rows = slice(b * GROUP, (b + 1) * GROUP)
        bc = mixed(state_refs, b, slice(None), tap_state[...])
        bc_ref[rows] = bc
        inject = bc[:, : bc.shape[1] // 2]
        tail = tail_ref[rows]
        for p in range(x_ref.shape[1] // lanes):
            span = slice(p * lanes, (p + 1) * lanes)
            x = mixed(inner_refs, b, span, tap_inner[:, span])
            x_ref[rows, span] = x
            weight = per_head(tail, p * heads_per, heads_per, head_width, lanes)
            scaled = (x.astype(jnp.float32) * weight).astype(jnp.bfloat16)
            contribution_ref[b, span] = lax.dot_general(
                scaled, inject, (((0,), (0,)), ((), ())), preferred_element_type=jnp.float32
            )


def intra_kernel(head_width, lanes, x_ref, bc_ref, cum_ref, cum_t_ref, step_t_ref, skip_ref, out_ref):
    states = bc_ref.shape[1] // 2
    heads_per = lanes // head_width
    scores = lax.dot_general(
        bc_ref[:, states:], bc_ref[:, :states], (((1,), (1,)), ((), ())),
        preferred_element_type=jnp.float32,
    )
    t = lax.broadcasted_iota(jnp.int32, scores.shape, 0)
    s = lax.broadcasted_iota(jnp.int32, scores.shape, 1)
    scores = jnp.where(s <= t, scores, 0.0)
    lane = lax.broadcasted_iota(jnp.int32, (x_ref.shape[0], lanes), 1)
    for p in range(x_ref.shape[1] // lanes):
        span = slice(p * lanes, (p + 1) * lanes)
        x = x_ref[:, span]
        total = None
        for k in range(heads_per):
            h = p * heads_per + k
            gaps = jnp.minimum(cum_ref[:, h : h + 1] - cum_t_ref[h : h + 1, :], 0.0)
            mixing = (scores * jnp.exp(gaps) * step_t_ref[h : h + 1, :]).astype(jnp.bfloat16)
            part = jnp.dot(mixing, x, preferred_element_type=jnp.float32)
            total = part if k == 0 else jnp.where(lane >= k * head_width, part, total)
        out_ref[:, span] = total + skip_ref[:, span] * x.astype(jnp.float32)


def gate_kernel(head_width, lanes, intra_ref, bc_ref, cum_ref, gate_ref, gain_ref, state_ref, out_ref, square_ref):
    states = bc_ref.shape[1] // 2
    heads_per = lanes // head_width
    readout = bc_ref[:, states:]
    grown = jnp.exp(cum_ref[...])
    squares = jnp.zeros((readout.shape[0], lanes), jnp.float32)
    for p in range(intra_ref.shape[1] // lanes):
        span = slice(p * lanes, (p + 1) * lanes)
        reads = lax.dot_general(
            readout, state_ref[0, span], (((1,), (1,)), ((), ())), preferred_element_type=jnp.float32
        )
        weight = per_head(grown, p * heads_per, heads_per, head_width, lanes)
        g = (intra_ref[:, span] + reads * weight) * silu(gate_ref[:, span].astype(jnp.float32))
        squares = squares + g * g
        out_ref[:, span] = (g * gain_ref[:, span]).astype(jnp.bfloat16)
    square_ref[...] = jnp.sum(squares, axis=1, keepdims=True)


def project(rows, *weights):
    return [jnp.dot(rows, weight, preferred_element_type=jnp.float32) for weight in weights]


ROWS = 128
PIECES = 10
VMEM_LIMIT = 56 * 1024 * 1024
MESH = pl.DeviceIdType.MESH
HIGHEST = lax.Precision.HIGHEST


def softplus(value):
    return jnp.maximum(value, 0.0) + jnp.log1p(jnp.exp(-jnp.abs(value)))


def chunk_of(index):
    return pl.ds(pl.multiple_of(index * ROWS, ROWS), ROWS)


def tile_of(index, width):
    return pl.ds(pl.multiple_of(index * width, width), width)


def layer_kernel(
    head_width,
    tok_in, gate_in, inner_in, statew_in, stepw_in, convi_in, convs_in, bias_in, rate_in, skip_in, gain_in, outw_in,
    out_ref,
    full, gate_w, inner_w, state_w, step_w, conv_i, conv_s, bias, rate, skip, gain, out_w,
    raw, halo, halo_out, step_acc, x_ref, bc_ref, y_ref, gate_ref, gated,
    cum_ref, step_ref, reach, ends, state, starts, state_out, owned, parts_ref, sums_out, sums_in, back, carried,
    decay_out, decay_in, square_acc,
    square_out, square_in, near_out, near_in, far_acc, far_out, far_in, own_out, own_in, own_acc, both,
    ready, local_sem, x_send, x_recv, f_send, f_recv, d_send, d_recv, halo_send, halo_recv,
    state_send, state_recv, back_send, back_recv, decay_send, decay_recv, sums_send, sums_recv,
    sq_send, sq_recv, near_send, near_recv, far_send, far_recv, own_send, own_recv,
):
    seq_count, tp_count = lax.axis_size("seq"), lax.axis_size("tp")
    seq, tp = lax.axis_index("seq"), lax.axis_index("tp")
    chip, core = tp // 2, tp % 2
    mate, across = chip * 2 + 1 - core, (1 - chip) * 2 + core
    rows, half = full.shape[1], full.shape[2]
    width = half // 2
    channels = inner_w.shape[1]
    states = state_w.shape[1] // 2
    heads = step_w.shape[0]
    chunks = rows // ROWS
    tile = min(256, channels)
    tiles = channels // tile
    spans = channels // 128
    per_span = 128 // head_width
    quarter = seq_count // 2
    side, place = seq // quarter, seq % quarter
    share = states // quarter
    heads_tile = tile // head_width
    piece = out_w.shape[1] // PIECES
    f32, bf16 = jnp.float32, jnp.bfloat16
    across_rows = (((1,), (1,)), ((), ()))

    def at_tp(index):
        return {"seq": seq, "tp": index}

    def at_seq(index):
        return {"seq": index, "tp": tp}

    def remote(src, dst, send, recv, device):
        return pltpu.make_async_remote_copy(
            src_ref=src, dst_ref=dst, send_sem=send, recv_sem=recv, device_id=device, device_id_type=MESH
        )

    barrier = pltpu.get_barrier_semaphore()
    for step in range(1, tp_count):
        pl.semaphore_signal(barrier, inc=1, device_id=at_tp((tp + step) % tp_count), device_id_type=MESH)
    def related(low, high):
        return (low < high) & ((low // quarter == high // quarter) | (high == low + quarter) | (high == low + 1))

    for d in range(seq_count):

        @pl.when(related(seq, d))
        def _():
            pl.semaphore_signal(barrier, inc=1, device_id=at_seq(d), device_id_type=MESH)

    lower = sum(jnp.where(related(d, seq), 1, 0) for d in range(seq_count))
    higher = sum(jnp.where(related(seq, d), 1, 0) for d in range(seq_count))

    mine = pl.ds(pl.multiple_of(core * width, width), width)
    theirs = pl.ds(pl.multiple_of((1 - core) * width, width), width)
    near_rows = pl.ds(pl.multiple_of(chip * half, half), half)
    far_rows = pl.ds(pl.multiple_of((1 - chip) * half, half), half)
    loads = [
        (tok_in, full.at[chip, :, mine]),
        (inner_in.at[near_rows], inner_w.at[near_rows]),
        (statew_in.at[near_rows], state_w.at[near_rows]),
        (stepw_in.at[:, near_rows], step_w.at[:, near_rows]),
        (inner_in.at[far_rows], inner_w.at[far_rows]),
        (statew_in.at[far_rows], state_w.at[far_rows]),
        (stepw_in.at[:, far_rows], step_w.at[:, far_rows]),
        (convi_in, conv_i),
        (convs_in, conv_s),
        (bias_in, bias),
        (rate_in, rate),
        (skip_in, skip),
        (gain_in, gain),
        (gate_in, gate_w),
        (outw_in, out_w),
    ]
    loads = [pltpu.make_async_copy(src, dst, local_sem.at[i]) for i, (src, dst) in enumerate(loads)]
    for load in loads:
        load.start()
    loads[0].wait()
    pl.semaphore_wait(barrier, tp_count - 1 + lower)
    for d in range(seq_count):

        @pl.when(related(d, seq))
        def _():
            pl.semaphore_signal(ready, inc=1, device_id=at_seq(d), device_id_type=MESH)


    order = [(rows - 16, 16)] + [(c * ROWS, ROWS) for c in range(chunks - 1)]
    order += [(rows - ROWS, ROWS // 2), (rows - ROWS // 2, ROWS // 2 - 16)]

    def crossing(i):
        part = full.at[chip, pl.ds(*order[i]), mine]
        return remote(part, part, x_send, x_recv.at[i], at_tp(across))

    def beside(columns):
        part = full.at[chip, :, columns]
        return remote(part, part, d_send, d_recv, at_tp(mate))

    def forwarded(i, columns):
        part = full.at[1 - chip, pl.ds(*order[i]), columns]
        return remote(part, part, f_send, f_recv.at[i], at_tp(mate))

    def relay(i):
        part = full.at[1 - chip, pl.ds(*order[i]), mine]
        remote(part, part, x_send, x_recv.at[i], at_tp(across)).wait_recv()
        forwarded(i, mine).start()

    def settle(i):
        forwarded(i, theirs).wait_recv()

    for i in range(len(order)):
        crossing(i).start()
    beside(mine).start()

    for load in loads[1:4]:
        load.wait()
    beside(theirs).wait_recv()

    near = full.at[chip]

    def first(j, _):
        cols = tile_of(j, tile)
        raw[:, cols] = jnp.dot(near[...], inner_w[near_rows, cols], preferred_element_type=f32)
        return 0

    early = min(3, tiles)
    lax.fori_loop(0, early, first, 0)
    relay(0)
    lax.fori_loop(early, tiles, first, 0)
    raw[:, channels:] = jnp.dot(near[...], state_w[near_rows, :], preferred_element_type=f32)
    step_acc[...] = lax.dot_general(near[...], step_w[:, near_rows], across_rows, preferred_element_type=f32)
    for load in loads[4:13]:
        load.wait()

    def rounded(value):
        return value.astype(bf16).astype(f32)

    far = full.at[1 - chip]

    def project_tile(at, j):
        cols = slice(j * tile, (j + 1) * tile)
        more = jnp.dot(far[at, :], inner_w[far_rows, cols], preferred_element_type=f32)
        raw[at, cols] = rounded(raw[at, cols] + more)

    def project_rest(at):
        more = jnp.dot(far[at, :], state_w[far_rows, :], preferred_element_type=f32)
        raw[at, channels:] = rounded(raw[at, channels:] + more)
        more = lax.dot_general(far[at, :], step_w[:, far_rows], across_rows, preferred_element_type=f32)
        step_acc[at, :] += more

    def project(at):
        for j in range(tiles):
            project_tile(at, j)
        project_rest(at)

    t_row = lax.broadcasted_iota(jnp.int32, (ROWS, ROWS), 0)
    s_col = lax.broadcasted_iota(jnp.int32, (ROWS, ROWS), 1)
    causal = s_col <= t_row

    def mix_chunk(c, final):
        at = chunk_of(c)
        time_step = softplus(step_acc[at, :] + bias[...])
        decay = -time_step * rate[...]
        cum = jnp.dot(causal.astype(f32), decay, preferred_element_type=f32, precision=HIGHEST)
        ending = cum[ROWS - 1 :, :]
        tail = jnp.exp(ending - cum) * time_step
        cum_ref[at, :] = cum
        step_ref[at, :] = time_step
        ends[c] = jnp.broadcast_to(ending, ends.shape[1:])
        if final is not None:
            final(0)
            total = ends[0]
            for k in range(1, chunks):
                total = total + ends[k]
            decay_out[...] = jnp.concatenate([total, jnp.zeros((8, 128 - heads), f32)], axis=1)
            for step in range(1, quarter):
                decay_copy((place + step) % quarter).start()
            decay_in[place] = decay_out[...]
        before = pl.ds(pl.multiple_of(jnp.maximum(c * ROWS - 8, 0), 8), 8)

        def conv(span, kernel):
            edge = jnp.where(c == 0, halo[:, span], raw[before, span])
            padded = jnp.concatenate([edge, raw[at, span]], axis=0)
            taps = kernel.shape[0]
            total = padded * kernel[taps - 1 : taps]
            for tap in range(taps - 1):
                total = total + pltpu.roll(padded, taps - 1 - tap, 0) * kernel[tap : tap + 1]
            return silu(total[8:]).astype(bf16)

        for p in range(2 * states // 128):
            span = slice(p * 128, (p + 1) * 128)
            bc_ref[at, span] = conv(slice(channels + p * 128, channels + (p + 1) * 128), conv_s[:, span])
        inject = bc_ref[at, :states]
        grown = jnp.exp(ending)
        waiting = []
        for j in range(tiles):
            pieces = []
            if final is not None and j + 1 < tiles:
                final(j + 1)
            for p in range(j * tile // 128, (j + 1) * tile // 128):
                span = slice(p * 128, (p + 1) * 128)
                x = conv(span, conv_i[:, span])
                x_ref[at, span] = x
                weight = per_head(tail, p * per_span, per_span, head_width, 128)
                pieces.append((x.astype(f32) * weight).astype(bf16))
            add = lax.dot_general(
                inject, jnp.concatenate(pieces, axis=1), (((0,), (0,)), ((), ())), preferred_element_type=f32
            )
            starts[c, j] = state[j].astype(bf16)
            weight = per_head(grown, j * heads_tile, heads_tile, head_width, tile)
            if final is not None:
                state_out[j] = (state[j] * weight + add).astype(bf16)
                waiting.append(j)
                if j in (1, tiles - 1):
                    for k in waiting:
                        for step in range(1, quarter):
                            state_copy(k, (place + step) % quarter).start()
                        owned[k, place] = state_out[k, share_of(place), :]
                    waiting.clear()
            else:
                state[j] = state[j] * weight + add

    def share_of(o):
        return pl.ds(pl.multiple_of(o * share, share), share)

    def at_place(o):
        return at_seq(side * quarter + o)

    def decay_copy(o):
        return remote(decay_out, decay_in.at[place], decay_send, decay_recv, at_place(o))

    def state_copy(j, o):
        return remote(
            state_out.at[j, share_of(o)], owned.at[j, place], state_send, state_recv.at[j], at_place(o)
        )

    def sums_copy(j):
        return remote(
            sums_out.at[j], sums_in.at[j], sums_send, sums_recv.at[j], at_seq((seq + quarter) % seq_count)
        )

    def back_copy(j, i):
        return remote(
            back.at[j, i], carried.at[j, share_of(place)], back_send, back_recv.at[j], at_place(i)
        )

    others = pl.ds(0, quarter - 1)

    def every(ref, send, recv):
        return remote(ref, ref, send, recv, at_tp(mate))

    def combine(j):
        if j == 0:
            every(decay_in.at[others], decay_send, decay_recv).wait_recv()
        every(owned.at[j, others], state_send, state_recv.at[j]).wait_recv()
        run = owned[j, 0].astype(f32)
        parts_ref[j, 0] = jnp.zeros((share, tile), f32)
        for i in range(1, quarter):
            parts_ref[j, i] = run
            grown = per_head(jnp.exp(decay_in[i][:1, :]), j * heads_tile, heads_tile, head_width, tile)
            run = run * grown + owned[j, i].astype(f32)

        @pl.when(side == 0)
        def _():
            sums_out[j] = run.astype(bf16)
            sums_copy(j).start()
            give_back(j, None)

    def give_back(j, before):
        total = jnp.zeros((8, 128), f32)
        for i in range(quarter):
            value = parts_ref[j, i]
            if before is not None:
                value = value + before * per_head(
                    jnp.exp(total[:1, :]), j * heads_tile, heads_tile, head_width, tile
                )
                total = total + decay_in[i]
            back[j, i] = value.astype(bf16)
        for step in range(1, quarter):
            back_copy(j, (place + step) % quarter).start()
        carried[j, share_of(place), :] = back[j, place]

    def finalize(j):
        @pl.when(side == 1)
        def _():
            sums_copy(j).wait_recv()
            give_back(j, sums_in[j].astype(f32))

    def await_carried(j):
        every(back.at[j, others], back_send, back_recv.at[j]).wait_recv()

    state[...] = jnp.zeros_like(state)

    settle(0)
    end_rows = far[rows - 16 :, :]
    for j in range(tiles):
        cols = slice(j * tile, (j + 1) * tile)
        more = jnp.dot(end_rows, inner_w[far_rows, cols], preferred_element_type=f32)
        halo_out[:, cols] = rounded(raw[rows - 8 :, cols] + more[8:])
    more = jnp.dot(end_rows, state_w[far_rows, :], preferred_element_type=f32)
    halo_out[:, channels:] = rounded(raw[rows - 8 :, channels:] + more[8:])

    def to_next():
        return remote(halo_out, halo, halo_send, halo_recv, at_seq(jnp.minimum(seq + 1, seq_count - 1)))

    @pl.when(seq < seq_count - 1)
    def _():
        pl.semaphore_wait(ready, higher)
        to_next().start()

    @pl.when(seq == 0)
    def _():
        halo[...] = jnp.zeros_like(halo)

    last = chunks - 1
    relay(1)
    loads[13].wait()

    def gate_near(j, _):
        cols = tile_of(j, tile)
        gate_ref[:, cols] = jnp.dot(near[...], gate_w[near_rows, cols], preferred_element_type=f32)
        return 0

    few = min(2, tiles)
    lax.fori_loop(0, few, gate_near, 0)
    settle(1)
    project(chunk_of(0))
    lax.fori_loop(few, tiles, gate_near, 0)
    relay(2)

    @pl.when(seq > 0)
    def _():
        remote(halo_out, halo, halo_send, halo_recv, at_seq(jnp.maximum(seq - 1, 0))).wait_recv()

    for c in range(1, last):
        mix_chunk(c - 1, None)
        settle(1 + c)
        project(chunk_of(c))
        relay(2 + c)
    mix_chunk(last - 1, None)
    settle(chunks)
    relay(chunks + 1)
    project(pl.ds(rows - ROWS, ROWS // 2))
    settle(chunks + 1)
    rest = pl.ds(rows - ROWS // 2, ROWS // 2)
    project_rest(rest)
    mix_chunk(last, lambda j: project_tile(rest, j))

    def inside(c, _):
        at = chunk_of(c)
        cum = cum_ref[at, :]
        eye = (t_row == s_col).astype(f32)
        flip = (((0,), (0,)), ((), ()))
        cum_t = lax.dot_general(cum, eye, flip, preferred_element_type=f32, precision=HIGHEST)
        step_t = lax.dot_general(step_ref[at, :], eye, flip, preferred_element_type=f32, precision=HIGHEST)
        readout = bc_ref[at, states:]
        scores = lax.dot_general(
            readout, bc_ref[at, :states], (((1,), (1,)), ((), ())), preferred_element_type=f32
        )
        scores = jnp.where(causal, scores, 0.0)
        grown = jnp.exp(cum)
        lane = lax.broadcasted_iota(jnp.int32, (ROWS, 128), 1)
        for p in range(spans):
            span = slice(p * 128, (p + 1) * 128)
            x = x_ref[at, span]
            mixes, parts = [], []
            for k in range(per_span):
                h = p * per_span + k
                gaps = jnp.minimum(cum[:, h : h + 1] - cum_t[h : h + 1, :], 0.0)
                mixes.append((scores * jnp.exp(gaps) * step_t[h : h + 1, :]).astype(bf16))
                own = (lane >= k * head_width) & (lane < (k + 1) * head_width)
                parts.append(jnp.where(own, x, jnp.zeros_like(x)))
            total = jnp.dot(
                jnp.concatenate(mixes, axis=1), jnp.concatenate(parts, axis=0), preferred_element_type=f32
            )
            lanes = slice(p * 128 % tile, p * 128 % tile + 128)
            reads = jnp.dot(readout, starts[c, p * 128 // tile, :, lanes], preferred_element_type=f32)
            weight = per_head(grown, p * per_span, per_span, head_width, 128)
            direct = per_head(skip[...], p * per_span, per_span, head_width, 128)
            y_ref[at, span] = total + reads * weight + direct * x.astype(f32)
        return 0

    def gate_tile(j, _):
        cols = tile_of(j, tile)
        more = jnp.dot(far[...], gate_w[far_rows, cols], preferred_element_type=f32)
        gate_ref[:, cols] = silu(rounded(gate_ref[:, cols] + more))
        return 0

    base = jnp.minimum(seq, 0)

    def run(body, index):
        lax.fori_loop(base + index, base + index + 1, body, 0)

    steps = [(None, 0), (None, 1), (run, 0), (combine, 0), (combine, 1), (run, 1), (combine, 2), (combine, 3)]
    steps += [(run, 2), (combine, 4), (run, 3), (finalize, 0), (run, 4), (finalize, 1), (finalize, 2)]
    steps += [(None, chunk) for chunk in range(2, chunks - 1)]
    steps += [(finalize, 3), (finalize, 4), (None, chunks - 1)]
    for action, index in steps:
        if action is None:
            run(inside, index)
        elif index < tiles and action is run:
            run(gate_tile, index)
        elif index < tiles and action is combine:
            action(index)
        elif index < tiles:
            action(index)
    offset = jnp.zeros_like(ends[0])
    for c in range(chunks):
        reach[chunk_of(c), :] = jnp.exp(cum_ref[chunk_of(c), :] + offset[:1, :])
        offset = offset + ends[c]
    loads[14].wait()

    def gate_pair(b, j):
        cols = slice(j * tile, (j + 1) * tile)
        for k in range(2):
            at = chunk_of(b * 2 + k)
            reads = jnp.dot(bc_ref[at, states:], carried[j], preferred_element_type=f32)
            weight = per_head(reach[at, :], j * heads_tile, heads_tile, head_width, tile)
            g = (y_ref[at, cols] + reads * weight) * gate_ref[at, cols]
            squares = jnp.zeros((ROWS, 128), f32)
            for q in range(tile // 128):
                p = j * tile // 128 + q
                part = g[:, q * 128 : (q + 1) * 128]
                squares = squares + part * part
                gated[at, p * 128 : (p + 1) * 128] = (part * gain[p : p + 1, :]).astype(bf16)
            square_acc[k] = squares if j == 0 else square_acc[k] + squares

    def close_pair(b):
        for k in range(2):
            square_out[b * 2 + k] = lax.dot_general(
                jnp.ones((8, 128), f32), square_acc[k], across_rows,
                preferred_element_type=f32, precision=HIGHEST,
            )

    def square_copy(b):
        return remote(square_out.at[b], square_in.at[tp], sq_send, sq_recv, at_tp(b))

    def pair_of(b):
        return tile_of(b, 2 * ROWS)

    most = channels - tile
    for j in range(tiles):
        if j == tiles - 1 and most:
            both[...] = jnp.dot(gated[pair_of(1 - chip), :most], out_w[:most, :piece], preferred_element_type=f32)
        await_carried(j)
        gate_pair(1 - chip, j)
    diagonal = (1 - chip) * 2 + 1 - core

    def near_copy(p):
        return remote(near_out.at[p], near_in.at[p], near_send, near_recv.at[p], at_tp(mate))

    def far_copy(p):
        return remote(far_out.at[p], far_in.at[p], far_send, far_recv.at[p], at_tp(across))

    def own_copy(p):
        return remote(own_out.at[p], own_in.at[p], own_send, own_recv, at_tp(mate))

    def pass_on(p):
        near_copy(p).wait_recv()
        far_out[p] = (far_acc[p] + near_in[p].astype(f32)).astype(bf16)
        far_copy(p).start()

    def far_piece(p, _):
        cols = tile_of(p, piece)
        both[...] = jnp.dot(gated[pair_of(1 - chip), :], out_w[:, cols], preferred_element_type=f32)
        near_out[p] = both[chunk_of(1 - core), :].astype(bf16)
        near_copy(p).start()
        far_acc[p] = both[chunk_of(core), :]

        pass_on(p - 1)
        return 0

    whole = jnp.dot(gated[pair_of(1 - chip), most:], out_w[most:, :piece], preferred_element_type=f32)
    both[...] = both[...] + whole if most else whole
    near_out[0] = both[chunk_of(1 - core), :].astype(bf16)
    near_copy(0).start()
    far_acc[0] = both[chunk_of(core), :]
    lax.fori_loop(base + 1, base + 2, far_piece, 0)
    close_pair(1 - chip)
    square_copy(across).start()
    square_copy(diagonal).start()
    lax.fori_loop(2, PIECES, far_piece, 0)
    pass_on(PIECES - 1)
    for j in range(tiles):
        gate_pair(chip, j)
    close_pair(chip)
    square_copy(mate).start()

    def own_piece(p, _):
        cols = tile_of(p, piece)
        both[...] = jnp.dot(gated[pair_of(chip), :], out_w[:, cols], preferred_element_type=f32)
        own_out[p] = both[chunk_of(1 - core), :].astype(bf16)
        own_copy(p).start()
        own_acc[p] = both[chunk_of(core), :]
        return 0

    lax.fori_loop(0, PIECES, own_piece, 0)

    square = square_out[tp]
    every(square_in.at[pl.ds(0, tp_count - 1)], sq_send, sq_recv).wait_recv()
    for step in range(1, tp_count):
        square = square + square_in[(tp + step) % tp_count]
    mean = square[:1, :] / (channels * tp_count)
    spread = jnp.broadcast_to(lax.rsqrt(mean + 1e-05), (ROWS, ROWS))
    scale = jnp.sum(jnp.where(t_row == s_col, spread, 0.0), axis=1, keepdims=True)

    every(own_in, own_send, own_recv).wait_recv()

    def finish(p, _):
        far_copy(p).wait_recv()
        total = own_acc[p] + own_in[p].astype(f32) + far_in[p].astype(f32)
        out_ref[:, tile_of(p, piece)] = (total * scale).astype(bf16)
        return 0

    lax.fori_loop(0, PIECES, finish, 0)

    every(full.at[chip, :, mine], x_send, x_recv.at[0]).wait_send()
    every(full.at[1 - chip, :, mine], f_send, f_recv.at[0]).wait_send()
    beside(mine).wait_send()

    @pl.when(seq < seq_count - 1)
    def _():
        to_next().wait_send()

    @pl.when(side == 0)
    def _():
        every(sums_out, sums_send, sums_recv.at[0]).wait_send()

    every(decay_in.at[others], decay_send, decay_recv).wait_send()
    every(owned.at[:, others], state_send, state_recv.at[0]).wait_send()
    every(back.at[:, others], back_send, back_recv.at[0]).wait_send()
    every(square_in.at[pl.ds(0, tp_count - 1)], sq_send, sq_recv).wait_send()
    every(near_out, near_send, near_recv.at[0]).wait_send()
    every(far_out, far_send, far_recv.at[0]).wait_send()
    every(own_out, own_send, own_recv).wait_send()


def fused(
    tokens, gate_weight, inner_weight, state_weight, step_weight, conv_inner, conv_state,
    step_bias, decay_rate, skip_gain, norm_gain, out_weight,
):
    rows, width = tokens.shape
    channels = inner_weight.shape[1]
    heads = step_weight.shape[1]
    if channels > 5 * 256 or rows < 3 * ROWS:
        return on_device(
            tokens, gate_weight, inner_weight, state_weight, step_weight, conv_inner, conv_state,
            step_bias, decay_rate, skip_gain, norm_gain, out_weight,
        )
    head_width = channels // heads
    states = state_weight.shape[1] // 2
    depth, out_width = inner_weight.shape[0], out_weight.shape[1]
    seq_count, tp_count = lax.axis_size("seq"), lax.axis_size("tp")
    chunks = rows // ROWS
    quarter = seq_count // 2
    share = states // quarter
    tile = min(256, channels)
    tiles = channels // tile
    arrivals = chunks + 2
    piece = out_width // PIECES
    f32, bf16 = jnp.float32, jnp.bfloat16
    dma, vmem = pltpu.SemaphoreType.DMA, pltpu.VMEM
    args = (
        tokens, gate_weight, inner_weight, state_weight, step_weight.T, conv_inner, conv_state,
        step_bias[None, :], decay_rate[None, :], skip_gain[None, :], norm_gain.reshape(-1, 128), out_weight,
    )
    scratch = [
        vmem((2, rows, 2 * width), bf16),
        vmem((depth, channels), bf16),
        vmem((depth, channels), bf16),
        vmem((depth, 2 * states), bf16),
        vmem((heads, depth), bf16),
        vmem(conv_inner.shape, f32),
        vmem(conv_state.shape, f32),
        vmem((1, heads), f32),
        vmem((1, heads), f32),
        vmem((1, heads), f32),
        vmem((channels // 128, 128), f32),
        vmem((channels, out_width), bf16),
        vmem((rows, channels + 2 * states), f32),
        vmem((8, channels + 2 * states), f32),
        vmem((8, channels + 2 * states), f32),
        vmem((rows, heads), f32),
        vmem((rows, channels), bf16),
        vmem((rows, 2 * states), bf16),
        vmem((rows, channels), f32),
        vmem((rows, channels), f32),
        vmem((rows, channels), bf16),
        vmem((rows, heads), f32),
        vmem((rows, heads), f32),
        vmem((rows, heads), f32),
        vmem((chunks, 8, heads), f32),
        vmem((tiles, states, tile), f32),
        vmem((chunks, tiles, states, tile), bf16),
        vmem((tiles, states, tile), bf16),
        vmem((tiles, quarter, share, tile), bf16),
        vmem((tiles, quarter, share, tile), f32),
        vmem((tiles, share, tile), bf16),
        vmem((tiles, share, tile), bf16),
        vmem((tiles, quarter, share, tile), bf16),
        vmem((tiles, states, tile), bf16),
        vmem((8, 128), f32),
        vmem((quarter, 8, 128), f32),
        vmem((2, ROWS, 128), f32),
        vmem((tp_count, 8, ROWS), f32),
        vmem((tp_count, 8, ROWS), f32),
    ]
    half_sums = vmem((PIECES, ROWS, piece), bf16)
    whole_sums = vmem((PIECES, ROWS, piece), f32)
    scratch += [half_sums, half_sums, whole_sums, half_sums, half_sums, half_sums, half_sums, whole_sums]
    scratch += [vmem((2 * ROWS, piece), f32)]
    scratch += [pltpu.SemaphoreType.REGULAR, dma((15,))]
    scratch += [dma, dma((arrivals,)), dma, dma((arrivals,)), dma, dma, dma, dma]
    scratch += [dma, dma((tiles,)), dma, dma((tiles,)), dma, dma, dma, dma((tiles,))]
    scratch += [dma, dma, dma, dma((PIECES,)), dma, dma((PIECES,)), dma, dma]
    anywhere = pl.BlockSpec(memory_space=pl.ANY)
    return pl.pallas_call(
        lambda *refs: layer_kernel(head_width, *refs),
        out_shape=pltpu.VMEM((rows // tp_count, out_width), bf16),
        in_specs=[anywhere] * len(args),
        out_specs=pl.BlockSpec(memory_space=pltpu.VMEM),
        scratch_shapes=scratch,
        compiler_params=pltpu.CompilerParams(
            collective_id=0, has_side_effects=True, vmem_limit_bytes=VMEM_LIMIT
        ),
        name="layer",
    )(*args)


def on_device(
    tokens,
    gate_weight,
    inner_weight,
    state_weight,
    step_weight,
    conv_inner,
    conv_state,
    step_bias,
    decay_rate,
    skip_gain,
    norm_gain,
    out_weight,
):
    tok_rows = tokens.shape[0]
    width_inner = inner_weight.shape[1]
    head_count = step_weight.shape[1]
    head_width = width_inner // head_count
    state_size = state_weight.shape[1] // 2
    blocks = tok_rows // GROUP
    size_tp = lax.axis_size("tp")
    me = lax.axis_index("tp")

    chunks = [None] * blocks
    for b in range(blocks - 1, -1, -1):
        chunks[b] = gather_features(tokens[b * GROUP : (b + 1) * GROUP])
    halo = shifted(chunks[-1][GROUP - HALO :], 1)
    chunks[0] = jnp.concatenate([halo, chunks[0]], axis=0)

    inner_raw, state_raw, step_raw = [None] * blocks, [None] * blocks, [None] * blocks
    for b in range(blocks - 1, -1, -1):
        i_b, s_b, t_b = project(chunks[b], inner_weight, state_weight, step_weight)
        inner_raw[b], state_raw[b] = i_b.astype(jnp.bfloat16), s_b.astype(jnp.bfloat16)
        step_raw[b] = t_b[HALO:] if b == 0 else t_b

    lanes = max(128, head_width)
    time_step = jax.nn.softplus(jnp.concatenate(step_raw, axis=0) + step_bias[None, :])
    log_decay = -time_step * decay_rate[None, :]
    grouped = log_decay.reshape(blocks, GROUP, head_count)
    cumulative = jnp.cumsum(grouped, axis=1)
    ending = cumulative[:, -1]
    tail = (jnp.exp(ending[:, None] - cumulative)).reshape(tok_rows, head_count) * time_step
    cumulative = cumulative.reshape(tok_rows, head_count)

    def cost(flops, count, exps):
        return pl.CostEstimate(flops=flops, bytes_accessed=count, transcendentals=exps)

    whole = tok_rows * width_inner
    x, bc, contribution = pl.pallas_call(
        lambda *refs: conv_kernel(blocks, head_width, lanes, *refs),
        out_shape=(
            jax.ShapeDtypeStruct((tok_rows, width_inner), jnp.bfloat16),
            jax.ShapeDtypeStruct((tok_rows, 2 * state_size), jnp.bfloat16),
            jax.ShapeDtypeStruct((blocks, width_inner, state_size), jnp.float32),
        ),
        cost_estimate=cost(2 * whole * state_size, 6 * whole, whole),
        name="conv",
    )(*inner_raw, *state_raw, conv_inner, conv_state, tail)
    contribution = contribution.reshape(blocks, head_count, head_width, state_size)
    local_state = jnp.zeros((head_count, head_width, state_size), jnp.float32)
    for b in range(blocks):
        local_state = jnp.exp(ending[b])[:, None, None] * local_state + contribution[b]

    def by_rows(width):
        return pl.BlockSpec((GROUP, width), lambda b: (b, 0))

    def by_columns(height):
        return pl.BlockSpec((height, GROUP), lambda b: (0, b))

    def fixed(width):
        return pl.BlockSpec((1, width), lambda b: (0, 0))

    intra = pl.pallas_call(
        lambda *refs: intra_kernel(head_width, lanes, *refs),
        grid=(blocks,),
        in_specs=[
            by_rows(width_inner),
            by_rows(2 * state_size),
            by_rows(head_count),
            by_columns(head_count),
            by_columns(head_count),
            fixed(width_inner),
        ],
        out_specs=by_rows(width_inner),
        out_shape=jax.ShapeDtypeStruct((tok_rows, width_inner), jnp.float32),
        cost_estimate=cost(4 * whole * GROUP, 6 * whole, GROUP * tok_rows * head_count),
        name="intra",
    )(x, bc, cumulative, cumulative.T, time_step.T, jnp.repeat(skip_gain, head_width)[None, :])

    gate = jnp.concatenate(
        [
            jnp.dot(c[c.shape[0] - GROUP :], gate_weight, preferred_element_type=jnp.float32).astype(jnp.bfloat16)
            for c in chunks
        ],
        axis=0,
    )

    carried, intra = earlier_state(
        local_state.astype(jnp.bfloat16).reshape(width_inner, state_size),
        jnp.sum(ending, axis=0),
        head_width,
        intra,
    )
    carried = carried.astype(jnp.float32).reshape(head_count, head_width, state_size)
    states = []
    for b in range(blocks):
        states.append(carried.astype(jnp.bfloat16).reshape(1, width_inner, state_size))
        carried = jnp.exp(ending[b])[:, None, None] * carried + contribution[b]

    gated, squares = pl.pallas_call(
        lambda *refs: gate_kernel(head_width, lanes, *refs),
        grid=(blocks,),
        in_specs=[
            by_rows(width_inner),
            by_rows(2 * state_size),
            by_rows(head_count),
            by_rows(width_inner),
            fixed(width_inner),
            pl.BlockSpec((1, width_inner, state_size), lambda b: (b, 0, 0)),
        ],
        out_specs=(by_rows(width_inner), by_rows(1)),
        out_shape=(
            jax.ShapeDtypeStruct((tok_rows, width_inner), jnp.bfloat16),
            jax.ShapeDtypeStruct((tok_rows, 1), jnp.float32),
        ),
        cost_estimate=cost(2 * whole * state_size, 8 * whole, whole),
        name="gate",
    )(intra, bc, cumulative, gate, norm_gain[None, :], jnp.concatenate(states, axis=0))

    square_total = sum_over_tp(squares[:, 0])
    share = tok_rows // size_tp
    mean_square = lax.dynamic_slice(square_total, (me * share,), (share,)) / (width_inner * size_tp)
    scale = lax.rsqrt(mean_square + 1e-05)[:, None]

    if size_tp != 4:
        part = jnp.dot(gated, out_weight, preferred_element_type=jnp.float32).astype(jnp.bfloat16)
        total = lax.psum_scatter(part, "tp", scatter_dimension=0, tiled=True)
        return (total.astype(jnp.float32) * scale).astype(jnp.bfloat16)

    side = me // 2

    def reduced(chip, weight):
        rows = lax.dynamic_slice(gated, (chip * 2 * share, 0), (2 * share, width_inner))
        both = jnp.dot(rows, weight, preferred_element_type=jnp.float32).astype(jnp.bfloat16)
        shape = (share, weight.shape[1])
        away = lax.dynamic_slice(both, ((1 - me % 2) * share, 0), shape)
        own = lax.dynamic_slice(both, ((me % 2) * share, 0), shape)
        return own.astype(jnp.float32) + swapped(away, 1).astype(jnp.float32)

    cuts = 2
    width_out = out_weight.shape[1] // cuts
    weights = [out_weight[:, c * width_out : (c + 1) * width_out] for c in range(cuts)]
    arrived = [swapped(reduced(side ^ 1, w).astype(jnp.bfloat16), 2) for w in weights]
    results = []
    for w, other in zip(weights, arrived):
        total = reduced(side, w) + other.astype(jnp.float32)
        results.append((total * scale).astype(jnp.bfloat16))
    return jnp.concatenate(results, axis=1)


def solution(mesh):
    in_specs = (
        P("seq", "tp"),
        P(None, "tp"),
        P(None, "tp"),
        P(),
        P(None, "tp"),
        P(None, "tp"),
        P(),
        P("tp"),
        P("tp"),
        P("tp"),
        P("tp"),
        P("tp", None),
    )
    out_specs = P(("seq", "tp"), None)
    quick = mesh.shape["tp"] == 4 and mesh.shape["seq"] == 8
    return jax.shard_map(
        fused if quick else on_device, mesh=mesh, in_specs=in_specs, out_specs=out_specs, check_vma=False
    )
```
